512 devices in a mesh: gx: 16 (over z_lo, core), gy: 32 (over x, z_hi, y).
Axes of the slice: x: 4, y: 4, z: 16 (z_hi: 2, z_lo: 8; z = z_hi * 8 + z_lo), core: 2. Of those that a mesh axis runs over, the one named last changes fastest.
Arguments:
- field: float32 [5, 1, 512, 4096], P(None, None, 'gx', 'gy'), may hold values from -6 to 6
- cotangent: float32 [5, 1, 512, 4096], P(None, None, 'gx', 'gy'), may hold values from -6 to 6
- lift: float32 [15, 32], replicated, may hold values from -1.5 to 1.5
- spectral: float32 [2, 2, 64, 32, 32], replicated, may hold values from -6 to 6
- pointwise: float32 [2, 32, 32], replicated, may hold values from -1 to 1
- project: float32 [32, 5], replicated, may hold values from -1 to 1
Outputs:
- field_grad: float32 [5, 1, 512, 4096], P(None, None, 'gx', 'gy')
The draws below stay inside these ranges and needn't reach their ends.
All inputs are finite; a program needn't handle non-finite values.
Results may differ from the reference program's by a relative error of at most 0.0003.
Values sent between devices are 32-bit elements; how exact they have to be, the bound alone decides.
A program may use at most 64 MiB of HBM per device.

```python
import jax
import jax.numpy as jnp
from jax import lax

VARS = 5
W = 32
MODES = 8
LAYERS = 2
NZ = 1
PX = 32
PY = 128
NX = 512
NY = 4096
N_GX = 16
N_GY = 32


def block_scale(rng, extent, split, smallest, high):
    factor_of, own = 1.0, jax.random.fold_in(rng, 6)
    for axis_at, blocks in split:
        heights = jnp.exp(jax.random.uniform(jax.random.fold_in(own, axis_at), (blocks,), jnp.float32, smallest / len(split), high / len(split)))
        factor_of = factor_of * jnp.repeat(heights, extent[axis_at] // blocks).reshape([-1 if axis == axis_at else 1 for axis in range(len(extent))])
    return factor_of


def gaussian(own_key, shape, deviation, limit, shards=(), kind=jnp.bfloat16):
    gain = block_scale(own_key, shape, shards, -0.22, 0.18) if shards else 1.0
    drawn = jax.random.normal(own_key, shape, jnp.float32) * deviation * gain
    return jnp.minimum(jnp.maximum(drawn, -limit), limit).astype(kind)


def setup_inputs(seed: int = 0) -> dict:
    streams_of = jax.random.split(jax.random.key(seed), 7)
    return {
        "field": gaussian(streams_of[0], (VARS, NZ, NX, NY), 1.0, 6.0, ((2, 16), (3, 32)), jnp.float32),
        "cotangent": gaussian(streams_of[1], (VARS, NZ, NX, NY), 1.0, 6.0, ((2, 16), (3, 32)), jnp.float32),
        "lift": gaussian(streams_of[2], (3 * VARS, W), (3 * VARS) ** -0.5, 1.5, (), jnp.float32),
        "spectral": gaussian(streams_of[3], (LAYERS, 2, MODES * MODES, W, W), ((PX * PY) ** 0.5 * (2 * W * MODES * MODES) ** -0.5), 6.0, (), jnp.float32),
        "pointwise": gaussian(streams_of[4], (LAYERS, W, W), W ** -0.5, 1.0, (), jnp.float32),
        "project": gaussian(streams_of[5], (W, VARS), W ** -0.5, 1.0, (), jnp.float32),
    }


highest = lax.Precision.HIGHEST

def pooled(values, factor):
    channels, levels, row_count, col_count = values.shape
    blocked = values.reshape(channels, levels, row_count // factor, factor, col_count // factor, factor)
    return blocked.mean(axis=(3, 5))

def spread(grads, factor):
    channels, levels, row_count, col_count = grads.shape
    widened = jnp.broadcast_to(grads[:, :, :, None, :, None], (channels, levels, row_count, factor, col_count, factor))
    return widened.reshape(channels, levels, row_count * factor, col_count * factor) / (factor * factor)

def mode_table(row_count, col_count, mode_side):
    cell_ids = jnp.arange(row_count * col_count, dtype=jnp.int32)
    cell_row = cell_ids // col_count
    cell_col = cell_ids % col_count
    mode_ids = jnp.arange(mode_side * mode_side, dtype=jnp.int32)
    wave_x = mode_ids // mode_side - mode_side // 2
    wave_y = mode_ids % mode_side
    period = row_count * col_count
    turns = (cell_row[:, None] * wave_x[None, :] * col_count + cell_col[:, None] * wave_y[None, :] * row_count) % period
    phase_angle = 2.0 * jnp.pi * turns.astype(jnp.float32) / period
    normalizer = 1.0 / jnp.sqrt(jnp.float32(period))
    return jnp.concatenate([jnp.cos(phase_angle), -jnp.sin(phase_angle)], axis=1) * normalizer

def network(features, lift, spectral, pointwise, project, table):
    channels, levels, row_count, col_count = features.shape
    cell_total = row_count * col_count
    hidden_width = lift.shape[1]
    mode_count = table.shape[1] // 2
    hidden = jnp.dot(lift.T, features.reshape(channels, levels * cell_total), precision=highest)
    for layer_index in range(spectral.shape[0]):
        coefficients = jnp.dot(hidden.reshape(hidden_width * levels, cell_total), table, precision=highest)
        coefficients = coefficients.reshape(hidden_width, levels, 2, mode_count)
        real_part = coefficients[:, :, 0]
        imag_part = coefficients[:, :, 1]
        w_real = spectral[layer_index, 0]
        w_imag = spectral[layer_index, 1]
        mixed_real = jnp.einsum('wzk,kwo->ozk', real_part, w_real, precision=highest) - jnp.einsum('wzk,kwo->ozk', imag_part, w_imag, precision=highest)
        mixed_imag = jnp.einsum('wzk,kwo->ozk', imag_part, w_real, precision=highest) + jnp.einsum('wzk,kwo->ozk', real_part, w_imag, precision=highest)
        mixed_modes = jnp.stack([mixed_real, mixed_imag], axis=2).reshape(hidden_width * levels, 2 * mode_count)
        spectral_part = jnp.dot(mixed_modes, table.T, precision=highest).reshape(hidden_width, levels * cell_total)
        pointwise_part = jnp.dot(pointwise[layer_index].T, hidden, precision=highest)
        hidden = jax.nn.gelu(spectral_part + pointwise_part, approximate=False)
    projected = jnp.dot(project.T, hidden, precision=highest)
    return projected.reshape(project.shape[1], levels, row_count, col_count)

def window_of(coarse, first_row, first_col, row_count, col_count):
    row_ids = ((first_row + jnp.arange(row_count, dtype=jnp.int32)) % coarse.shape[2]).astype(jnp.int32)
    col_ids = ((first_col + jnp.arange(col_count, dtype=jnp.int32)) % coarse.shape[3]).astype(jnp.int32)
    return (row_ids, col_ids, jnp.take(jnp.take(coarse, row_ids, axis=2), col_ids, axis=3))

def reference(field, cotangent, lift, spectral, pointwise, project):
    table = mode_table(PX, PY, MODES)
    half_pooled = pooled(field, 2)
    quarter = pooled(field, 4)

    def one_patch(sums_carry, number):
        grad_half, grad_quarter = sums_carry
        patch_row = (number // N_GY).astype(jnp.int32)
        patch_col = (number % N_GY).astype(jnp.int32)
        anchor = (jnp.int32(0), jnp.int32(0), (patch_row * PX).astype(jnp.int32), (patch_col * PY).astype(jnp.int32))
        own_part = lax.dynamic_slice(field, anchor, (VARS, NZ, PX, PY))
        target = lax.dynamic_slice(cotangent, anchor, (VARS, NZ, PX, PY))
        mid_rows, mid_cols, mid_window = window_of(half_pooled, patch_row * (PX // 2) - PX // 4, patch_col * (PY // 2) - PY // 4, PX, PY)
        far_rows, far_cols, far_window = window_of(quarter, patch_row * (PX // 4) - 3 * PX // 8, patch_col * (PY // 4) - 3 * PY // 8, PX, PY)
        features = jnp.concatenate([own_part, mid_window, far_window], axis=0)
        _, pullback = jax.vjp(lambda inputs: network(inputs, lift, spectral, pointwise, project, table), features)
        grad_features, = pullback(target)
        grad_half = grad_half.at[:, :, mid_rows[:, None], mid_cols[None, :]].add(grad_features[VARS:2 * VARS])
        grad_quarter = grad_quarter.at[:, :, far_rows[:, None], far_cols[None, :]].add(grad_features[2 * VARS:])
        return ((grad_half, grad_quarter), grad_features[:VARS])
    start = (jnp.zeros_like(half_pooled), jnp.zeros_like(quarter))
    (grad_half, grad_quarter), own_grads = lax.scan(one_patch, start, jnp.arange(N_GX * N_GY, dtype=jnp.int32))
    own_grads = own_grads.reshape(N_GX, N_GY, VARS, NZ, PX, PY).transpose(2, 3, 0, 4, 1, 5).reshape(VARS, NZ, NX, NY)
    return own_grads + spread(grad_half, 2) + spread(grad_quarter, 4)
```

```python
import functools
import math

import jax
import jax.numpy as jnp
import numpy as np
from jax import lax
from jax.experimental import pallas as pl
from jax.experimental.pallas import tpu as pltpu
from jax.sharding import PartitionSpec as P

F32, BF16 = jnp.float32, jnp.bfloat16
LOOP = False
ROWS, COLS, W, CIN, MD = 32, 128, 32, 16, 8
WAVES = [(0, 0), (1, 0), (1, 1), (2, 0), (2, 1), (3, 0), (3, 1), (4, 0), (4, 1)]
NWAVE = len(WAVES)
HIGHEST = lax.Precision.HIGHEST


def mode_waves():
    j = np.arange(COLS)[:, None]
    kx = np.repeat(np.arange(MD) - MD // 2, MD)[None, :]
    ky = np.tile(np.arange(MD), MD)[None, :]
    b = 2 * np.pi * ((j * ky) % COLS) / COLS
    scale = 1.0 / math.sqrt(ROWS * COLS)
    parts = []
    for k, is_sin in WAVES:
        hit = (np.abs(kx) == k).astype(np.float64)
        if is_sin:
            sg = np.sign(kx) * hit
            re, im = -sg * np.sin(b), -sg * np.cos(b)
        else:
            re, im = hit * np.cos(b), -hit * np.sin(b)
        parts.append(np.concatenate([re, im], axis=1) * scale)
    table = np.concatenate(parts, axis=0).astype(np.float32)
    hi = table.astype(jnp.bfloat16)
    lo = (table - hi.astype(np.float32)).astype(jnp.bfloat16)
    return np.concatenate([hi, lo], axis=1)


def wave(k, i):
    return math.cos(2 * math.pi * k * i / ROWS), math.sin(2 * math.pi * k * i / ROWS)


def weighted(terms):
    total = None
    for c, x in terms:
        if abs(c) < 1e-12:
            continue
        t = x if abs(c - 1) < 1e-12 else (-x if abs(c + 1) < 1e-12 else x * np.float32(c))
        total = t if total is None else total + t
    return total


def tree_sum(xs):
    xs = list(xs)
    while len(xs) > 1:
        xs = [xs[i] + xs[i + 1] if i + 1 < len(xs) else xs[i] for i in range(0, len(xs), 2)]
    return xs[0]


def to_waves(x):
    s = [x[i] + x[i + 16] for i in range(16)]
    d = [x[i] - x[i + 16] for i in range(16)]
    dc = [d[0]] + [d[i] - d[16 - i] for i in range(1, 8)]
    ds = [None] + [d[i] + d[16 - i] for i in range(1, 8)] + [d[8]]
    out = {}
    for k in (1, 3):
        out[(k, 0)] = weighted([(wave(k, i)[0], dc[i]) for i in range(8)])
        out[(k, 1)] = weighted([(wave(k, i)[1], ds[i]) for i in range(1, 9)])
    p = [s[i] + s[i + 8] for i in range(8)]
    m = [s[i] - s[i + 8] for i in range(8)]
    mc = [m[0]] + [m[i] - m[8 - i] for i in range(1, 4)]
    ms = [None] + [m[i] + m[8 - i] for i in range(1, 4)] + [m[4]]
    out[(2, 0)] = weighted([(wave(2, i)[0], mc[i]) for i in range(4)])
    out[(2, 1)] = weighted([(wave(2, i)[1], ms[i]) for i in range(1, 5)])
    q = [p[i] - p[i + 4] for i in range(4)]
    r = np.float32(math.sqrt(0.5))
    out[(4, 0)] = q[0] + r * (q[1] - q[3])
    out[(4, 1)] = q[2] + r * (q[1] + q[3])
    out[(0, 0)] = tree_sum([p[i] + p[i + 4] for i in range(4)])
    return [out[w] for w in WAVES]


def to_rows(a):
    a = dict(zip(WAVES, a))
    r = np.float32(math.sqrt(0.5))
    c0, c4, s4 = a[(0, 0)], a[(4, 0)], a[(4, 1)]
    u, v = r * (c4 + s4), r * (s4 - c4)
    e04 = [c0 + c4, c0 + u, c0 + s4, c0 + v, c0 - c4, c0 - u, c0 - s4, c0 - v]
    c2 = [weighted([(wave(2, i)[0], a[(2, 0)])]) for i in range(4)]
    s2 = [None] + [weighted([(wave(2, i)[1], a[(2, 1)])]) for i in range(1, 5)]
    e2 = [c2[0]] + [c2[i] + s2[i] for i in range(1, 4)] + [s2[4]] + [s2[8 - i] - c2[8 - i] for i in range(5, 8)]
    ev = [e04[i] + e2[i] for i in range(8)] + [e04[i] - e2[i] for i in range(8)]
    oc = [weighted([(wave(k, i)[0], a[(k, 0)]) for k in (1, 3)]) for i in range(8)]
    os_ = [None] + [weighted([(wave(k, i)[1], a[(k, 1)]) for k in (1, 3)]) for i in range(1, 9)]
    od = [oc[0]] + [oc[i] + os_[i] for i in range(1, 8)] + [os_[8]] + [os_[16 - i] - oc[16 - i] for i in range(9, 16)]
    return [ev[i] + od[i] for i in range(16)] + [ev[i] - od[i] for i in range(16)]


def split(x):
    hi = x.astype(BF16)
    lo = (x - hi.astype(F32)).astype(BF16)
    return hi, lo


def tall(x):
    hi, lo = split(x)
    return jnp.concatenate([hi, lo, hi], axis=0)


def wide(x):
    hi, lo = split(x)
    return jnp.concatenate([hi, hi, lo], axis=1)


def channel_mix(left, x_ref, width, out_ref, out_width):
    for i in range(0, ROWS, 2):
        right = jnp.concatenate([tall(x_ref[(i + t) * width:(i + t + 1) * width, :]) for t in range(2)], axis=1)
        got = jnp.dot(left, right, preferred_element_type=F32)
        out_ref[i * out_width:(i + 1) * out_width, :] = got[:, :COLS]
        out_ref[(i + 1) * out_width:(i + 2) * out_width, :] = got[:, COLS:]


def each_group(width, fn):
    if LOOP:
        @pl.loop(0, width // 8)
        def _(n):
            fn(pl.multiple_of(n * 8, 8))
    else:
        for g in range(0, width, 8):
            fn(g)


def analyse(x_ref, width, g_ref, waves_ref):
    def group(g):
        got = to_waves([x_ref[pl.ds(i * width + g, 8), :] for i in range(ROWS)])
        for n in range(NWAVE):
            g_ref[pl.ds(g, 8), n * COLS:(n + 1) * COLS] = got[n]
    each_group(width, group)
    hi, lo = split(g_ref[0:width, :])
    both = jnp.dot(jnp.concatenate([hi, lo], axis=0), waves_ref[...], preferred_element_type=F32)
    return (both[:width, :COLS] + both[width:, :COLS]) + (both[:width, COLS:] + both[width:, COLS:])


def synthesise(coef, width, a_ref, waves_ref):
    hi, lo = split(coef)
    left = jnp.concatenate([jnp.concatenate([hi, hi], axis=1), jnp.concatenate([lo, lo], axis=1)], axis=0)
    both = lax.dot_general(left, waves_ref[...], (((1,), (1,)), ((), ())), preferred_element_type=F32)
    a_ref[0:width, :] = both[:width] + both[width:]


def waves_of(a_ref, g):
    return [a_ref[pl.ds(g, 8), n * COLS:(n + 1) * COLS] for n in range(NWAVE)]


def half_swap(x):
    return jnp.concatenate([x[:, 64:], x[:, :64]], axis=1)


def mix_modes(coef, wr_ref, wi_ref, layer, c_ref):
    c_ref[0:W, :] = coef
    c_ref[W:2 * W, :] = half_swap(coef)
    accs = [None] * 4
    for w in range(W):
        t = (wr_ref[layer, w] * jnp.broadcast_to(c_ref[w:w + 1, :], (W, COLS))
             + wi_ref[layer, w] * jnp.broadcast_to(c_ref[W + w:W + w + 1, :], (W, COLS)))
        accs[w % 4] = t if accs[w % 4] is None else accs[w % 4] + t
    return (accs[0] + accs[1]) + (accs[2] + accs[3])


def unmix_modes(grad, wr_ref, wi_ref, layer, r_ref):
    swapped = half_swap(grad)
    for w in range(W):
        t = wr_ref[layer, w] * grad - wi_ref[layer, w] * swapped
        r_ref[w * 8:(w + 1) * 8, :] = (t[0:8] + t[8:16]) + (t[16:24] + t[24:32])
    return tree_sum([r_ref[pl.ds(s, W, stride=8), :] for s in range(8)])


def gelu_parts(x):
    cdf = 0.5 * lax.erf(x * np.float32(math.sqrt(0.5))) + 0.5
    pdf = jnp.exp(-0.5 * (x * x)) * np.float32(1.0 / math.sqrt(2 * math.pi))
    return x * cdf, cdf + x * pdf


def prepare(spectral_ref, wr_ref, wi_ref):
    for layer in range(2):
        for w in range(W):
            re, im = spectral_ref[layer, 0, w], spectral_ref[layer, 1, w]
            wr_ref[layer, w] = jnp.concatenate([re, re], axis=1)
            wi_ref[layer, w] = jnp.concatenate([-im, im], axis=1)


def network_grad(f_ref, cot_ref, lift_ref, spectral_ref, point_ref, proj_ref, waves_ref, out_ref, scr, prep=True):
    wr, wi, g, a, c, r, pw, h, d1, pc = scr
    if prep:
        prepare(spectral_ref, wr, wi)
    lift16 = jnp.concatenate([lift_ref[...], jnp.zeros((1, W), F32)], axis=0)
    p1, p2 = point_ref[0], point_ref[1]
    both1 = jnp.dot(lift16, p1, precision=HIGHEST, preferred_element_type=F32)
    both1_t = jnp.transpose(both1)
    lift_t = jnp.transpose(lift16)
    proj8 = jnp.concatenate([proj_ref[...], jnp.zeros((3, W), F32)], axis=0)
    proj_t = jnp.transpose(proj8)
    channel_mix(wide(proj_t), cot_ref, 8, pc, W)
    channel_mix(wide(both1_t), f_ref, CIN, pw, W)
    coef = analyse(f_ref, CIN, g, waves_ref)
    coef = jnp.dot(lift_t, coef, precision=HIGHEST, preferred_element_type=F32)
    synthesise(mix_modes(coef, wr, wi, 0, c), W, a, waves_ref)
    def group1(gr):
        rows = to_rows(waves_of(a, gr))
        for i in range(ROWS):
            sl = pl.ds(i * W + gr, 8)
            val, der = gelu_parts(rows[i] + pw[sl, :])
            h[sl, :] = val
            d1[sl, :] = der
    each_group(W, group1)
    channel_mix(wide(jnp.transpose(p2)), h, W, pw, W)
    coef = analyse(h, W, g, waves_ref)
    synthesise(mix_modes(coef, wr, wi, 1, c), W, a, waves_ref)
    def group2(gr):
        rows = to_rows(waves_of(a, gr))
        for i in range(ROWS):
            sl = pl.ds(i * W + gr, 8)
            _, der = gelu_parts(rows[i] + pw[sl, :])
            h[sl, :] = der * pc[sl, :]
    each_group(W, group2)
    channel_mix(wide(p2), h, W, pw, W)
    coef = analyse(h, W, g, waves_ref)
    synthesise(unmix_modes(coef, wr, wi, 1, r), W, a, waves_ref)
    def group3(gr):
        rows = to_rows(waves_of(a, gr))
        for i in range(ROWS):
            sl = pl.ds(i * W + gr, 8)
            h[sl, :] = d1[sl, :] * (rows[i] + pw[sl, :])
    each_group(W, group3)
    channel_mix(wide(both1), h, W, pw, CIN)
    coef = analyse(h, W, g, waves_ref)
    coef = unmix_modes(coef, wr, wi, 0, r)
    coef = jnp.dot(lift16, coef, precision=HIGHEST, preferred_element_type=F32)
    synthesise(coef, CIN, a, waves_ref)
    def group4(gr):
        rows = to_rows(waves_of(a, gr))
        for i in range(ROWS):
            sl = pl.ds(i * CIN + gr, 8)
            out_ref[sl, :] = rows[i] + pw[sl, :]
    each_group(CIN, group4)


VARS = 5
TILE = 8
MESH = pl.DeviceIdType.MESH
AROUND = sorted(
    ((dx, dy) for dx in range(-2, 3) for dy in range(-2, 3) if (dx, dy) != (0, 0)),
    key=lambda o: (o[1] == 0, abs(o[1]), abs(o[0]), o),
)


def tiles_of(dx, dy):
    if abs(dx) == 2 or abs(dy) == 2:
        return 1
    return VARS if dx == 0 or dy == 0 else 3


START = {}
TILES = 0
for _o in AROUND:
    START[_o] = TILES
    TILES += tiles_of(*_o)


def pieces(dx, dy):
    out = []
    far_col, near_col = 0, 32 if dy == -1 else 0
    blocks = {-1: (1,), 0: (0, 1), 1: (0,)}[dx]
    for ch in range(VARS):
        if dx == 0:
            for rb in blocks:
                out.append(("near", ch, rb, near_col, 32, ch, 32 * rb))
            out.append(("far", ch, 0, far_col, 32, ch, 64))
        elif dy == 0:
            out.append(("near", ch, blocks[0], 0, 64, ch, 0))
            out.append(("far", ch, 0, 0, 32, ch, 64))
        else:
            base = 64 * (ch % 2)
            out.append(("near", ch, blocks[0], near_col, 32, ch // 2, base))
            out.append(("far", ch, 0, far_col, 32, ch // 2, base + 32))
    return out


def far_edge_col(dy):
    return 16 if dy == -2 else 0


def near_lane(col, dy=0):
    return 32 + col + 64 * dy


def far_lane(col, dy=0):
    return 48 + col + 32 * dy


FAR_ROW = {-2: 0, -1: 4, 0: 12, 1: 20, 2: 28}


def lane_ids():
    return lax.broadcasted_iota(jnp.int32, (TILE, COLS), 1)


def row_ids():
    return lax.broadcasted_iota(jnp.int32, (TILE, COLS), 0)


def turned(x, shift, axis=1, period=None):
    shift %= period or x.shape[axis]
    return x if shift == 0 else pltpu.roll(x, shift, axis)


class Lanes:
    def __init__(self):
        self.lane = lane_ids()
        self.row = row_ids()
        self.masks = {}

    def mask(self, first, width):
        key = (first, width)
        if key not in self.masks:
            self.masks[key] = (self.lane >= first) & (self.lane < first + width)
        return self.masks[key]

    def put(self, base, value, first, width):
        return value if base is None else jnp.where(self.mask(first, width), value, base)

    def only(self, value, first, width):
        return jnp.where(self.mask(first, width), value, 0.0)


def pool_maps():
    j = np.arange(COLS)[:, None]
    lane = np.arange(COLS)[None, :]
    gather = np.concatenate(
        [((lane - 32) % 64 == j // 2) * 0.25, ((lane - 48) % 32 == j // 4) * 0.0625], axis=1
    )
    spread = np.concatenate(
        [(j - 32 == lane // 2) * 0.25, (j - 48 == lane // 4) * 0.0625], axis=1
    )
    return np.concatenate([gather, spread], axis=0).astype(jnp.bfloat16)


def mapped(rows, table):
    hi, lo = split(rows)
    both = jnp.dot(jnp.concatenate([hi, lo], axis=0), table, preferred_element_type=F32)
    return both[: rows.shape[0]] + both[rows.shape[0]:]


def send_tiles(lanes, near, far, buf):
    rolled = {}

    def near_at(ch, rb, col, lane):
        key = ("n", ch, rb, (lane - near_lane(col)) % 64)
        if key not in rolled:
            rolled[key] = turned(near[ch][rb], key[3], period=64)
        return rolled[key]

    def far_at(ch, col, lane):
        key = ("f", ch, (lane - far_lane(col)) % 32)
        if key not in rolled:
            rolled[key] = turned(far[ch], key[2], period=32)
        return rolled[key]

    strips = {}
    for dx, dy in AROUND:
        start = START[dx, dy]
        if abs(dy) == 2:
            if ("y", dy) not in strips:
                tile = None
                for ch in range(VARS):
                    tile = lanes.put(tile, far_at(ch, far_edge_col(dy), 16 * ch), 16 * ch, 16)
                strips["y", dy] = tile
            buf[start * TILE:(start + 1) * TILE, :] = strips["y", dy]
        elif abs(dx) == 2:
            if ("x", dx) not in strips:
                tile = None
                for ch in range(4):
                    tile = lanes.put(tile, far_at(ch, 0, 32 * ch), 32 * ch, 32)
                last = far_at(4, 0, 0)
                if dx == -2:
                    tile = turned(tile, 4, axis=0)
                else:
                    last = turned(last, 4, axis=0)
                strips["x", dx] = jnp.where(lanes.mask(0, 32) & (lanes.row >= 4), last, tile)
            buf[start * TILE:(start + 1) * TILE, :] = strips["x", dx]
        else:
            tiles = [None] * tiles_of(dx, dy)
            for kind, ch, rb, col, width, tile, lane in pieces(dx, dy):
                value = near_at(ch, rb, col, lane) if kind == "near" else far_at(ch, col, lane)
                tiles[tile] = lanes.put(tiles[tile], value, lane, width)
            for n, value in enumerate(tiles):
                buf[(start + n) * TILE:(start + n + 1) * TILE, :] = value


def tile_at(buf, o, n=0):
    first = (START[o] + n) * TILE
    return buf[first:first + TILE, :]


def read_windows(lanes, near, far, buf, f_ref):
    blocks = {}
    rows = {}
    for ch in range(VARS):
        blocks[ch, 1], blocks[ch, 2] = near[ch]
        rows[ch, 0] = far[ch]
    for dx in (0, -1, 1):
        for dy in (0, -1, 1):
            if (dx, dy) == (0, 0):
                continue
            for kind, ch, rb, col, width, tile, lane in pieces(dx, dy):
                value = tile_at(buf, (dx, dy), tile)
                if kind == "near":
                    key = (ch, {-1: 0, 0: 1 + rb, 1: 3}[dx])
                    to, table = near_lane(col, dy), blocks
                else:
                    key, to, table = (ch, dx), far_lane(col, dy), rows
                table[key] = lanes.put(table.get(key), turned(value, to - lane), to, width)
    for dx in (-2, 2):
        for dy in (0, -1, 1):
            value = tile_at(buf, (dx, dy))
            low = turned(value, 4, axis=0)
            for ch in range(VARS):
                to, lane = far_lane(0, dy), 32 * ch if ch < 4 else 0
                got = turned(value if ch < 4 else low, to - lane)
                rows[ch, dx] = lanes.put(rows.get((ch, dx)), got, to, 32)
    for dx in range(-2, 3):
        for dy in (-2, 2):
            value = tile_at(buf, (dx, dy))
            if dx == -2:
                value = turned(value, 4, axis=0)
            for ch in range(VARS):
                to = far_lane(far_edge_col(dy), dy)
                rows[ch, dx] = lanes.put(rows[ch, dx], turned(value, to - 16 * ch), to, 16)
    for (ch, k), value in blocks.items():
        f_ref[pl.ds(8 * k * CIN + VARS + ch, TILE, stride=CIN), :] = value
    for (ch, dx), value in rows.items():
        count = 4 if abs(dx) == 2 else TILE
        f_ref[pl.ds(FAR_ROW[dx] * CIN + 2 * VARS + ch, count, stride=CIN), :] = value[:count]


def window_tiles(go):
    near = {(ch, k): go[pl.ds(8 * k * CIN + VARS + ch, TILE, stride=CIN), :] for ch in range(VARS) for k in range(4)}
    far = {}
    for ch in range(VARS):
        for dx in range(-2, 3):
            first = 24 if dx == 2 else FAR_ROW[dx]
            far[ch, dx] = go[pl.ds(first * CIN + 2 * VARS + ch, TILE, stride=CIN), :]
    return near, far


def send_grads(lanes, near, far, buf):
    for dx, dy in AROUND:
        start = START[dx, dy]
        if abs(dy) == 2:
            tile = None
            for ch in range(VARS):
                got = turned(far[ch, dx], 16 * ch - far_lane(far_edge_col(dy), dy))
                tile = lanes.put(tile, got, 16 * ch, 16)
            if abs(dx) == 2:
                tile = turned(tile, 4, axis=0)
                keep = lanes.row >= 4 if dx == -2 else lanes.row < 4
                tile = jnp.where(keep, tile, 0.0)
            buf[start * TILE:(start + 1) * TILE, :] = tile
        elif abs(dx) == 2:
            tile = None
            for ch in range(4):
                tile = lanes.put(tile, turned(far[ch, dx], 32 * ch - far_lane(0, dy)), 32 * ch, 32)
            last = turned(far[4, dx], -far_lane(0, dy))
            if dx == -2:
                last = turned(last, 4, axis=0)
            else:
                tile = turned(tile, 4, axis=0)
            buf[start * TILE:(start + 1) * TILE, :] = jnp.where(lanes.mask(0, 32) & (lanes.row >= 4), last, tile)
        else:
            tiles = [None] * tiles_of(dx, dy)
            for kind, ch, rb, col, width, tile, lane in pieces(dx, dy):
                if kind == "near":
                    value = turned(near[ch, {-1: 0, 0: 1 + rb, 1: 3}[dx]], lane - near_lane(col, dy))
                else:
                    value = turned(far[ch, dx], lane - far_lane(col, dy))
                tiles[tile] = lanes.put(tiles[tile], value, lane, width)
            for n, value in enumerate(tiles):
                buf[(start + n) * TILE:(start + n + 1) * TILE, :] = value


def sum_grads(lanes, near, far, buf):
    n_sum = {(ch, rb): lanes.only(near[ch, 1 + rb], 32, 64) for ch in range(VARS) for rb in range(2)}
    f_sum = {ch: lanes.only(far[ch, 0], 48, 32) for ch in range(VARS)}
    for dx in (-1, 0, 1):
        for dy in (-1, 0, 1):
            if (dx, dy) == (0, 0):
                continue
            for kind, ch, rb, col, width, tile, lane in pieces(dx, dy):
                value = tile_at(buf, (dx, dy), tile)
                if kind == "near":
                    to = near_lane(col)
                    n_sum[ch, rb] += lanes.only(turned(value, to - lane), to, width)
                else:
                    to = far_lane(col)
                    f_sum[ch] += lanes.only(turned(value, to - lane), to, width)
    for dx in (-2, 2):
        value = tree_sum([tile_at(buf, (dx, dy)) for dy in (-1, 0, 1)])
        low = turned(value, 4, axis=0)
        keep = lanes.row >= 4 if dx == -2 else lanes.row < 4
        for ch in range(VARS):
            natural = (ch < 4) == (dx == 2)
            lane = 32 * ch if ch < 4 else 0
            got = turned(value if natural else low, far_lane(0) - lane)
            f_sum[ch] += jnp.where(lanes.mask(48, 32) & keep, got, 0.0)
    for dy in (-2, 2):
        value = tree_sum([tile_at(buf, (dx, dy)) for dx in range(-2, 3)])
        for ch in range(VARS):
            to = far_lane(far_edge_col(dy))
            f_sum[ch] += lanes.only(turned(value, to - 16 * ch), to, 16)
    return (
        jnp.concatenate([n_sum[ch, rb] for ch in range(VARS) for rb in range(2)], axis=0),
        jnp.concatenate([f_sum[ch] for ch in range(VARS)], axis=0),
    )


def kernel(counts, field_hbm, cot_hbm, lift_hbm, spectral_hbm, point_hbm, proj_hbm, waves_hbm, maps_hbm, out_ref,
           field, cot, lift, spectral, point, proj, waves, maps, f, ct, go, pooled, spread_near, spread_far,
           fwd_out, fwd_in, bwd_out, bwd_in, load_sem, send_sem, recv_sem, *scr):
    gx, gy = lax.axis_index("gx"), lax.axis_index("gy")
    n_gx, n_gy = counts

    def device(dx, dy):
        return (lax.rem(gx + (dx + n_gx), n_gx), lax.rem(gy + (dy + n_gy), n_gy))

    barrier = pltpu.get_barrier_semaphore()
    for dx, dy in AROUND:
        pl.semaphore_signal(barrier, inc=1, device_id=device(dx, dy), device_id_type=MESH)
    loads = [
        pltpu.make_async_copy(src, dst, load_sem.at[n])
        for n, (src, dst) in enumerate([
            (field_hbm, field), (maps_hbm, maps), (cot_hbm, cot), (lift_hbm, lift), (point_hbm, point),
            (proj_hbm, proj), (spectral_hbm, spectral), (waves_hbm, waves)])
    ]
    for copy in loads:
        copy.start()

    def exchange(turn, src, dst):
        copies = {}
        for n, (dx, dy) in enumerate(AROUND):
            sign = -1 if turn == 0 else 1
            span = pl.ds(START[dx, dy] * TILE, tiles_of(dx, dy) * TILE)
            copies[dx, dy] = pltpu.make_async_remote_copy(
                src_ref=src.at[span], dst_ref=dst.at[span], send_sem=send_sem.at[turn, n], recv_sem=recv_sem.at[turn, n],
                device_id=device(sign * dx, sign * dy), device_id_type=MESH)
            copies[dx, dy].start()
        return copies

    lanes = Lanes()
    loads[0].wait()
    loads[1].wait()
    half = field[pl.ds(0, 80, stride=2), :] + field[pl.ds(1, 80, stride=2), :]
    pooled[...] = half
    quarter = pooled[pl.ds(0, 40, stride=2), :] + pooled[pl.ds(1, 40, stride=2), :]
    got = mapped(jnp.concatenate([half, quarter], axis=0), maps[0:COLS, :])
    near = [[got[ch * 16 + rb * 8:ch * 16 + rb * 8 + 8, :COLS] for rb in range(2)] for ch in range(VARS)]
    far = [got[80 + ch * 8:80 + ch * 8 + 8, COLS:] for ch in range(VARS)]
    send_tiles(lanes, near, far, fwd_out)
    pl.semaphore_wait(barrier, len(AROUND))
    sent = exchange(0, fwd_out, fwd_in)

    for copy in loads[2:]:
        copy.wait()
    f[...] = jnp.zeros_like(f)
    ct[...] = jnp.zeros_like(ct)
    for v in range(VARS):
        f[pl.ds(v, ROWS, stride=CIN), :] = field[v * ROWS:(v + 1) * ROWS, :]
        ct[pl.ds(v, ROWS, stride=8), :] = cot[v * ROWS:(v + 1) * ROWS, :]
    prepare(spectral, scr[0], scr[1])
    for copy in sent.values():
        copy.wait_recv()
    read_windows(lanes, near, far, fwd_in, f)
    network_grad(f, ct, lift, spectral, point, proj, waves, go, scr, prep=False)

    near, far = window_tiles(go)
    send_grads(lanes, near, far, bwd_out)
    back = exchange(1, bwd_out, bwd_in)
    for copy in back.values():
        copy.wait_recv()
    n_sum, f_sum = sum_grads(lanes, near, far, bwd_in)
    got = mapped(jnp.concatenate([n_sum, f_sum], axis=0), maps[COLS:, :])
    for k in range(2):
        spread_near[pl.ds(k, 80, stride=2), :] = got[:80, :COLS]
    for k in range(4):
        spread_far[pl.ds(k, 40, stride=4), :] = got[80:, COLS:]
    for v in range(VARS):
        span = slice(v * ROWS, (v + 1) * ROWS)
        out_ref[span, :] = go[pl.ds(v, ROWS, stride=CIN), :] + spread_near[span, :] + spread_far[span, :]
    for copies in (sent, back):
        for copy in copies.values():
            copy.wait_send()


def body(counts, field, cotangent, lift, spectral, pointwise, project):
    vmem = lambda *shape, dtype=F32: pltpu.VMEM(shape, dtype)
    flat = (VARS * ROWS, COLS)
    hbm = pl.BlockSpec(memory_space=pltpu.MemorySpace.HBM)
    call = pl.pallas_call(
        functools.partial(kernel, counts),
        out_shape=jax.ShapeDtypeStruct(flat, F32),
        in_specs=[hbm] * 8,
        out_specs=pl.BlockSpec(memory_space=pltpu.VMEM),
        scratch_shapes=[
            vmem(*flat), vmem(*flat), vmem(3 * VARS, W), vmem(2, 2, W, W, MD * MD), vmem(2, W, W), vmem(VARS, W),
            vmem(NWAVE * COLS, 2 * COLS, dtype=BF16), vmem(2 * COLS, 2 * COLS, dtype=BF16),
            vmem(ROWS * CIN, COLS), vmem(ROWS * 8, COLS), vmem(ROWS * CIN, COLS),
            vmem(80, COLS), vmem(*flat), vmem(*flat),
            vmem(TILES * TILE, COLS), vmem(TILES * TILE, COLS), vmem(TILES * TILE, COLS), vmem(TILES * TILE, COLS),
            pltpu.SemaphoreType.DMA((8,)), pltpu.SemaphoreType.DMA((2, len(AROUND))),
            pltpu.SemaphoreType.DMA((2, len(AROUND))),
            vmem(2, W, W, COLS), vmem(2, W, W, COLS), vmem(W, NWAVE * COLS), vmem(W, NWAVE * COLS),
            vmem(2 * W, COLS), vmem(W * 8, COLS), vmem(ROWS * W, COLS), vmem(ROWS * W, COLS), vmem(ROWS * W, COLS),
            vmem(ROWS * W, COLS),
        ],
        compiler_params=pltpu.CompilerParams(collective_id=0, has_side_effects=True, vmem_limit_bytes=48 << 20),
        name="patch_grad",
    )
    out = call(
        field.reshape(flat), cotangent.reshape(flat), lift, spectral.transpose(0, 1, 3, 4, 2), pointwise, project.T,
        jnp.asarray(mode_waves()), jnp.asarray(pool_maps()))
    return out.reshape(field.shape)


def solution(mesh):
    counts = (mesh.shape["gx"], mesh.shape["gy"])
    return jax.shard_map(
        functools.partial(body, counts),
        mesh=mesh,
        in_specs=(P(None, None, "gx", "gy"), P(None, None, "gx", "gy"), P(), P(), P(), P()),
        out_specs=P(None, None, "gx", "gy"),
        check_vma=False,
    )
```

```python
import functools
import math

import jax
import jax.numpy as jnp
import numpy as np
from jax import lax
from jax.experimental import pallas as pl
from jax.experimental.pallas import tpu as pltpu
from jax.sharding import PartitionSpec as P

F32, BF16 = jnp.float32, jnp.bfloat16
LOOP = False
ROWS, COLS, W, CIN, MD = 32, 128, 32, 16, 8
WAVES = [(0, 0), (1, 0), (1, 1), (2, 0), (2, 1), (3, 0), (3, 1), (4, 0), (4, 1)]
NWAVE = len(WAVES)
HIGHEST = lax.Precision.HIGHEST


def mode_waves():
    j = np.arange(COLS)[:, None]
    kx = np.repeat(np.arange(MD) - MD // 2, MD)[None, :]
    ky = np.tile(np.arange(MD), MD)[None, :]
    b = 2 * np.pi * ((j * ky) % COLS) / COLS
    scale = 1.0 / math.sqrt(ROWS * COLS)
    parts = []
    for k, is_sin in WAVES:
        hit = (np.abs(kx) == k).astype(np.float64)
        if is_sin:
            sg = np.sign(kx) * hit
            re, im = -sg * np.sin(b), -sg * np.cos(b)
        else:
            re, im = hit * np.cos(b), -hit * np.sin(b)
        parts.append(np.concatenate([re, im], axis=1) * scale)
    table = np.concatenate(parts, axis=0).astype(np.float32)
    hi = table.astype(jnp.bfloat16)
    lo = (table - hi.astype(np.float32)).astype(jnp.bfloat16)
    return np.concatenate([hi, lo], axis=1)


def wave(k, i):
    return math.cos(2 * math.pi * k * i / ROWS), math.sin(2 * math.pi * k * i / ROWS)


def weighted(terms):
    total = None
    for c, x in terms:
        if abs(c) < 1e-12:
            continue
        t = x if abs(c - 1) < 1e-12 else (-x if abs(c + 1) < 1e-12 else x * np.float32(c))
        total = t if total is None else total + t
    return total


def tree_sum(xs):
    xs = list(xs)
    while len(xs) > 1:
        xs = [xs[i] + xs[i + 1] if i + 1 < len(xs) else xs[i] for i in range(0, len(xs), 2)]
    return xs[0]


def to_waves(x):
    s = [x[i] + x[i + 16] for i in range(16)]
    d = [x[i] - x[i + 16] for i in range(16)]
    dc = [d[0]] + [d[i] - d[16 - i] for i in range(1, 8)]
    ds = [None] + [d[i] + d[16 - i] for i in range(1, 8)] + [d[8]]
    out = {}
    for k in (1, 3):
        out[(k, 0)] = weighted([(wave(k, i)[0], dc[i]) for i in range(8)])
        out[(k, 1)] = weighted([(wave(k, i)[1], ds[i]) for i in range(1, 9)])
    p = [s[i] + s[i + 8] for i in range(8)]
    m = [s[i] - s[i + 8] for i in range(8)]
    mc = [m[0]] + [m[i] - m[8 - i] for i in range(1, 4)]
    ms = [None] + [m[i] + m[8 - i] for i in range(1, 4)] + [m[4]]
    out[(2, 0)] = weighted([(wave(2, i)[0], mc[i]) for i in range(4)])
    out[(2, 1)] = weighted([(wave(2, i)[1], ms[i]) for i in range(1, 5)])
    q = [p[i] - p[i + 4] for i in range(4)]
    r = np.float32(math.sqrt(0.5))
    out[(4, 0)] = q[0] + r * (q[1] - q[3])
    out[(4, 1)] = q[2] + r * (q[1] + q[3])
    out[(0, 0)] = tree_sum([p[i] + p[i + 4] for i in range(4)])
    return [out[w] for w in WAVES]


def to_rows(a):
    a = dict(zip(WAVES, a))
    r = np.float32(math.sqrt(0.5))
    c0, c4, s4 = a[(0, 0)], a[(4, 0)], a[(4, 1)]
    u, v = r * (c4 + s4), r * (s4 - c4)
    e04 = [c0 + c4, c0 + u, c0 + s4, c0 + v, c0 - c4, c0 - u, c0 - s4, c0 - v]
    c2 = [weighted([(wave(2, i)[0], a[(2, 0)])]) for i in range(4)]
    s2 = [None] + [weighted([(wave(2, i)[1], a[(2, 1)])]) for i in range(1, 5)]
    e2 = [c2[0]] + [c2[i] + s2[i] for i in range(1, 4)] + [s2[4]] + [s2[8 - i] - c2[8 - i] for i in range(5, 8)]
    ev = [e04[i] + e2[i] for i in range(8)] + [e04[i] - e2[i] for i in range(8)]
    oc = [weighted([(wave(k, i)[0], a[(k, 0)]) for k in (1, 3)]) for i in range(8)]
    os_ = [None] + [weighted([(wave(k, i)[1], a[(k, 1)]) for k in (1, 3)]) for i in range(1, 9)]
    od = [oc[0]] + [oc[i] + os_[i] for i in range(1, 8)] + [os_[8]] + [os_[16 - i] - oc[16 - i] for i in range(9, 16)]
    return [ev[i] + od[i] for i in range(16)] + [ev[i] - od[i] for i in range(16)]


def split(x):
    hi = x.astype(BF16)
    lo = (x - hi.astype(F32)).astype(BF16)
    return hi, lo


def tall(x):
    hi, lo = split(x)
    return jnp.concatenate([hi, lo, hi], axis=0)


def wide(x):
    hi, lo = split(x)
    return jnp.concatenate([hi, hi, lo], axis=1)


def channel_mix(left, x_ref, width, out_ref, out_width):
    for i in range(0, ROWS, 2):
        right = jnp.concatenate([tall(x_ref[(i + t) * width:(i + t + 1) * width, :]) for t in range(2)], axis=1)
        got = jnp.dot(left, right, preferred_element_type=F32)
        out_ref[i * out_width:(i + 1) * out_width, :] = got[:, :COLS]
        out_ref[(i + 1) * out_width:(i + 2) * out_width, :] = got[:, COLS:]


def each_group(width, fn):
    if LOOP:
        @pl.loop(0, width // 8)
        def _(n):
            fn(pl.multiple_of(n * 8, 8))
    else:
        for g in range(0, width, 8):
            fn(g)


def analyse(x_ref, width, g_ref, waves_ref):
    def group(g):
        got = to_waves([x_ref[pl.ds(i * width + g, 8), :] for i in range(ROWS)])
        for n in range(NWAVE):
            g_ref[pl.ds(g, 8), n * COLS:(n + 1) * COLS] = got[n]
    each_group(width, group)
    hi, lo = split(g_ref[0:width, :])
    both = jnp.dot(jnp.concatenate([hi, lo], axis=0), waves_ref[...], preferred_element_type=F32)
    return (both[:width, :COLS] + both[width:, :COLS]) + (both[:width, COLS:] + both[width:, COLS:])


def synthesise(coef, width, a_ref, waves_ref):
    hi, lo = split(coef)
    left = jnp.concatenate([jnp.concatenate([hi, hi], axis=1), jnp.concatenate([lo, lo], axis=1)], axis=0)
    both = lax.dot_general(left, waves_ref[...], (((1,), (1,)), ((), ())), preferred_element_type=F32)
    a_ref[0:width, :] = both[:width] + both[width:]


def waves_of(a_ref, g):
    return [a_ref[pl.ds(g, 8), n * COLS:(n + 1) * COLS] for n in range(NWAVE)]


def half_swap(x):
    return jnp.concatenate([x[:, 64:], x[:, :64]], axis=1)


def mix_modes(coef, wr_ref, wi_ref, layer, c_ref):
    c_ref[0:W, :] = coef
    c_ref[W:2 * W, :] = half_swap(coef)
    accs = [None] * 4
    for w in range(W):
        t = (wr_ref[layer, w] * jnp.broadcast_to(c_ref[w:w + 1, :], (W, COLS))
             + wi_ref[layer, w] * jnp.broadcast_to(c_ref[W + w:W + w + 1, :], (W, COLS)))
        accs[w % 4] = t if accs[w % 4] is None else accs[w % 4] + t
    return (accs[0] + accs[1]) + (accs[2] + accs[3])


def unmix_modes(grad, wr_ref, wi_ref, layer, r_ref):
    swapped = half_swap(grad)
    for w in range(W):
        t = wr_ref[layer, w] * grad - wi_ref[layer, w] * swapped
        r_ref[w * 8:(w + 1) * 8, :] = (t[0:8] + t[8:16]) + (t[16:24] + t[24:32])
    return tree_sum([r_ref[pl.ds(s, W, stride=8), :] for s in range(8)])


def gelu_parts(x):
    cdf = 0.5 * lax.erf(x * np.float32(math.sqrt(0.5))) + 0.5
    pdf = jnp.exp(-0.5 * (x * x)) * np.float32(1.0 / math.sqrt(2 * math.pi))
    return x * cdf, cdf + x * pdf


def prepare(spectral_ref, wr_ref, wi_ref):
    for layer in range(2):
        for w in range(W):
            re, im = spectral_ref[layer, 0, w], spectral_ref[layer, 1, w]
            wr_ref[layer, w] = jnp.concatenate([re, re], axis=1)
            wi_ref[layer, w] = jnp.concatenate([-im, im], axis=1)


def network_grad(f_ref, cot_ref, lift_ref, spectral_ref, point_ref, proj_ref, waves_ref, out_ref, scr, prep=True):
    wr, wi, g, a, c, r, pw, h, d1, pc = scr
    if prep:
        prepare(spectral_ref, wr, wi)
    lift16 = jnp.concatenate([lift_ref[...], jnp.zeros((1, W), F32)], axis=0)
    p1, p2 = point_ref[0], point_ref[1]
    both1 = jnp.dot(lift16, p1, precision=HIGHEST, preferred_element_type=F32)
    both1_t = jnp.transpose(both1)
    lift_t = jnp.transpose(lift16)
    proj8 = jnp.concatenate([proj_ref[...], jnp.zeros((3, W), F32)], axis=0)
    proj_t = jnp.transpose(proj8)
    channel_mix(wide(proj_t), cot_ref, 8, pc, W)
    channel_mix(wide(both1_t), f_ref, CIN, pw, W)
    coef = analyse(f_ref, CIN, g, waves_ref)
    coef = jnp.dot(lift_t, coef, precision=HIGHEST, preferred_element_type=F32)
    synthesise(mix_modes(coef, wr, wi, 0, c), W, a, waves_ref)
    def group1(gr):
        rows = to_rows(waves_of(a, gr))
        for i in range(ROWS):
            sl = pl.ds(i * W + gr, 8)
            val, der = gelu_parts(rows[i] + pw[sl, :])
            h[sl, :] = val
            d1[sl, :] = der
    each_group(W, group1)
    channel_mix(wide(jnp.transpose(p2)), h, W, pw, W)
    coef = analyse(h, W, g, waves_ref)
    synthesise(mix_modes(coef, wr, wi, 1, c), W, a, waves_ref)
    def group2(gr):
        rows = to_rows(waves_of(a, gr))
        for i in range(ROWS):
            sl = pl.ds(i * W + gr, 8)
            _, der = gelu_parts(rows[i] + pw[sl, :])
            h[sl, :] = der * pc[sl, :]
    each_group(W, group2)
    channel_mix(wide(p2), h, W, pw, W)
    coef = analyse(h, W, g, waves_ref)
    synthesise(unmix_modes(coef, wr, wi, 1, r), W, a, waves_ref)
    def group3(gr):
        rows = to_rows(waves_of(a, gr))
        for i in range(ROWS):
            sl = pl.ds(i * W + gr, 8)
            h[sl, :] = d1[sl, :] * (rows[i] + pw[sl, :])
    each_group(W, group3)
    channel_mix(wide(both1), h, W, pw, CIN)
    coef = analyse(h, W, g, waves_ref)
    coef = unmix_modes(coef, wr, wi, 0, r)
    coef = jnp.dot(lift16, coef, precision=HIGHEST, preferred_element_type=F32)
    synthesise(coef, CIN, a, waves_ref)
    def group4(gr):
        rows = to_rows(waves_of(a, gr))
        for i in range(ROWS):
            sl = pl.ds(i * CIN + gr, 8)
            out_ref[sl, :] = rows[i] + pw[sl, :]
    each_group(CIN, group4)


VARS = 5
TILE = 8
MESH = pl.DeviceIdType.MESH
AROUND = sorted(
    ((dx, dy) for dx in range(-2, 3) for dy in range(-2, 3) if (dx, dy) != (0, 0)),
    key=lambda o: (o[1] == 0, abs(o[1]), abs(o[0]), o),
)


def tiles_of(dx, dy):
    if abs(dx) == 2 or abs(dy) == 2:
        return 1
    return VARS if dx == 0 or dy == 0 else 3


START = {}
TILES = 0
for _o in AROUND:
    START[_o] = TILES
    TILES += tiles_of(*_o)


def pieces(dx, dy):
    out = []
    far_col, near_col = 0, 32 if dy == -1 else 0
    blocks = {-1: (1,), 0: (0, 1), 1: (0,)}[dx]
    for ch in range(VARS):
        if dx == 0:
            for rb in blocks:
                out.append(("near", ch, rb, near_col, 32, ch, 32 * rb))
            out.append(("far", ch, 0, far_col, 32, ch, 64))
        elif dy == 0:
            out.append(("near", ch, blocks[0], 0, 64, ch, 0))
            out.append(("far", ch, 0, 0, 32, ch, 64))
        else:
            base = 64 * (ch % 2)
            out.append(("near", ch, blocks[0], near_col, 32, ch // 2, base))
            out.append(("far", ch, 0, far_col, 32, ch // 2, base + 32))
    return out


def far_edge_col(dy):
    return 16 if dy == -2 else 0


def near_lane(col, dy=0):
    return 32 + col + 64 * dy


def far_lane(col, dy=0):
    return 48 + col + 32 * dy


FAR_ROW = {-2: 0, -1: 4, 0: 12, 1: 20, 2: 28}


def lane_ids():
    return lax.broadcasted_iota(jnp.int32, (TILE, COLS), 1)


def row_ids():
    return lax.broadcasted_iota(jnp.int32, (TILE, COLS), 0)


def turned(x, shift, axis=1, period=None):
    shift %= period or x.shape[axis]
    return x if shift == 0 else pltpu.roll(x, shift, axis)


class Lanes:
    def __init__(self):
        self.lane = lane_ids()
        self.row = row_ids()
        self.masks = {}

    def mask(self, first, width):
        key = (first, width)
        if key not in self.masks:
            self.masks[key] = (self.lane >= first) & (self.lane < first + width)
        return self.masks[key]

    def put(self, base, value, first, width):
        return value if base is None else jnp.where(self.mask(first, width), value, base)

    def only(self, value, first, width):
        return jnp.where(self.mask(first, width), value, 0.0)


def pool_maps():
    j = np.arange(COLS)[:, None]
    lane = np.arange(COLS)[None, :]
    gather = np.concatenate(
        [((lane - 32) % 64 == j // 2) * 0.25, ((lane - 48) % 32 == j // 4) * 0.0625], axis=1
    )
    spread = np.concatenate(
        [(j - 32 == lane // 2) * 0.25, (j - 48 == lane // 4) * 0.0625], axis=1
    )
    return np.concatenate([gather, spread], axis=0).astype(jnp.bfloat16)


def mapped(rows, table):
    hi, lo = split(rows)
    both = jnp.dot(jnp.concatenate([hi, lo], axis=0), table, preferred_element_type=F32)
    return both[: rows.shape[0]] + both[rows.shape[0]:]


def send_tiles(lanes, near, far, buf):
    rolled = {}

    def near_at(ch, rb, col, lane):
        key = ("n", ch, rb, (lane - near_lane(col)) % 64)
        if key not in rolled:
            rolled[key] = turned(near[ch][rb], key[3], period=64)
        return rolled[key]

    def far_at(ch, col, lane):
        key = ("f", ch, (lane - far_lane(col)) % 32)
        if key not in rolled:
            rolled[key] = turned(far[ch], key[2], period=32)
        return rolled[key]

    strips = {}
    for dx, dy in AROUND:
        start = START[dx, dy]
        if abs(dy) == 2:
            if ("y", dy) not in strips:
                tile = None
                for ch in range(VARS):
                    tile = lanes.put(tile, far_at(ch, far_edge_col(dy), 16 * ch), 16 * ch, 16)
                strips["y", dy] = tile
            buf[start * TILE:(start + 1) * TILE, :] = strips["y", dy]
        elif abs(dx) == 2:
            if ("x", dx) not in strips:
                tile = None
                for ch in range(4):
                    tile = lanes.put(tile, far_at(ch, 0, 32 * ch), 32 * ch, 32)
                last = far_at(4, 0, 0)
                if dx == -2:
                    tile = turned(tile, 4, axis=0)
                else:
                    last = turned(last, 4, axis=0)
                strips["x", dx] = jnp.where(lanes.mask(0, 32) & (lanes.row >= 4), last, tile)
            buf[start * TILE:(start + 1) * TILE, :] = strips["x", dx]
        else:
            tiles = [None] * tiles_of(dx, dy)
            for kind, ch, rb, col, width, tile, lane in pieces(dx, dy):
                value = near_at(ch, rb, col, lane) if kind == "near" else far_at(ch, col, lane)
                tiles[tile] = lanes.put(tiles[tile], value, lane, width)
            for n, value in enumerate(tiles):
                buf[(start + n) * TILE:(start + n + 1) * TILE, :] = value


def tile_at(buf, o, n=0):
    first = (START[o] + n) * TILE
    return buf[first:first + TILE, :]


def read_windows(lanes, near, far, buf, f_ref):
    blocks = {}
    rows = {}
    for ch in range(VARS):
        blocks[ch, 1], blocks[ch, 2] = near[ch]
        rows[ch, 0] = far[ch]
    for dx in (0, -1, 1):
        for dy in (0, -1, 1):
            if (dx, dy) == (0, 0):
                continue
            for kind, ch, rb, col, width, tile, lane in pieces(dx, dy):
                value = tile_at(buf, (dx, dy), tile)
                if kind == "near":
                    key = (ch, {-1: 0, 0: 1 + rb, 1: 3}[dx])
                    to, table = near_lane(col, dy), blocks
                else:
                    key, to, table = (ch, dx), far_lane(col, dy), rows
                table[key] = lanes.put(table.get(key), turned(value, to - lane), to, width)
    for dx in (-2, 2):
        for dy in (0, -1, 1):
            value = tile_at(buf, (dx, dy))
            low = turned(value, 4, axis=0)
            for ch in range(VARS):
                to, lane = far_lane(0, dy), 32 * ch if ch < 4 else 0
                got = turned(value if ch < 4 else low, to - lane)
                rows[ch, dx] = lanes.put(rows.get((ch, dx)), got, to, 32)
    for dx in range(-2, 3):
        for dy in (-2, 2):
            value = tile_at(buf, (dx, dy))
            if dx == -2:
                value = turned(value, 4, axis=0)
            for ch in range(VARS):
                to = far_lane(far_edge_col(dy), dy)
                rows[ch, dx] = lanes.put(rows[ch, dx], turned(value, to - 16 * ch), to, 16)
    for (ch, k), value in blocks.items():
        f_ref[pl.ds(8 * k * CIN + VARS + ch, TILE, stride=CIN), :] = value
    for (ch, dx), value in rows.items():
        count = 4 if abs(dx) == 2 else TILE
        f_ref[pl.ds(FAR_ROW[dx] * CIN + 2 * VARS + ch, count, stride=CIN), :] = value[:count]


def window_tiles(go):
    near = {(ch, k): go[pl.ds(8 * k * CIN + VARS + ch, TILE, stride=CIN), :] for ch in range(VARS) for k in range(4)}
    far = {}
    for ch in range(VARS):
        for dx in range(-2, 3):
            first = 24 if dx == 2 else FAR_ROW[dx]
            far[ch, dx] = go[pl.ds(first * CIN + 2 * VARS + ch, TILE, stride=CIN), :]
    return near, far


def send_grads(lanes, near, far, buf):
    for dx, dy in AROUND:
        start = START[dx, dy]
        if abs(dy) == 2:
            tile = None
            for ch in range(VARS):
                got = turned(far[ch, dx], 16 * ch - far_lane(far_edge_col(dy), dy))
                tile = lanes.put(tile, got, 16 * ch, 16)
            if abs(dx) == 2:
                tile = turned(tile, 4, axis=0)
                keep = lanes.row >= 4 if dx == -2 else lanes.row < 4
                tile = jnp.where(keep, tile, 0.0)
            buf[start * TILE:(start + 1) * TILE, :] = tile
        elif abs(dx) == 2:
            tile = None
            for ch in range(4):
                tile = lanes.put(tile, turned(far[ch, dx], 32 * ch - far_lane(0, dy)), 32 * ch, 32)
            last = turned(far[4, dx], -far_lane(0, dy))
            if dx == -2:
                last = turned(last, 4, axis=0)
            else:
                tile = turned(tile, 4, axis=0)
            buf[start * TILE:(start + 1) * TILE, :] = jnp.where(lanes.mask(0, 32) & (lanes.row >= 4), last, tile)
        else:
            tiles = [None] * tiles_of(dx, dy)
            for kind, ch, rb, col, width, tile, lane in pieces(dx, dy):
                if kind == "near":
                    value = turned(near[ch, {-1: 0, 0: 1 + rb, 1: 3}[dx]], lane - near_lane(col, dy))
                else:
                    value = turned(far[ch, dx], lane - far_lane(col, dy))
                tiles[tile] = lanes.put(tiles[tile], value, lane, width)
            for n, value in enumerate(tiles):
                buf[(start + n) * TILE:(start + n + 1) * TILE, :] = value


def sum_grads(lanes, near, far, buf):
    n_sum = {(ch, rb): lanes.only(near[ch, 1 + rb], 32, 64) for ch in range(VARS) for rb in range(2)}
    f_sum = {ch: lanes.only(far[ch, 0], 48, 32) for ch in range(VARS)}
    for dx in (-1, 0, 1):
        for dy in (-1, 0, 1):
            if (dx, dy) == (0, 0):
                continue
            for kind, ch, rb, col, width, tile, lane in pieces(dx, dy):
                value = tile_at(buf, (dx, dy), tile)
                if kind == "near":
                    to = near_lane(col)
                    n_sum[ch, rb] += lanes.only(turned(value, to - lane), to, width)
                else:
                    to = far_lane(col)
                    f_sum[ch] += lanes.only(turned(value, to - lane), to, width)
    for dx in (-2, 2):
        value = tree_sum([tile_at(buf, (dx, dy)) for dy in (-1, 0, 1)])
        low = turned(value, 4, axis=0)
        keep = lanes.row >= 4 if dx == -2 else lanes.row < 4
        for ch in range(VARS):
            natural = (ch < 4) == (dx == 2)
            lane = 32 * ch if ch < 4 else 0
            got = turned(value if natural else low, far_lane(0) - lane)
            f_sum[ch] += jnp.where(lanes.mask(48, 32) & keep, got, 0.0)
    for dy in (-2, 2):
        value = tree_sum([tile_at(buf, (dx, dy)) for dx in range(-2, 3)])
        for ch in range(VARS):
            to = far_lane(far_edge_col(dy))
            f_sum[ch] += lanes.only(turned(value, to - 16 * ch), to, 16)
    return (
        jnp.concatenate([n_sum[ch, rb] for ch in range(VARS) for rb in range(2)], axis=0),
        jnp.concatenate([f_sum[ch] for ch in range(VARS)], axis=0),
    )


def kernel(counts, field_hbm, cot_hbm, lift_hbm, spectral_hbm, point_hbm, proj_hbm, waves_hbm, maps_hbm, out_ref,
           field, cot, lift, spectral, point, proj, waves, maps, f, ct, go, pooled, spread_near, spread_far,
           fwd_out, fwd_in, bwd_out, bwd_in, load_sem, send_sem, recv_sem, *scr):
    gx, gy = lax.axis_index("gx"), lax.axis_index("gy")
    n_gx, n_gy = counts

    def device(dx, dy):
        return (lax.rem(gx + (dx + n_gx), n_gx), lax.rem(gy + (dy + n_gy), n_gy))

    barrier = pltpu.get_barrier_semaphore()
    for dx, dy in AROUND:
        pl.semaphore_signal(barrier, inc=1, device_id=device(dx, dy), device_id_type=MESH)
    loads = [
        pltpu.make_async_copy(src, dst, load_sem.at[n])
        for n, (src, dst) in enumerate([
            (field_hbm, field), (maps_hbm, maps), (cot_hbm, cot), (lift_hbm, lift), (point_hbm, point),
            (proj_hbm, proj), (spectral_hbm, spectral), (waves_hbm, waves)])
    ]
    for copy in loads:
        copy.start()

    def exchange(turn, src, dst):
        copies = {}
        for n, (dx, dy) in enumerate(AROUND):
            sign = -1 if turn == 0 else 1
            span = pl.ds(START[dx, dy] * TILE, tiles_of(dx, dy) * TILE)
            copies[dx, dy] = pltpu.make_async_remote_copy(
                src_ref=src.at[span], dst_ref=dst.at[span], send_sem=send_sem.at[turn, n], recv_sem=recv_sem.at[turn, n],
                device_id=device(sign * dx, sign * dy), device_id_type=MESH)
            copies[dx, dy].start()
        return copies

    lanes = Lanes()
    loads[0].wait()
    loads[1].wait()
    half = field[pl.ds(0, 80, stride=2), :] + field[pl.ds(1, 80, stride=2), :]
    pooled[...] = half
    quarter = pooled[pl.ds(0, 40, stride=2), :] + pooled[pl.ds(1, 40, stride=2), :]
    got = mapped(jnp.concatenate([half, quarter], axis=0), maps[0:COLS, :])
    near = [[got[ch * 16 + rb * 8:ch * 16 + rb * 8 + 8, :COLS] for rb in range(2)] for ch in range(VARS)]
    far = [got[80 + ch * 8:80 + ch * 8 + 8, COLS:] for ch in range(VARS)]
    send_tiles(lanes, near, far, fwd_out)
    pl.semaphore_wait(barrier, len(AROUND))
    sent = exchange(0, fwd_out, fwd_in)

    for copy in loads[2:]:
        copy.wait()
    f[...] = jnp.zeros_like(f)
    ct[...] = jnp.zeros_like(ct)
    for v in range(VARS):
        f[pl.ds(v, ROWS, stride=CIN), :] = field[v * ROWS:(v + 1) * ROWS, :]
        ct[pl.ds(v, ROWS, stride=8), :] = cot[v * ROWS:(v + 1) * ROWS, :]
    prepare(spectral, scr[0], scr[1])
    for copy in sent.values():
        copy.wait_recv()
    read_windows(lanes, near, far, fwd_in, f)
    network_grad(f, ct, lift, spectral, point, proj, waves, go, scr, prep=False)

    near, far = window_tiles(go)
    send_grads(lanes, near, far, bwd_out)
    back = exchange(1, bwd_out, bwd_in)
    for copy in back.values():
        copy.wait_recv()
    n_sum, f_sum = sum_grads(lanes, near, far, bwd_in)
    got = mapped(jnp.concatenate([n_sum, f_sum], axis=0), maps[COLS:, :])
    for k in range(2):
        spread_near[pl.ds(k, 80, stride=2), :] = got[:80, :COLS]
    for k in range(4):
        spread_far[pl.ds(k, 40, stride=4), :] = got[80:, COLS:]
    for v in range(VARS):
        span = slice(v * ROWS, (v + 1) * ROWS)
        out_ref[span, :] = go[pl.ds(v, ROWS, stride=CIN), :] + spread_near[span, :] + spread_far[span, :]
    for copies in (sent, back):
        for copy in copies.values():
            copy.wait_send()


def body(counts, field, cotangent, lift, spectral, pointwise, project):
    vmem = lambda *shape, dtype=F32: pltpu.VMEM(shape, dtype)
    flat = (VARS * ROWS, COLS)
    hbm = pl.BlockSpec(memory_space=pltpu.MemorySpace.HBM)
    call = pl.pallas_call(
        functools.partial(kernel, counts),
        out_shape=pltpu.VMEM(flat, F32),
        in_specs=[hbm] * 8,
        out_specs=pl.BlockSpec(memory_space=pltpu.VMEM),
        scratch_shapes=[
            vmem(*flat), vmem(*flat), vmem(3 * VARS, W), vmem(2, 2, W, W, MD * MD), vmem(2, W, W), vmem(VARS, W),
            vmem(NWAVE * COLS, 2 * COLS, dtype=BF16), vmem(2 * COLS, 2 * COLS, dtype=BF16),
            vmem(ROWS * CIN, COLS), vmem(ROWS * 8, COLS), vmem(ROWS * CIN, COLS),
            vmem(80, COLS), vmem(*flat), vmem(*flat),
            vmem(TILES * TILE, COLS), vmem(TILES * TILE, COLS), vmem(TILES * TILE, COLS), vmem(TILES * TILE, COLS),
            pltpu.SemaphoreType.DMA((8,)), pltpu.SemaphoreType.DMA((2, len(AROUND))),
            pltpu.SemaphoreType.DMA((2, len(AROUND))),
            vmem(2, W, W, COLS), vmem(2, W, W, COLS), vmem(W, NWAVE * COLS), vmem(W, NWAVE * COLS),
            vmem(2 * W, COLS), vmem(W * 8, COLS), vmem(ROWS * W, COLS), vmem(ROWS * W, COLS), vmem(ROWS * W, COLS),
            vmem(ROWS * W, COLS),
        ],
        compiler_params=pltpu.CompilerParams(collective_id=0, has_side_effects=True, vmem_limit_bytes=55300 << 10),
        name="patch_grad",
    )
    out = call(
        field.reshape(flat), cotangent.reshape(flat), lift, spectral.transpose(0, 1, 3, 4, 2), pointwise, project.T,
        jnp.asarray(mode_waves()), jnp.asarray(pool_maps()))
    return out.reshape(field.shape)


def solution(mesh):
    counts = (mesh.shape["gx"], mesh.shape["gy"])
    return jax.shard_map(
        functools.partial(body, counts),
        mesh=mesh,
        in_specs=(P(None, None, "gx", "gy"), P(None, None, "gx", "gy"), P(), P(), P(), P()),
        out_specs=P(None, None, "gx", "gy"),
        check_vma=False,
    )
```

```python
import functools
import math

import jax
import jax.numpy as jnp
import numpy as np
from jax import lax
from jax.experimental import pallas as pl
from jax.experimental.pallas import tpu as pltpu
from jax.sharding import PartitionSpec as P

F32, BF16 = jnp.float32, jnp.bfloat16
LOOP = False
ROWS, COLS, W, CIN, MD = 32, 128, 32, 16, 8
WAVES = [(0, 0), (1, 0), (1, 1), (2, 0), (2, 1), (3, 0), (3, 1), (4, 0), (4, 1)]
NWAVE = len(WAVES)
HIGHEST = lax.Precision.HIGHEST


def mode_waves():
    j = np.arange(COLS)[:, None]
    kx = np.repeat(np.arange(MD) - MD // 2, MD)[None, :]
    ky = np.tile(np.arange(MD), MD)[None, :]
    b = 2 * np.pi * ((j * ky) % COLS) / COLS
    scale = 1.0 / math.sqrt(ROWS * COLS)
    parts = []
    for k, is_sin in WAVES:
        hit = (np.abs(kx) == k).astype(np.float64)
        if is_sin:
            sg = np.sign(kx) * hit
            re, im = -sg * np.sin(b), -sg * np.cos(b)
        else:
            re, im = hit * np.cos(b), -hit * np.sin(b)
        parts.append(np.concatenate([re, im], axis=1) * scale)
    table = np.concatenate(parts, axis=0).astype(np.float32)
    hi = table.astype(jnp.bfloat16)
    lo = (table - hi.astype(np.float32)).astype(jnp.bfloat16)
    return np.concatenate([hi, lo], axis=1)


def wave(k, i):
    return math.cos(2 * math.pi * k * i / ROWS), math.sin(2 * math.pi * k * i / ROWS)


def weighted(terms):
    total = None
    for c, x in terms:
        if abs(c) < 1e-12:
            continue
        t = x if abs(c - 1) < 1e-12 else (-x if abs(c + 1) < 1e-12 else x * np.float32(c))
        total = t if total is None else total + t
    return total


def tree_sum(xs):
    xs = list(xs)
    while len(xs) > 1:
        xs = [xs[i] + xs[i + 1] if i + 1 < len(xs) else xs[i] for i in range(0, len(xs), 2)]
    return xs[0]


def to_waves(x):
    s = [x[i] + x[i + 16] for i in range(16)]
    d = [x[i] - x[i + 16] for i in range(16)]
    dc = [d[0]] + [d[i] - d[16 - i] for i in range(1, 8)]
    ds = [None] + [d[i] + d[16 - i] for i in range(1, 8)] + [d[8]]
    out = {}
    for k in (1, 3):
        out[(k, 0)] = weighted([(wave(k, i)[0], dc[i]) for i in range(8)])
        out[(k, 1)] = weighted([(wave(k, i)[1], ds[i]) for i in range(1, 9)])
    p = [s[i] + s[i + 8] for i in range(8)]
    m = [s[i] - s[i + 8] for i in range(8)]
    mc = [m[0]] + [m[i] - m[8 - i] for i in range(1, 4)]
    ms = [None] + [m[i] + m[8 - i] for i in range(1, 4)] + [m[4]]
    out[(2, 0)] = weighted([(wave(2, i)[0], mc[i]) for i in range(4)])
    out[(2, 1)] = weighted([(wave(2, i)[1], ms[i]) for i in range(1, 5)])
    q = [p[i] - p[i + 4] for i in range(4)]
    r = np.float32(math.sqrt(0.5))
    out[(4, 0)] = q[0] + r * (q[1] - q[3])
    out[(4, 1)] = q[2] + r * (q[1] + q[3])
    out[(0, 0)] = tree_sum([p[i] + p[i + 4] for i in range(4)])
    return [out[w] for w in WAVES]


def to_rows(a):
    a = dict(zip(WAVES, a))
    r = np.float32(math.sqrt(0.5))
    c0, c4, s4 = a[(0, 0)], a[(4, 0)], a[(4, 1)]
    u, v = r * (c4 + s4), r * (s4 - c4)
    e04 = [c0 + c4, c0 + u, c0 + s4, c0 + v, c0 - c4, c0 - u, c0 - s4, c0 - v]
    c2 = [weighted([(wave(2, i)[0], a[(2, 0)])]) for i in range(4)]
    s2 = [None] + [weighted([(wave(2, i)[1], a[(2, 1)])]) for i in range(1, 5)]
    e2 = [c2[0]] + [c2[i] + s2[i] for i in range(1, 4)] + [s2[4]] + [s2[8 - i] - c2[8 - i] for i in range(5, 8)]
    ev = [e04[i] + e2[i] for i in range(8)] + [e04[i] - e2[i] for i in range(8)]
    oc = [weighted([(wave(k, i)[0], a[(k, 0)]) for k in (1, 3)]) for i in range(8)]
    os_ = [None] + [weighted([(wave(k, i)[1], a[(k, 1)]) for k in (1, 3)]) for i in range(1, 9)]
    od = [oc[0]] + [oc[i] + os_[i] for i in range(1, 8)] + [os_[8]] + [os_[16 - i] - oc[16 - i] for i in range(9, 16)]
    return [ev[i] + od[i] for i in range(16)] + [ev[i] - od[i] for i in range(16)]


def split(x):
    hi = x.astype(BF16)
    lo = (x - hi.astype(F32)).astype(BF16)
    return hi, lo


def tall(x):
    hi, lo = split(x)
    return jnp.concatenate([hi, lo, hi], axis=0)


def wide(x):
    hi, lo = split(x)
    return jnp.concatenate([hi, hi, lo], axis=1)


def channel_mix(left, x_ref, width, out_ref, out_width):
    for i in range(0, ROWS, 2):
        right = jnp.concatenate([tall(x_ref[(i + t) * width:(i + t + 1) * width, :]) for t in range(2)], axis=1)
        got = jnp.dot(left, right, preferred_element_type=F32)
        out_ref[i * out_width:(i + 1) * out_width, :] = got[:, :COLS]
        out_ref[(i + 1) * out_width:(i + 2) * out_width, :] = got[:, COLS:]


def each_group(width, fn):
    if LOOP:
        @pl.loop(0, width // 8)
        def _(n):
            fn(pl.multiple_of(n * 8, 8))
    else:
        for g in range(0, width, 8):
            fn(g)


def analyse(x_ref, width, g_ref, waves_ref):
    def group(g):
        got = to_waves([x_ref[pl.ds(i * width + g, 8), :] for i in range(ROWS)])
        for n in range(NWAVE):
            g_ref[pl.ds(g, 8), n * COLS:(n + 1) * COLS] = got[n]
    each_group(width, group)
    hi, lo = split(g_ref[0:width, :])
    both = jnp.dot(jnp.concatenate([hi, lo], axis=0), waves_ref[...], preferred_element_type=F32)
    return (both[:width, :COLS] + both[width:, :COLS]) + (both[:width, COLS:] + both[width:, COLS:])


def synthesise(coef, width, a_ref, waves_ref):
    hi, lo = split(coef)
    left = jnp.concatenate([jnp.concatenate([hi, hi], axis=1), jnp.concatenate([lo, lo], axis=1)], axis=0)
    both = lax.dot_general(left, waves_ref[...], (((1,), (1,)), ((), ())), preferred_element_type=F32)
    a_ref[0:width, :] = both[:width] + both[width:]


def waves_of(a_ref, g):
    return [a_ref[pl.ds(g, 8), n * COLS:(n + 1) * COLS] for n in range(NWAVE)]


def half_swap(x):
    return jnp.concatenate([x[:, 64:], x[:, :64]], axis=1)


def mix_modes(coef, wr_ref, wi_ref, layer, c_ref):
    c_ref[0:W, :] = coef
    c_ref[W:2 * W, :] = half_swap(coef)
    accs = [None] * 4
    for w in range(W):
        t = (wr_ref[layer, w] * jnp.broadcast_to(c_ref[w:w + 1, :], (W, COLS))
             + wi_ref[layer, w] * jnp.broadcast_to(c_ref[W + w:W + w + 1, :], (W, COLS)))
        accs[w % 4] = t if accs[w % 4] is None else accs[w % 4] + t
    return (accs[0] + accs[1]) + (accs[2] + accs[3])


def unmix_modes(grad, wr_ref, wi_ref, layer, r_ref):
    swapped = half_swap(grad)
    for w in range(W):
        t = wr_ref[layer, w] * grad - wi_ref[layer, w] * swapped
        r_ref[w * 8:(w + 1) * 8, :] = (t[0:8] + t[8:16]) + (t[16:24] + t[24:32])
    return tree_sum([r_ref[pl.ds(s, W, stride=8), :] for s in range(8)])


def gelu_parts(x):
    cdf = 0.5 * lax.erf(x * np.float32(math.sqrt(0.5))) + 0.5
    pdf = jnp.exp(-0.5 * (x * x)) * np.float32(1.0 / math.sqrt(2 * math.pi))
    return x * cdf, cdf + x * pdf


def prepare(spectral_ref, wr_ref, wi_ref):
    for layer in range(2):
        for w in range(W):
            re, im = spectral_ref[layer, 0, w], spectral_ref[layer, 1, w]
            wr_ref[layer, w] = jnp.concatenate([re, re], axis=1)
            wi_ref[layer, w] = jnp.concatenate([-im, im], axis=1)


def network_setup(cot_ref, lift_ref, spectral_ref, point_ref, proj_ref, scr):
    prepare(spectral_ref, scr[0], scr[1])
    lift16 = jnp.concatenate([lift_ref[...], jnp.zeros((1, W), F32)], axis=0)
    p1, p2 = point_ref[0], point_ref[1]
    both1 = jnp.dot(lift16, p1, precision=HIGHEST, preferred_element_type=F32)
    both1_t = jnp.transpose(both1)
    lift_t = jnp.transpose(lift16)
    proj8 = jnp.concatenate([proj_ref[...], jnp.zeros((3, W), F32)], axis=0)
    proj_t = jnp.transpose(proj8)
    channel_mix(wide(proj_t), cot_ref, 8, scr[-1], W)
    return {
        "in": wide(both1_t), "out": wide(both1), "point": wide(p2), "point_t": wide(jnp.transpose(p2)),
        "lift": lift16, "lift_t": lift_t,
    }


def network_grad(f_ref, setup, waves_ref, out_ref, scr):
    wr, wi, g, a, c, r, pw, h, d1, pc = scr
    w = setup
    channel_mix(w["in"], f_ref, CIN, pw, W)
    coef = analyse(f_ref, CIN, g, waves_ref)
    coef = jnp.dot(w["lift_t"], coef, precision=HIGHEST, preferred_element_type=F32)
    synthesise(mix_modes(coef, wr, wi, 0, c), W, a, waves_ref)
    def group1(gr):
        rows = to_rows(waves_of(a, gr))
        for i in range(ROWS):
            sl = pl.ds(i * W + gr, 8)
            val, der = gelu_parts(rows[i] + pw[sl, :])
            h[sl, :] = val
            d1[sl, :] = der
    each_group(W, group1)
    channel_mix(w["point_t"], h, W, pw, W)
    coef = analyse(h, W, g, waves_ref)
    synthesise(mix_modes(coef, wr, wi, 1, c), W, a, waves_ref)
    def group2(gr):
        rows = to_rows(waves_of(a, gr))
        for i in range(ROWS):
            sl = pl.ds(i * W + gr, 8)
            _, der = gelu_parts(rows[i] + pw[sl, :])
            h[sl, :] = der * pc[sl, :]
    each_group(W, group2)
    channel_mix(w["point"], h, W, pw, W)
    coef = analyse(h, W, g, waves_ref)
    synthesise(unmix_modes(coef, wr, wi, 1, r), W, a, waves_ref)
    def group3(gr):
        rows = to_rows(waves_of(a, gr))
        for i in range(ROWS):
            sl = pl.ds(i * W + gr, 8)
            h[sl, :] = d1[sl, :] * (rows[i] + pw[sl, :])
    each_group(W, group3)
    channel_mix(w["out"], h, W, pw, CIN)
    coef = analyse(h, W, g, waves_ref)
    coef = unmix_modes(coef, wr, wi, 0, r)
    coef = jnp.dot(w["lift"], coef, precision=HIGHEST, preferred_element_type=F32)
    synthesise(coef, CIN, a, waves_ref)
    def group4(gr):
        rows = to_rows(waves_of(a, gr))
        for i in range(ROWS):
            sl = pl.ds(i * CIN + gr, 8)
            out_ref[sl, :] = rows[i] + pw[sl, :]
    each_group(CIN, group4)


VARS = 5
TILE = 8
MESH = pl.DeviceIdType.MESH
AROUND = sorted(
    ((dx, dy) for dx in range(-2, 3) for dy in range(-2, 3) if (dx, dy) != (0, 0)),
    key=lambda o: (o[1] == 0, abs(o[1]), abs(o[0]), o),
)


def tiles_of(dx, dy):
    if abs(dx) == 2 or abs(dy) == 2:
        return 1
    return VARS if dx == 0 or dy == 0 else 3


START = {}
TILES = 0
for _o in AROUND:
    START[_o] = TILES
    TILES += tiles_of(*_o)


def pieces(dx, dy):
    out = []
    far_col, near_col = 0, 32 if dy == -1 else 0
    blocks = {-1: (1,), 0: (0, 1), 1: (0,)}[dx]
    for ch in range(VARS):
        if dx == 0:
            for rb in blocks:
                out.append(("near", ch, rb, near_col, 32, ch, 32 * rb))
            out.append(("far", ch, 0, far_col, 32, ch, 64))
        elif dy == 0:
            out.append(("near", ch, blocks[0], 0, 64, ch, 0))
            out.append(("far", ch, 0, 0, 32, ch, 64))
        else:
            base = 64 * (ch % 2)
            out.append(("near", ch, blocks[0], near_col, 32, ch // 2, base))
            out.append(("far", ch, 0, far_col, 32, ch // 2, base + 32))
    return out


def far_edge_col(dy):
    return 16 if dy == -2 else 0


def near_lane(col, dy=0):
    return 32 + col + 64 * dy


def far_lane(col, dy=0):
    return 48 + col + 32 * dy


FAR_ROW = {-2: 0, -1: 4, 0: 12, 1: 20, 2: 28}


def lane_ids():
    return lax.broadcasted_iota(jnp.int32, (TILE, COLS), 1)


def row_ids():
    return lax.broadcasted_iota(jnp.int32, (TILE, COLS), 0)


def turned(x, shift, axis=1, period=None):
    shift %= period or x.shape[axis]
    return x if shift == 0 else pltpu.roll(x, shift, axis)


class Lanes:
    def __init__(self):
        self.lane = lane_ids()
        self.row = row_ids()
        self.masks = {}

    def mask(self, first, width):
        key = (first, width)
        if key not in self.masks:
            self.masks[key] = (self.lane >= first) & (self.lane < first + width)
        return self.masks[key]

    def put(self, base, value, first, width):
        return value if base is None else jnp.where(self.mask(first, width), value, base)

    def only(self, value, first, width):
        return jnp.where(self.mask(first, width), value, 0.0)


def pool_maps():
    j = np.arange(COLS)[:, None]
    lane = np.arange(COLS)[None, :]
    gather = np.concatenate(
        [((lane - 32) % 64 == j // 2) * 0.25, ((lane - 48) % 32 == j // 4) * 0.0625], axis=1
    )
    spread = np.concatenate(
        [(j - 32 == lane // 2) * 0.25, (j - 48 == lane // 4) * 0.0625], axis=1
    )
    return np.concatenate([gather, spread], axis=0).astype(jnp.bfloat16)


def mapped(rows, table):
    hi, lo = split(rows)
    both = jnp.dot(jnp.concatenate([hi, lo], axis=0), table, preferred_element_type=F32)
    return both[: rows.shape[0]] + both[rows.shape[0]:]


def send_tiles(lanes, near, far, buf):
    rolled = {}

    def near_at(ch, rb, col, lane):
        key = ("n", ch, rb, (lane - near_lane(col)) % 64)
        if key not in rolled:
            rolled[key] = turned(near[ch][rb], key[3], period=64)
        return rolled[key]

    def far_at(ch, col, lane):
        key = ("f", ch, (lane - far_lane(col)) % 32)
        if key not in rolled:
            rolled[key] = turned(far[ch], key[2], period=32)
        return rolled[key]

    strips = {}
    for dx, dy in AROUND:
        start = START[dx, dy]
        if abs(dy) == 2:
            if ("y", dy) not in strips:
                tile = None
                for ch in range(VARS):
                    tile = lanes.put(tile, far_at(ch, far_edge_col(dy), 16 * ch), 16 * ch, 16)
                strips["y", dy] = tile
            buf[start * TILE:(start + 1) * TILE, :] = strips["y", dy]
        elif abs(dx) == 2:
            if ("x", dx) not in strips:
                tile = None
                for ch in range(4):
                    tile = lanes.put(tile, far_at(ch, 0, 32 * ch), 32 * ch, 32)
                last = far_at(4, 0, 0)
                if dx == -2:
                    tile = turned(tile, 4, axis=0)
                else:
                    last = turned(last, 4, axis=0)
                strips["x", dx] = jnp.where(lanes.mask(0, 32) & (lanes.row >= 4), last, tile)
            buf[start * TILE:(start + 1) * TILE, :] = strips["x", dx]
        else:
            tiles = [None] * tiles_of(dx, dy)
            for kind, ch, rb, col, width, tile, lane in pieces(dx, dy):
                value = near_at(ch, rb, col, lane) if kind == "near" else far_at(ch, col, lane)
                tiles[tile] = lanes.put(tiles[tile], value, lane, width)
            for n, value in enumerate(tiles):
                buf[(start + n) * TILE:(start + n + 1) * TILE, :] = value


def tile_at(buf, o, n=0):
    first = (START[o] + n) * TILE
    return buf[first:first + TILE, :]


def read_windows(lanes, near, far, buf, f_ref):
    blocks = {}
    rows = {}
    for ch in range(VARS):
        blocks[ch, 1], blocks[ch, 2] = near[ch]
        rows[ch, 0] = far[ch]
    for dx in (0, -1, 1):
        for dy in (0, -1, 1):
            if (dx, dy) == (0, 0):
                continue
            for kind, ch, rb, col, width, tile, lane in pieces(dx, dy):
                value = tile_at(buf, (dx, dy), tile)
                if kind == "near":
                    key = (ch, {-1: 0, 0: 1 + rb, 1: 3}[dx])
                    to, table = near_lane(col, dy), blocks
                else:
                    key, to, table = (ch, dx), far_lane(col, dy), rows
                table[key] = lanes.put(table.get(key), turned(value, to - lane), to, width)
    for dx in (-2, 2):
        for dy in (0, -1, 1):
            value = tile_at(buf, (dx, dy))
            low = turned(value, 4, axis=0)
            for ch in range(VARS):
                to, lane = far_lane(0, dy), 32 * ch if ch < 4 else 0
                got = turned(value if ch < 4 else low, to - lane)
                rows[ch, dx] = lanes.put(rows.get((ch, dx)), got, to, 32)
    for dx in range(-2, 3):
        for dy in (-2, 2):
            value = tile_at(buf, (dx, dy))
            if dx == -2:
                value = turned(value, 4, axis=0)
            for ch in range(VARS):
                to = far_lane(far_edge_col(dy), dy)
                rows[ch, dx] = lanes.put(rows[ch, dx], turned(value, to - 16 * ch), to, 16)
    for (ch, k), value in blocks.items():
        f_ref[pl.ds(8 * k * CIN + VARS + ch, TILE, stride=CIN), :] = value
    for (ch, dx), value in rows.items():
        count = 4 if abs(dx) == 2 else TILE
        f_ref[pl.ds(FAR_ROW[dx] * CIN + 2 * VARS + ch, count, stride=CIN), :] = value[:count]


def window_tiles(go):
    near = {(ch, k): go[pl.ds(8 * k * CIN + VARS + ch, TILE, stride=CIN), :] for ch in range(VARS) for k in range(4)}
    far = {}
    for ch in range(VARS):
        for dx in range(-2, 3):
            first = 24 if dx == 2 else FAR_ROW[dx]
            far[ch, dx] = go[pl.ds(first * CIN + 2 * VARS + ch, TILE, stride=CIN), :]
    return near, far


def send_grads(lanes, near, far, buf):
    for dx, dy in AROUND:
        start = START[dx, dy]
        if abs(dy) == 2:
            tile = None
            for ch in range(VARS):
                got = turned(far[ch, dx], 16 * ch - far_lane(far_edge_col(dy), dy))
                tile = lanes.put(tile, got, 16 * ch, 16)
            if abs(dx) == 2:
                tile = turned(tile, 4, axis=0)
                keep = lanes.row >= 4 if dx == -2 else lanes.row < 4
                tile = jnp.where(keep, tile, 0.0)
            buf[start * TILE:(start + 1) * TILE, :] = tile
        elif abs(dx) == 2:
            tile = None
            for ch in range(4):
                tile = lanes.put(tile, turned(far[ch, dx], 32 * ch - far_lane(0, dy)), 32 * ch, 32)
            last = turned(far[4, dx], -far_lane(0, dy))
            if dx == -2:
                last = turned(last, 4, axis=0)
            else:
                tile = turned(tile, 4, axis=0)
            buf[start * TILE:(start + 1) * TILE, :] = jnp.where(lanes.mask(0, 32) & (lanes.row >= 4), last, tile)
        else:
            tiles = [None] * tiles_of(dx, dy)
            for kind, ch, rb, col, width, tile, lane in pieces(dx, dy):
                if kind == "near":
                    value = turned(near[ch, {-1: 0, 0: 1 + rb, 1: 3}[dx]], lane - near_lane(col, dy))
                else:
                    value = turned(far[ch, dx], lane - far_lane(col, dy))
                tiles[tile] = lanes.put(tiles[tile], value, lane, width)
            for n, value in enumerate(tiles):
                buf[(start + n) * TILE:(start + n + 1) * TILE, :] = value


def sum_grads(lanes, near, far, buf):
    n_sum = {(ch, rb): lanes.only(near[ch, 1 + rb], 32, 64) for ch in range(VARS) for rb in range(2)}
    f_sum = {ch: lanes.only(far[ch, 0], 48, 32) for ch in range(VARS)}
    for dx in (-1, 0, 1):
        for dy in (-1, 0, 1):
            if (dx, dy) == (0, 0):
                continue
            for kind, ch, rb, col, width, tile, lane in pieces(dx, dy):
                value = tile_at(buf, (dx, dy), tile)
                if kind == "near":
                    to = near_lane(col)
                    n_sum[ch, rb] += lanes.only(turned(value, to - lane), to, width)
                else:
                    to = far_lane(col)
                    f_sum[ch] += lanes.only(turned(value, to - lane), to, width)
    for dx in (-2, 2):
        value = tree_sum([tile_at(buf, (dx, dy)) for dy in (-1, 0, 1)])
        low = turned(value, 4, axis=0)
        keep = lanes.row >= 4 if dx == -2 else lanes.row < 4
        for ch in range(VARS):
            natural = (ch < 4) == (dx == 2)
            lane = 32 * ch if ch < 4 else 0
            got = turned(value if natural else low, far_lane(0) - lane)
            f_sum[ch] += jnp.where(lanes.mask(48, 32) & keep, got, 0.0)
    for dy in (-2, 2):
        value = tree_sum([tile_at(buf, (dx, dy)) for dx in range(-2, 3)])
        for ch in range(VARS):
            to = far_lane(far_edge_col(dy))
            f_sum[ch] += lanes.only(turned(value, to - 16 * ch), to, 16)
    return (
        jnp.concatenate([n_sum[ch, rb] for ch in range(VARS) for rb in range(2)], axis=0),
        jnp.concatenate([f_sum[ch] for ch in range(VARS)], axis=0),
    )


Y_SIDE = 4
EDGES = (1, -1, 2, -2)
RELAY = {1: 0, -1: VARS, 2: 2 * VARS, -2: 2 * VARS + 1}
PASSED = {-1: 0, 1: 3, -2: 6, 2: 7}


def repack(lanes, main, e, buf, first):
    for dx in (-1, 1):
        tiles = [None] * 3
        for kind, ch, rb, _, width, tile, lane in pieces(dx, -e):
            value = turned(main[ch], lane - (32 * rb if kind == "near" else 64))
            tiles[tile] = lanes.put(tiles[tile], value, lane, width)
        for n, value in enumerate(tiles):
            row = (first + PASSED[dx] + n) * TILE
            buf[row:row + TILE, :] = value
    strip = None
    for ch in range(4):
        strip = lanes.put(strip, turned(main[ch], 32 * ch - 64), 32 * ch, 32)
    last = turned(main[4], -64)
    corner = lanes.mask(0, 32) & (lanes.row >= 4)
    for dx in (-2, 2):
        row = (first + PASSED[dx]) * TILE
        low, high = (turned(strip, 4, axis=0), last) if dx == -2 else (strip, turned(last, 4, axis=0))
        buf[row:row + TILE, :] = jnp.where(corner, high, low)


def kernel(counts, field_hbm, cot_hbm, lift_hbm, spectral_hbm, point_hbm, proj_hbm, waves_hbm, maps_hbm, out_ref,
           field, cot, lift, spectral, point, proj, waves, maps, f, ct, go, pooled, spread_near, spread_far,
           fwd_out, fwd_in, bwd_out, bwd_in, relay_in, relay_out, load_sem, send_sem, recv_sem, to_mid_sem, at_mid_sem,
           from_mid_sem, *scr):
    gx, gy = lax.axis_index("gx"), lax.axis_index("gy")
    n_gx, n_gy = counts
    half_z = n_gx // 2
    n_z = 2 * half_z
    y = lax.rem(gy, Y_SIDE)
    index = {o: n for n, o in enumerate(AROUND)}

    def device(dx, dy, base=None):
        bx, by = base or (gx, gy)
        return (lax.rem(bx + (dx + n_gx), n_gx), lax.rem(by + (dy + n_gy), n_gy))

    def crosses(e):
        return (y + e < 0) | (y + e >= Y_SIDE)

    def middle(place, sign):
        px, py = place
        core, group = lax.rem(px, 2), lax.div(py, Y_SIDE)
        z = lax.rem(group, 2) * half_z + lax.div(px, 2)
        step = sign * (n_z // 4)
        z = lax.rem(z + jnp.where(core == 0, n_z + step, n_z - step), n_z)
        row = lax.div(group, 2) * (2 * Y_SIDE) + lax.div(z, half_z) * Y_SIDE + lax.rem(py, Y_SIDE)
        return (2 * lax.rem(z, half_z) + core, row)

    mine, source = middle((gx, gy), 1), middle((gx, gy), -1)

    barrier = pltpu.get_barrier_semaphore()
    pl.semaphore_signal(barrier, inc=1, device_id=source, device_id_type=MESH)
    for dx, dy in AROUND:
        owner = device(dx, dy)
        if dy != 0:
            via, far_one = middle(owner, 1), crosses(dy)
            owner = tuple(jnp.where(far_one, a, b) for a, b in zip(via, owner))
        pl.semaphore_signal(barrier, inc=1, device_id=owner, device_id_type=MESH)
    loads = [
        pltpu.make_async_copy(src, dst, load_sem.at[n])
        for n, (src, dst) in enumerate([
            (field_hbm, field), (maps_hbm, maps), (cot_hbm, cot), (lift_hbm, lift), (point_hbm, point),
            (proj_hbm, proj), (spectral_hbm, spectral), (waves_hbm, waves)])
    ]
    for copy in loads:
        copy.start()

    def span(o):
        return pl.ds(START[o] * TILE, tiles_of(*o) * TILE)

    def direct(turn, src, dst, o):
        sign = -1 if turn == 0 else 1
        return pltpu.make_async_remote_copy(
            src_ref=src.at[span(o)], dst_ref=dst.at[span(o)], send_sem=send_sem.at[turn, index[o]],
            recv_sem=recv_sem.at[turn, index[o]], device_id=device(sign * o[0], sign * o[1]), device_id_type=MESH)

    def to_middle(e):
        tiles = tiles_of(0, -e)
        return pltpu.make_async_remote_copy(
            src_ref=fwd_out.at[span((0, -e))], dst_ref=relay_in.at[pl.ds(RELAY[e] * TILE, tiles * TILE)],
            send_sem=to_mid_sem.at[EDGES.index(e)], recv_sem=at_mid_sem.at[EDGES.index(e)], device_id=mine,
            device_id_type=MESH)

    def from_middle(e, ex):
        o = (-ex, -e)
        if abs(e) == 2 or ex == 0:
            first, ref = RELAY[e], relay_in
        else:
            first, ref = PASSED[-ex] + (0 if e == 1 else 8), relay_out
        return pltpu.make_async_remote_copy(
            src_ref=ref.at[pl.ds(first * TILE, tiles_of(*o) * TILE)], dst_ref=fwd_in.at[span(o)],
            send_sem=from_mid_sem.at[EDGES.index(e), ex + 2], recv_sem=recv_sem.at[0, index[o]],
            device_id=device(ex, e, source), device_id_type=MESH)

    lanes = Lanes()
    loads[0].wait()
    loads[1].wait()
    half = field[pl.ds(0, 80, stride=2), :] + field[pl.ds(1, 80, stride=2), :]
    pooled[...] = half
    quarter = pooled[pl.ds(0, 40, stride=2), :] + pooled[pl.ds(1, 40, stride=2), :]
    got = mapped(jnp.concatenate([half, quarter], axis=0), maps[0:COLS, :])
    near = [[got[ch * 16 + rb * 8:ch * 16 + rb * 8 + 8, :COLS] for rb in range(2)] for ch in range(VARS)]
    far = [got[80 + ch * 8:80 + ch * 8 + 8, COLS:] for ch in range(VARS)]
    send_tiles(lanes, near, far, fwd_out)
    pl.semaphore_wait(barrier, len(AROUND) + 1)
    for e in EDGES:
        @pl.when(crosses(e))
        def _(e=e):
            to_middle(e).start()
    for o in AROUND:
        if o[1] == 0:
            direct(0, fwd_out, fwd_in, o).start()
    for dy in EDGES:
        @pl.when(jnp.logical_not(crosses(-dy)))
        def _(dy=dy):
            for dx in (0, -1, 1, -2, 2):
                direct(0, fwd_out, fwd_in, (dx, dy)).start()

    for copy in loads[2:]:
        copy.wait()
    f[...] = jnp.zeros_like(f)
    ct[...] = jnp.zeros_like(ct)
    for v in range(VARS):
        f[pl.ds(v, ROWS, stride=CIN), :] = field[v * ROWS:(v + 1) * ROWS, :]
        ct[pl.ds(v, ROWS, stride=8), :] = cot[v * ROWS:(v + 1) * ROWS, :]
    setup = network_setup(ct, lift, spectral, point, proj, scr)
    for e in EDGES:
        @pl.when(crosses(e))
        def _(e=e):
            to_middle(e).wait_recv()
            from_middle(e, 0).start()
            if abs(e) == 1:
                main = [relay_in[(RELAY[e] + ch) * TILE:(RELAY[e] + ch + 1) * TILE, :] for ch in range(VARS)]
                repack(Lanes(), main, e, relay_out, 0 if e == 1 else 8)
            for ex in (-1, 1, -2, 2):
                from_middle(e, ex).start()
    for o in AROUND:
        direct(0, fwd_out, fwd_in, o).wait_recv()
    read_windows(lanes, near, far, fwd_in, f)
    network_grad(f, setup, waves, go, scr)

    near, far = window_tiles(go)
    send_grads(lanes, near, far, bwd_out)
    for o in AROUND:
        direct(1, bwd_out, bwd_in, o).start()
    for o in AROUND:
        direct(1, bwd_out, bwd_in, o).wait_recv()
    n_sum, f_sum = sum_grads(lanes, near, far, bwd_in)
    got = mapped(jnp.concatenate([n_sum, f_sum], axis=0), maps[COLS:, :])
    for k in range(2):
        spread_near[pl.ds(k, 80, stride=2), :] = got[:80, :COLS]
    for k in range(4):
        spread_far[pl.ds(k, 40, stride=4), :] = got[80:, COLS:]
    for v in range(VARS):
        rows = slice(v * ROWS, (v + 1) * ROWS)
        out_ref[rows, :] = go[pl.ds(v, ROWS, stride=CIN), :] + spread_near[rows, :] + spread_far[rows, :]
    for o in AROUND:
        if o[1] == 0:
            direct(0, fwd_out, fwd_in, o).wait_send()
        direct(1, bwd_out, bwd_in, o).wait_send()
    for e in EDGES:
        @pl.when(crosses(e))
        def _(e=e):
            to_middle(e).wait_send()
            for ex in range(-2, 3):
                from_middle(e, ex).wait_send()

        @pl.when(jnp.logical_not(crosses(-e)))
        def _(dy=e):
            for dx in (0, -1, 1, -2, 2):
                direct(0, fwd_out, fwd_in, (dx, dy)).wait_send()


def body(counts, field, cotangent, lift, spectral, pointwise, project):
    vmem = lambda *shape, dtype=F32: pltpu.VMEM(shape, dtype)
    flat = (VARS * ROWS, COLS)
    hbm = pl.BlockSpec(memory_space=pltpu.MemorySpace.HBM)
    call = pl.pallas_call(
        functools.partial(kernel, counts),
        out_shape=pltpu.VMEM(flat, F32),
        in_specs=[hbm] * 8,
        out_specs=pl.BlockSpec(memory_space=pltpu.VMEM),
        scratch_shapes=[
            vmem(*flat), vmem(*flat), vmem(3 * VARS, W), vmem(2, 2, W, W, MD * MD), vmem(2, W, W), vmem(VARS, W),
            vmem(NWAVE * COLS, 2 * COLS, dtype=BF16), vmem(2 * COLS, 2 * COLS, dtype=BF16),
            vmem(ROWS * CIN, COLS), vmem(ROWS * 8, COLS), vmem(ROWS * CIN, COLS),
            vmem(80, COLS), vmem(*flat), vmem(*flat),
            vmem(TILES * TILE, COLS), vmem(TILES * TILE, COLS), vmem(TILES * TILE, COLS), vmem(TILES * TILE, COLS),
            vmem(12 * TILE, COLS), vmem(16 * TILE, COLS),
            pltpu.SemaphoreType.DMA((8,)), pltpu.SemaphoreType.DMA((2, len(AROUND))),
            pltpu.SemaphoreType.DMA((2, len(AROUND))),
            pltpu.SemaphoreType.DMA((4,)), pltpu.SemaphoreType.DMA((4,)), pltpu.SemaphoreType.DMA((4, 5)),
            vmem(2, W, W, COLS), vmem(2, W, W, COLS), vmem(W, NWAVE * COLS), vmem(W, NWAVE * COLS),
            vmem(2 * W, COLS), vmem(W * 8, COLS), vmem(ROWS * W, COLS), vmem(ROWS * W, COLS), vmem(ROWS * W, COLS),
            vmem(ROWS * W, COLS),
        ],
        compiler_params=pltpu.CompilerParams(collective_id=0, has_side_effects=True, vmem_limit_bytes=55300 << 10),
        name="patch_grad",
    )
    out = call(
        field.reshape(flat), cotangent.reshape(flat), lift, spectral.transpose(0, 1, 3, 4, 2), pointwise, project.T,
        jnp.asarray(mode_waves()), jnp.asarray(pool_maps()))
    return out.reshape(field.shape)


def solution(mesh):
    counts = (mesh.shape["gx"], mesh.shape["gy"])
    return jax.shard_map(
        functools.partial(body, counts),
        mesh=mesh,
        in_specs=(P(None, None, "gx", "gy"), P(None, None, "gx", "gy"), P(), P(), P(), P()),
        out_specs=P(None, None, "gx", "gy"),
        check_vma=False,
    )
```

```python
import functools
import math

import jax
import jax.numpy as jnp
import numpy as np
from jax import lax
from jax.experimental import pallas as pl
from jax.experimental.pallas import tpu as pltpu
from jax.sharding import PartitionSpec as P

F32, BF16 = jnp.float32, jnp.bfloat16
LOOP = False
ROWS, COLS, W, CIN, MD = 32, 128, 32, 16, 8
WAVES = [(0, 0), (1, 0), (1, 1), (2, 0), (2, 1), (3, 0), (3, 1), (4, 0), (4, 1)]
NWAVE = len(WAVES)
HIGHEST = lax.Precision.HIGHEST


def mode_waves():
    j = np.arange(COLS)[:, None]
    kx = np.repeat(np.arange(MD) - MD // 2, MD)[None, :]
    ky = np.tile(np.arange(MD), MD)[None, :]
    b = 2 * np.pi * ((j * ky) % COLS) / COLS
    scale = 1.0 / math.sqrt(ROWS * COLS)
    parts = []
    for k, is_sin in WAVES:
        hit = (np.abs(kx) == k).astype(np.float64)
        if is_sin:
            sg = np.sign(kx) * hit
            re, im = -sg * np.sin(b), -sg * np.cos(b)
        else:
            re, im = hit * np.cos(b), -hit * np.sin(b)
        parts.append(np.concatenate([re, im], axis=1) * scale)
    table = np.concatenate(parts, axis=0).astype(np.float32)
    hi = table.astype(jnp.bfloat16)
    lo = (table - hi.astype(np.float32)).astype(jnp.bfloat16)
    return np.concatenate([hi, lo], axis=1)


def wave(k, i):
    return math.cos(2 * math.pi * k * i / ROWS), math.sin(2 * math.pi * k * i / ROWS)


def weighted(terms):
    total = None
    for c, x in terms:
        if abs(c) < 1e-12:
            continue
        t = x if abs(c - 1) < 1e-12 else (-x if abs(c + 1) < 1e-12 else x * np.float32(c))
        total = t if total is None else total + t
    return total


def tree_sum(xs):
    xs = list(xs)
    while len(xs) > 1:
        xs = [xs[i] + xs[i + 1] if i + 1 < len(xs) else xs[i] for i in range(0, len(xs), 2)]
    return xs[0]


def to_waves(x):
    s = [x[i] + x[i + 16] for i in range(16)]
    d = [x[i] - x[i + 16] for i in range(16)]
    dc = [d[0]] + [d[i] - d[16 - i] for i in range(1, 8)]
    ds = [None] + [d[i] + d[16 - i] for i in range(1, 8)] + [d[8]]
    out = {}
    for k in (1, 3):
        out[(k, 0)] = weighted([(wave(k, i)[0], dc[i]) for i in range(8)])
        out[(k, 1)] = weighted([(wave(k, i)[1], ds[i]) for i in range(1, 9)])
    p = [s[i] + s[i + 8] for i in range(8)]
    m = [s[i] - s[i + 8] for i in range(8)]
    mc = [m[0]] + [m[i] - m[8 - i] for i in range(1, 4)]
    ms = [None] + [m[i] + m[8 - i] for i in range(1, 4)] + [m[4]]
    out[(2, 0)] = weighted([(wave(2, i)[0], mc[i]) for i in range(4)])
    out[(2, 1)] = weighted([(wave(2, i)[1], ms[i]) for i in range(1, 5)])
    q = [p[i] - p[i + 4] for i in range(4)]
    r = np.float32(math.sqrt(0.5))
    out[(4, 0)] = q[0] + r * (q[1] - q[3])
    out[(4, 1)] = q[2] + r * (q[1] + q[3])
    out[(0, 0)] = tree_sum([p[i] + p[i + 4] for i in range(4)])
    return [out[w] for w in WAVES]


def to_rows(a):
    a = dict(zip(WAVES, a))
    r = np.float32(math.sqrt(0.5))
    c0, c4, s4 = a[(0, 0)], a[(4, 0)], a[(4, 1)]
    u, v = r * (c4 + s4), r * (s4 - c4)
    e04 = [c0 + c4, c0 + u, c0 + s4, c0 + v, c0 - c4, c0 - u, c0 - s4, c0 - v]
    c2 = [weighted([(wave(2, i)[0], a[(2, 0)])]) for i in range(4)]
    s2 = [None] + [weighted([(wave(2, i)[1], a[(2, 1)])]) for i in range(1, 5)]
    e2 = [c2[0]] + [c2[i] + s2[i] for i in range(1, 4)] + [s2[4]] + [s2[8 - i] - c2[8 - i] for i in range(5, 8)]
    ev = [e04[i] + e2[i] for i in range(8)] + [e04[i] - e2[i] for i in range(8)]
    oc = [weighted([(wave(k, i)[0], a[(k, 0)]) for k in (1, 3)]) for i in range(8)]
    os_ = [None] + [weighted([(wave(k, i)[1], a[(k, 1)]) for k in (1, 3)]) for i in range(1, 9)]
    od = [oc[0]] + [oc[i] + os_[i] for i in range(1, 8)] + [os_[8]] + [os_[16 - i] - oc[16 - i] for i in range(9, 16)]
    return [ev[i] + od[i] for i in range(16)] + [ev[i] - od[i] for i in range(16)]


def split(x):
    hi = x.astype(BF16)
    lo = (x - hi.astype(F32)).astype(BF16)
    return hi, lo


def tall(x):
    hi, lo = split(x)
    return jnp.concatenate([hi, lo, hi], axis=0)


def wide(x):
    hi, lo = split(x)
    return jnp.concatenate([hi, hi, lo], axis=1)


def channel_mix(left, x_ref, width, out_ref, out_width):
    for i in range(0, ROWS, 2):
        right = jnp.concatenate([tall(x_ref[(i + t) * width:(i + t + 1) * width, :]) for t in range(2)], axis=1)
        got = jnp.dot(left, right, preferred_element_type=F32)
        out_ref[i * out_width:(i + 1) * out_width, :] = got[:, :COLS]
        out_ref[(i + 1) * out_width:(i + 2) * out_width, :] = got[:, COLS:]


def each_group(width, fn):
    if LOOP:
        @pl.loop(0, width // 8)
        def _(n):
            fn(pl.multiple_of(n * 8, 8))
    else:
        for g in range(0, width, 8):
            fn(g)


def analyse(x_ref, width, g_ref, waves_ref):
    def group(g):
        got = to_waves([x_ref[pl.ds(i * width + g, 8), :] for i in range(ROWS)])
        for n in range(NWAVE):
            g_ref[pl.ds(g, 8), n * COLS:(n + 1) * COLS] = got[n]
    each_group(width, group)
    hi, lo = split(g_ref[0:width, :])
    both = jnp.dot(jnp.concatenate([hi, lo], axis=0), waves_ref[...], preferred_element_type=F32)
    return (both[:width, :COLS] + both[width:, :COLS]) + (both[:width, COLS:] + both[width:, COLS:])


def synthesise(coef, width, a_ref, waves_ref):
    hi, lo = split(coef)
    left = jnp.concatenate([jnp.concatenate([hi, hi], axis=1), jnp.concatenate([lo, lo], axis=1)], axis=0)
    both = lax.dot_general(left, waves_ref[...], (((1,), (1,)), ((), ())), preferred_element_type=F32)
    a_ref[0:width, :] = both[:width] + both[width:]


def waves_of(a_ref, g):
    return [a_ref[pl.ds(g, 8), n * COLS:(n + 1) * COLS] for n in range(NWAVE)]


def half_swap(x):
    return jnp.concatenate([x[:, 64:], x[:, :64]], axis=1)


def mix_modes(coef, wr_ref, wi_ref, layer, c_ref):
    c_ref[0:W, :] = coef
    c_ref[W:2 * W, :] = half_swap(coef)
    accs = [None] * 4
    for w in range(W):
        t = (wr_ref[layer, w] * jnp.broadcast_to(c_ref[w:w + 1, :], (W, COLS))
             + wi_ref[layer, w] * jnp.broadcast_to(c_ref[W + w:W + w + 1, :], (W, COLS)))
        accs[w % 4] = t if accs[w % 4] is None else accs[w % 4] + t
    return (accs[0] + accs[1]) + (accs[2] + accs[3])


def unmix_modes(grad, wr_ref, wi_ref, layer, r_ref):
    swapped = half_swap(grad)
    for w in range(W):
        t = wr_ref[layer, w] * grad - wi_ref[layer, w] * swapped
        r_ref[w * 8:(w + 1) * 8, :] = (t[0:8] + t[8:16]) + (t[16:24] + t[24:32])
    return tree_sum([r_ref[pl.ds(s, W, stride=8), :] for s in range(8)])


def gelu_parts(x):
    cdf = 0.5 * lax.erf(x * np.float32(math.sqrt(0.5))) + 0.5
    pdf = jnp.exp(-0.5 * (x * x)) * np.float32(1.0 / math.sqrt(2 * math.pi))
    return x * cdf, cdf + x * pdf


def prepare(spectral_ref, wr_ref, wi_ref):
    for layer in range(2):
        for w in range(W):
            re, im = spectral_ref[layer, 0, w], spectral_ref[layer, 1, w]
            wr_ref[layer, w] = jnp.concatenate([re, re], axis=1)
            wi_ref[layer, w] = jnp.concatenate([-im, im], axis=1)


def network_setup(cot_ref, lift_ref, spectral_ref, point_ref, proj_ref, scr):
    prepare(spectral_ref, scr[0], scr[1])
    lift16 = jnp.concatenate([lift_ref[...], jnp.zeros((1, W), F32)], axis=0)
    p1, p2 = point_ref[0], point_ref[1]
    both1 = jnp.dot(lift16, p1, precision=HIGHEST, preferred_element_type=F32)
    both1_t = jnp.transpose(both1)
    lift_t = jnp.transpose(lift16)
    proj8 = jnp.concatenate([proj_ref[...], jnp.zeros((3, W), F32)], axis=0)
    proj_t = jnp.transpose(proj8)
    channel_mix(wide(proj_t), cot_ref, 8, scr[-1], W)
    return {
        "in": wide(both1_t), "out": wide(both1), "point": wide(p2), "point_t": wide(jnp.transpose(p2)),
        "lift": lift16, "lift_t": lift_t,
    }


def network_grad(f_ref, setup, waves_ref, out_ref, scr):
    wr, wi, g, a, c, r, pw, h, d1, pc = scr
    w = setup
    channel_mix(w["in"], f_ref, CIN, pw, W)
    coef = analyse(f_ref, CIN, g, waves_ref)
    coef = jnp.dot(w["lift_t"], coef, precision=HIGHEST, preferred_element_type=F32)
    synthesise(mix_modes(coef, wr, wi, 0, c), W, a, waves_ref)
    def group1(gr):
        rows = to_rows(waves_of(a, gr))
        for i in range(ROWS):
            sl = pl.ds(i * W + gr, 8)
            val, der = gelu_parts(rows[i] + pw[sl, :])
            h[sl, :] = val
            d1[sl, :] = der
    each_group(W, group1)
    channel_mix(w["point_t"], h, W, pw, W)
    coef = analyse(h, W, g, waves_ref)
    synthesise(mix_modes(coef, wr, wi, 1, c), W, a, waves_ref)
    def group2(gr):
        rows = to_rows(waves_of(a, gr))
        for i in range(ROWS):
            sl = pl.ds(i * W + gr, 8)
            _, der = gelu_parts(rows[i] + pw[sl, :])
            h[sl, :] = der * pc[sl, :]
    each_group(W, group2)
    channel_mix(w["point"], h, W, pw, W)
    coef = analyse(h, W, g, waves_ref)
    synthesise(unmix_modes(coef, wr, wi, 1, r), W, a, waves_ref)
    def group3(gr):
        rows = to_rows(waves_of(a, gr))
        for i in range(ROWS):
            sl = pl.ds(i * W + gr, 8)
            h[sl, :] = d1[sl, :] * (rows[i] + pw[sl, :])
    each_group(W, group3)
    channel_mix(w["out"], h, W, pw, CIN)
    coef = analyse(h, W, g, waves_ref)
    coef = unmix_modes(coef, wr, wi, 0, r)
    coef = jnp.dot(w["lift"], coef, precision=HIGHEST, preferred_element_type=F32)
    synthesise(coef, CIN, a, waves_ref)
    def group4(gr):
        rows = to_rows(waves_of(a, gr))
        for i in range(ROWS):
            sl = pl.ds(i * CIN + gr, 8)
            out_ref[sl, :] = rows[i] + pw[sl, :]
    each_group(CIN, group4)


VARS = 5
TILE = 8
MESH = pl.DeviceIdType.MESH
AROUND = sorted(
    ((dx, dy) for dx in range(-2, 3) for dy in range(-2, 3) if (dx, dy) != (0, 0)),
    key=lambda o: (o[1] == 0, abs(o[1]), abs(o[0]), o),
)


ROUND = [o for o in AROUND if o[0] > 0]


def tiles_of(dx, dy):
    if abs(dx) == 2 or abs(dy) == 2:
        return 1
    return VARS if dx == 0 or dy == 0 else 3


START = {}
TILES = 0
for _o in AROUND:
    START[_o] = TILES
    TILES += tiles_of(*_o)


def pieces(dx, dy):
    out = []
    far_col, near_col = 0, 32 if dy == -1 else 0
    blocks = {-1: (1,), 0: (0, 1), 1: (0,)}[dx]
    for ch in range(VARS):
        if dx == 0:
            for rb in blocks:
                out.append(("near", ch, rb, near_col, 32, ch, 32 * rb))
            out.append(("far", ch, 0, far_col, 32, ch, 64))
        elif dy == 0:
            out.append(("near", ch, blocks[0], 0, 64, ch, 0))
            out.append(("far", ch, 0, 0, 32, ch, 64))
        else:
            base = 64 * (ch % 2)
            out.append(("near", ch, blocks[0], near_col, 32, ch // 2, base))
            out.append(("far", ch, 0, far_col, 32, ch // 2, base + 32))
    return out


def far_edge_col(dy):
    return 16 if dy == -2 else 0


def near_lane(col, dy=0):
    return 32 + col + 64 * dy


def far_lane(col, dy=0):
    return 48 + col + 32 * dy


FAR_ROW = {-2: 0, -1: 4, 0: 12, 1: 20, 2: 28}


def lane_ids():
    return lax.broadcasted_iota(jnp.int32, (TILE, COLS), 1)


def row_ids():
    return lax.broadcasted_iota(jnp.int32, (TILE, COLS), 0)


def turned(x, shift, axis=1, period=None):
    shift %= period or x.shape[axis]
    return x if shift == 0 else pltpu.roll(x, shift, axis)


class Lanes:
    def __init__(self):
        self.lane = lane_ids()
        self.row = row_ids()
        self.masks = {}

    def mask(self, first, width):
        key = (first, width)
        if key not in self.masks:
            self.masks[key] = (self.lane >= first) & (self.lane < first + width)
        return self.masks[key]

    def put(self, base, value, first, width):
        return value if base is None else jnp.where(self.mask(first, width), value, base)

    def only(self, value, first, width):
        return jnp.where(self.mask(first, width), value, 0.0)


def pool_maps():
    j = np.arange(COLS)[:, None]
    lane = np.arange(COLS)[None, :]
    gather = np.concatenate(
        [((lane - 32) % 64 == j // 2) * 0.25, ((lane - 48) % 32 == j // 4) * 0.0625], axis=1
    )
    spread = np.concatenate(
        [(j - 32 == lane // 2) * 0.25, (j - 48 == lane // 4) * 0.0625], axis=1
    )
    return np.concatenate([gather, spread], axis=0).astype(jnp.bfloat16)


def mapped(rows, table):
    hi, lo = split(rows)
    both = jnp.dot(jnp.concatenate([hi, lo], axis=0), table, preferred_element_type=F32)
    return both[: rows.shape[0]] + both[rows.shape[0]:]


def send_tiles(lanes, near, far, buf):
    rolled = {}

    def near_at(ch, rb, col, lane):
        key = ("n", ch, rb, (lane - near_lane(col)) % 64)
        if key not in rolled:
            rolled[key] = turned(near[ch][rb], key[3], period=64)
        return rolled[key]

    def far_at(ch, col, lane):
        key = ("f", ch, (lane - far_lane(col)) % 32)
        if key not in rolled:
            rolled[key] = turned(far[ch], key[2], period=32)
        return rolled[key]

    strips = {}
    for dx, dy in AROUND:
        start = START[dx, dy]
        if abs(dy) == 2:
            if ("y", dy) not in strips:
                tile = None
                for ch in range(VARS):
                    tile = lanes.put(tile, far_at(ch, far_edge_col(dy), 16 * ch), 16 * ch, 16)
                strips["y", dy] = tile
            buf[start * TILE:(start + 1) * TILE, :] = strips["y", dy]
        elif abs(dx) == 2:
            if ("x", dx) not in strips:
                tile = None
                for ch in range(4):
                    tile = lanes.put(tile, far_at(ch, 0, 32 * ch), 32 * ch, 32)
                last = far_at(4, 0, 0)
                if dx == -2:
                    tile = turned(tile, 4, axis=0)
                else:
                    last = turned(last, 4, axis=0)
                strips["x", dx] = jnp.where(lanes.mask(0, 32) & (lanes.row >= 4), last, tile)
            buf[start * TILE:(start + 1) * TILE, :] = strips["x", dx]
        else:
            tiles = [None] * tiles_of(dx, dy)
            for kind, ch, rb, col, width, tile, lane in pieces(dx, dy):
                value = near_at(ch, rb, col, lane) if kind == "near" else far_at(ch, col, lane)
                tiles[tile] = lanes.put(tiles[tile], value, lane, width)
            for n, value in enumerate(tiles):
                buf[(start + n) * TILE:(start + n + 1) * TILE, :] = value


def tile_at(buf, o, n=0):
    first = (START[o] + n) * TILE
    return buf[first:first + TILE, :]


def read_windows(lanes, near, far, buf, f_ref):
    blocks = {}
    rows = {}
    for ch in range(VARS):
        blocks[ch, 1], blocks[ch, 2] = near[ch]
        rows[ch, 0] = far[ch]
    for dx in (0, -1, 1):
        for dy in (0, -1, 1):
            if (dx, dy) == (0, 0):
                continue
            for kind, ch, rb, col, width, tile, lane in pieces(dx, dy):
                value = tile_at(buf, (dx, dy), tile)
                if kind == "near":
                    key = (ch, {-1: 0, 0: 1 + rb, 1: 3}[dx])
                    to, table = near_lane(col, dy), blocks
                else:
                    key, to, table = (ch, dx), far_lane(col, dy), rows
                table[key] = lanes.put(table.get(key), turned(value, to - lane), to, width)
    for dx in (-2, 2):
        for dy in (0, -1, 1):
            value = tile_at(buf, (dx, dy))
            low = turned(value, 4, axis=0)
            for ch in range(VARS):
                to, lane = far_lane(0, dy), 32 * ch if ch < 4 else 0
                got = turned(value if ch < 4 else low, to - lane)
                rows[ch, dx] = lanes.put(rows.get((ch, dx)), got, to, 32)
    for dx in range(-2, 3):
        for dy in (-2, 2):
            value = tile_at(buf, (dx, dy))
            if dx == -2:
                value = turned(value, 4, axis=0)
            for ch in range(VARS):
                to = far_lane(far_edge_col(dy), dy)
                rows[ch, dx] = lanes.put(rows[ch, dx], turned(value, to - 16 * ch), to, 16)
    for (ch, k), value in blocks.items():
        f_ref[pl.ds(8 * k * CIN + VARS + ch, TILE, stride=CIN), :] = value
    for (ch, dx), value in rows.items():
        count = 4 if abs(dx) == 2 else TILE
        f_ref[pl.ds(FAR_ROW[dx] * CIN + 2 * VARS + ch, count, stride=CIN), :] = value[:count]


def window_tiles(go):
    near = {(ch, k): go[pl.ds(8 * k * CIN + VARS + ch, TILE, stride=CIN), :] for ch in range(VARS) for k in range(4)}
    far = {}
    for ch in range(VARS):
        for dx in range(-2, 3):
            first = 24 if dx == 2 else FAR_ROW[dx]
            far[ch, dx] = go[pl.ds(first * CIN + 2 * VARS + ch, TILE, stride=CIN), :]
    return near, far


def send_grads(lanes, near, far, buf):
    for dx, dy in AROUND:
        start = START[dx, dy]
        if abs(dy) == 2:
            tile = None
            for ch in range(VARS):
                got = turned(far[ch, dx], 16 * ch - far_lane(far_edge_col(dy), dy))
                tile = lanes.put(tile, got, 16 * ch, 16)
            if abs(dx) == 2:
                tile = turned(tile, 4, axis=0)
                keep = lanes.row >= 4 if dx == -2 else lanes.row < 4
                tile = jnp.where(keep, tile, 0.0)
            buf[start * TILE:(start + 1) * TILE, :] = tile
        elif abs(dx) == 2:
            tile = None
            for ch in range(4):
                tile = lanes.put(tile, turned(far[ch, dx], 32 * ch - far_lane(0, dy)), 32 * ch, 32)
            last = turned(far[4, dx], -far_lane(0, dy))
            if dx == -2:
                last = turned(last, 4, axis=0)
            else:
                tile = turned(tile, 4, axis=0)
            buf[start * TILE:(start + 1) * TILE, :] = jnp.where(lanes.mask(0, 32) & (lanes.row >= 4), last, tile)
        else:
            tiles = [None] * tiles_of(dx, dy)
            for kind, ch, rb, col, width, tile, lane in pieces(dx, dy):
                if kind == "near":
                    value = turned(near[ch, {-1: 0, 0: 1 + rb, 1: 3}[dx]], lane - near_lane(col, dy))
                else:
                    value = turned(far[ch, dx], lane - far_lane(col, dy))
                tiles[tile] = lanes.put(tiles[tile], value, lane, width)
            for n, value in enumerate(tiles):
                buf[(start + n) * TILE:(start + n + 1) * TILE, :] = value


def sum_grads(lanes, near, far, buf):
    n_sum = {(ch, rb): lanes.only(near[ch, 1 + rb], 32, 64) for ch in range(VARS) for rb in range(2)}
    f_sum = {ch: lanes.only(far[ch, 0], 48, 32) for ch in range(VARS)}
    for dx in (-1, 0, 1):
        for dy in (-1, 0, 1):
            if (dx, dy) == (0, 0):
                continue
            for kind, ch, rb, col, width, tile, lane in pieces(dx, dy):
                value = tile_at(buf, (dx, dy), tile)
                if kind == "near":
                    to = near_lane(col)
                    n_sum[ch, rb] += lanes.only(turned(value, to - lane), to, width)
                else:
                    to = far_lane(col)
                    f_sum[ch] += lanes.only(turned(value, to - lane), to, width)
    for dx in (-2, 2):
        value = tree_sum([tile_at(buf, (dx, dy)) for dy in (-1, 0, 1)])
        low = turned(value, 4, axis=0)
        keep = lanes.row >= 4 if dx == -2 else lanes.row < 4
        for ch in range(VARS):
            natural = (ch < 4) == (dx == 2)
            lane = 32 * ch if ch < 4 else 0
            got = turned(value if natural else low, far_lane(0) - lane)
            f_sum[ch] += jnp.where(lanes.mask(48, 32) & keep, got, 0.0)
    for dy in (-2, 2):
        value = tree_sum([tile_at(buf, (dx, dy)) for dx in range(-2, 3)])
        for ch in range(VARS):
            to = far_lane(far_edge_col(dy))
            f_sum[ch] += lanes.only(turned(value, to - 16 * ch), to, 16)
    return (
        jnp.concatenate([n_sum[ch, rb] for ch in range(VARS) for rb in range(2)], axis=0),
        jnp.concatenate([f_sum[ch] for ch in range(VARS)], axis=0),
    )


Y_SIDE = 4
EDGES = (1, -1, 2, -2)
RELAY = {1: 0, -1: VARS, 2: 2 * VARS, -2: 2 * VARS + 1}
PASSED = {-1: 0, 1: 3, -2: 6, 2: 7}


def repack(lanes, main, e, buf, first):
    for dx in (-1, 1):
        tiles = [None] * 3
        for kind, ch, rb, _, width, tile, lane in pieces(dx, -e):
            value = turned(main[ch], lane - (32 * rb if kind == "near" else 64))
            tiles[tile] = lanes.put(tiles[tile], value, lane, width)
        for n, value in enumerate(tiles):
            row = (first + PASSED[dx] + n) * TILE
            buf[row:row + TILE, :] = value
    strip = None
    for ch in range(4):
        strip = lanes.put(strip, turned(main[ch], 32 * ch - 64), 32 * ch, 32)
    last = turned(main[4], -64)
    corner = lanes.mask(0, 32) & (lanes.row >= 4)
    for dx in (-2, 2):
        row = (first + PASSED[dx]) * TILE
        low, high = (turned(strip, 4, axis=0), last) if dx == -2 else (strip, turned(last, 4, axis=0))
        buf[row:row + TILE, :] = jnp.where(corner, high, low)


def kernel(counts, field_hbm, cot_hbm, lift_hbm, spectral_hbm, point_hbm, proj_hbm, waves_hbm, maps_hbm, out_ref,
           field, cot, lift, spectral, point, proj, waves, maps, f, ct, go, pooled, spread_near, spread_far,
           fwd_out, fwd_in, bwd_out, bwd_in, relay_in, relay_out, load_sem, send_sem, recv_sem, to_mid_sem, at_mid_sem,
           from_mid_sem, stage_in, stage_sem, ready_sem, *scr):
    gx, gy = lax.axis_index("gx"), lax.axis_index("gy")
    n_gx, n_gy = counts
    loads = [
        pltpu.make_async_copy(src, dst, load_sem.at[n])
        for n, (src, dst) in enumerate([
            (field_hbm, field), (maps_hbm, maps), (cot_hbm, cot), (lift_hbm, lift), (point_hbm, point),
            (proj_hbm, proj), (spectral_hbm, spectral), (waves_hbm, waves)])
    ]
    for copy in loads:
        copy.start()
    half_z = n_gx // 2
    n_z = 2 * half_z
    y = lax.rem(gy, Y_SIDE)
    index = {o: n for n, o in enumerate(AROUND)}

    def device(dx, dy, base=None):
        bx, by = base or (gx, gy)
        return (lax.rem(bx + (dx + n_gx), n_gx), lax.rem(by + (dy + n_gy), n_gy))

    def crosses(e):
        return (y + e < 0) | (y + e >= Y_SIDE)

    def middle(place, sign):
        px, py = place
        core, group = lax.rem(px, 2), lax.div(py, Y_SIDE)
        z = lax.rem(group, 2) * half_z + lax.div(px, 2)
        step = sign * (n_z // 4)
        z = lax.rem(z + jnp.where(core == 0, n_z + step, n_z - step), n_z)
        row = lax.div(group, 2) * (2 * Y_SIDE) + lax.div(z, half_z) * Y_SIDE + lax.rem(py, Y_SIDE)
        return (2 * lax.rem(z, half_z) + core, row)

    mine, source = middle((gx, gy), 1), middle((gx, gy), -1)

    hop = 2 * ((half_z - 1) // 2)
    staged = lax.div(gx, 2) == hop // 2
    stage_source = gx - hop
    edge = gx < 2

    def stage_of(px):
        return px + hop

    def goes_round(o, px):
        round_end = px - o[0] < 0
        return round_end if o[1] == 0 else round_end & jnp.logical_not(crosses(-o[1]))

    def count(flag):
        return jnp.where(flag, 1, 0)

    quarter_z, half_here = n_z // 4, lax.rem(lax.div(gy, Y_SIDE), 2)
    early_here = half_here * half_z + lax.div(gx, 2) < quarter_z
    early, tell_later = {}, {}
    for dx in range(-2, 3):
        ox = lax.rem(gx + (dx + n_gx), n_gx)
        oz = (1 - half_here) * half_z + lax.div(ox, 2)
        oz += jnp.where(lax.rem(ox, 2) == 0, n_z + quarter_z, n_z - quarter_z)
        early[dx] = lax.rem(oz, n_z) < quarter_z

    barrier = pltpu.get_barrier_semaphore()
    by_middle = half_here == 0
    relays = lax.rem(lax.div(source[1], Y_SIDE), 2) == 0
    pl.when(relays)(functools.partial(
        pl.semaphore_signal, barrier, inc=1, device_id=source, device_id_type=MESH))
    for dx, dy in AROUND:
        owner = sender = device(dx, dy)
        if dx != 0:
            round_end = gx + dx >= n_gx
            sender = (jnp.where(round_end, stage_of(owner[0]), owner[0]), owner[1])
        told = functools.partial(pl.semaphore_signal, barrier, inc=1, device_id_type=MESH)
        if dy == 0:
            told(device_id=sender)
            continue
        via, far_one = middle(owner, 1), crosses(dy)
        across = tuple(jnp.where(half_here == 1, a, b) for a, b in zip(via, owner))
        sender = tuple(jnp.where(far_one, a, b) for a, b in zip(across, sender))
        tell_later[dx, dy] = (far_one & (half_here == 1) & early[dx], via)
        pl.when(jnp.logical_not(tell_later[dx, dy][0]))(functools.partial(told, device_id=sender))

    @pl.when(early_here & relays)
    def _():
        for e in EDGES:
            @pl.when(crosses(e))
            def _(e=e):
                for ex in range(-2, 3):
                    pl.semaphore_signal(barrier, inc=1, device_id=device(ex, e, source), device_id_type=MESH)

    @pl.when(staged)
    def _():
        pl.semaphore_signal(barrier, inc=1, device_id=(stage_source, gy), device_id_type=MESH)

    expected = len(AROUND) + count(by_middle) + count(edge)
    for o in AROUND:
        if o[0] > 0:
            expected += count(staged & goes_round(o, stage_source)) - count(goes_round(o, gx))
    for later, _ in tell_later.values():
        expected += count(later)
    for e in EDGES:
        expected += 5 * (count(crosses(e) & relays & jnp.logical_not(early_here)) - count(crosses(e) & by_middle))
    def span(o):
        return pl.ds(START[o] * TILE, tiles_of(*o) * TILE)

    def direct(turn, src, dst, o):
        sign = -1 if turn == 0 else 1
        return pltpu.make_async_remote_copy(
            src_ref=src.at[span(o)], dst_ref=dst.at[span(o)], send_sem=send_sem.at[turn, index[o]],
            recv_sem=recv_sem.at[turn, index[o]], device_id=device(sign * o[0], sign * o[1]), device_id_type=MESH)

    def to_middle(e):
        tiles = tiles_of(0, -e)
        return pltpu.make_async_remote_copy(
            src_ref=fwd_out.at[span((0, -e))], dst_ref=relay_in.at[pl.ds(RELAY[e] * TILE, tiles * TILE)],
            send_sem=to_mid_sem.at[EDGES.index(e)], recv_sem=at_mid_sem.at[EDGES.index(e)], device_id=mine,
            device_id_type=MESH)

    def from_middle(e, ex):
        o = (-ex, -e)
        if abs(e) == 2 or ex == 0:
            first, ref = RELAY[e], relay_in
        else:
            first, ref = PASSED[-ex] + (0 if e == 1 else 8), relay_out
        return pltpu.make_async_remote_copy(
            src_ref=ref.at[pl.ds(first * TILE, tiles_of(*o) * TILE)], dst_ref=fwd_in.at[span(o)],
            send_sem=from_mid_sem.at[EDGES.index(e), ex + 2], recv_sem=recv_sem.at[0, index[o]],
            device_id=device(ex, e, source), device_id_type=MESH)

    def to_stage(o):
        return pltpu.make_async_remote_copy(
            src_ref=fwd_out.at[span(o)], dst_ref=stage_in.at[span(o)], send_sem=stage_sem.at[0, index[o]],
            recv_sem=stage_sem.at[1, index[o]], device_id=(stage_of(gx), gy), device_id_type=MESH)

    def from_stage(o):
        return pltpu.make_async_remote_copy(
            src_ref=stage_in.at[span(o)], dst_ref=fwd_in.at[span(o)], send_sem=stage_sem.at[2, index[o]],
            recv_sem=recv_sem.at[0, index[o]], device_id=device(-o[0], -o[1], (stage_source, gy)), device_id_type=MESH)

    lanes = Lanes()
    loads[0].wait()
    loads[1].wait()
    half = field[pl.ds(0, 80, stride=2), :] + field[pl.ds(1, 80, stride=2), :]
    pooled[...] = half
    quarter = pooled[pl.ds(0, 40, stride=2), :] + pooled[pl.ds(1, 40, stride=2), :]
    got = mapped(jnp.concatenate([half, quarter], axis=0), maps[0:COLS, :])
    near = [[got[ch * 16 + rb * 8:ch * 16 + rb * 8 + 8, :COLS] for rb in range(2)] for ch in range(VARS)]
    far = [got[80 + ch * 8:80 + ch * 8 + 8, COLS:] for ch in range(VARS)]
    send_tiles(lanes, near, far, fwd_out)
    pl.semaphore_wait(barrier, expected)
    for o, (later, via) in tell_later.items():
        pl.when(later)(functools.partial(
            pl.semaphore_signal, ready_sem.at[index[o]], inc=1, device_id=via, device_id_type=MESH))

    def pass_on(e, ex):
        pl.when(early_here)(functools.partial(pl.semaphore_wait, ready_sem.at[index[-ex, -e]], 1))
        from_middle(e, ex).start()

    for e in EDGES:
        @pl.when(crosses(e) & by_middle)
        def _(e=e):
            to_middle(e).start()
    for o in ROUND:
        @pl.when(goes_round(o, gx))
        def _(o=o):
            to_stage(o).start()

    def goes_directly(o):
        target = gx - o[0]
        inside = target >= 0
        if o[1] == 0:
            return inside
        across = crosses(-o[1])
        return (across & jnp.logical_not(by_middle)) | (inside & jnp.logical_not(across))

    for o in AROUND:
        @pl.when(goes_directly(o))
        def _(o=o):
            direct(0, fwd_out, fwd_in, o).start()

    for copy in loads[2:]:
        copy.wait()
    f[...] = jnp.zeros_like(f)
    ct[...] = jnp.zeros_like(ct)
    for v in range(VARS):
        f[pl.ds(v, ROWS, stride=CIN), :] = field[v * ROWS:(v + 1) * ROWS, :]
        ct[pl.ds(v, ROWS, stride=8), :] = cot[v * ROWS:(v + 1) * ROWS, :]
    setup = network_setup(ct, lift, spectral, point, proj, scr)

    @pl.when(staged)
    def _():
        for o in ROUND:
            @pl.when(goes_round(o, stage_source))
            def _(o=o):
                to_stage(o).wait_recv()
                from_stage(o).start()

    for e in EDGES:
        @pl.when(crosses(e) & relays)
        def _(e=e):
            to_middle(e).wait_recv()
            pass_on(e, 0)
            if abs(e) == 1:
                main = [relay_in[(RELAY[e] + ch) * TILE:(RELAY[e] + ch + 1) * TILE, :] for ch in range(VARS)]
                repack(Lanes(), main, e, relay_out, 0 if e == 1 else 8)
            for ex in (-1, 1, -2, 2):
                pass_on(e, ex)

    for o in AROUND:
        direct(0, fwd_out, fwd_in, o).wait_recv()
    read_windows(lanes, near, far, fwd_in, f)
    network_grad(f, setup, waves, go, scr)

    near, far = window_tiles(go)
    send_grads(lanes, near, far, bwd_out)
    for o in AROUND:
        direct(1, bwd_out, bwd_in, o).start()
    for o in AROUND:
        direct(1, bwd_out, bwd_in, o).wait_recv()
    n_sum, f_sum = sum_grads(lanes, near, far, bwd_in)
    got = mapped(jnp.concatenate([n_sum, f_sum], axis=0), maps[COLS:, :])
    for k in range(2):
        spread_near[pl.ds(k, 80, stride=2), :] = got[:80, :COLS]
    for k in range(4):
        spread_far[pl.ds(k, 40, stride=4), :] = got[80:, COLS:]
    for v in range(VARS):
        rows = slice(v * ROWS, (v + 1) * ROWS)
        out_ref[rows, :] = go[pl.ds(v, ROWS, stride=CIN), :] + spread_near[rows, :] + spread_far[rows, :]
    for o in AROUND:
        direct(1, bwd_out, bwd_in, o).wait_send()

        @pl.when(goes_directly(o))
        def _(o=o):
            direct(0, fwd_out, fwd_in, o).wait_send()
    for e in EDGES:
        pl.when(crosses(e) & by_middle)(to_middle(e).wait_send)

        @pl.when(crosses(e) & relays)
        def _(e=e):
            for ex in range(-2, 3):
                from_middle(e, ex).wait_send()
    for o in ROUND:
        @pl.when(goes_round(o, gx))
        def _(o=o):
            to_stage(o).wait_send()

        @pl.when(staged & goes_round(o, stage_source))
        def _(o=o):
            from_stage(o).wait_send()


def body(counts, field, cotangent, lift, spectral, pointwise, project):
    vmem = lambda *shape, dtype=F32: pltpu.VMEM(shape, dtype)
    flat = (VARS * ROWS, COLS)
    hbm = pl.BlockSpec(memory_space=pltpu.MemorySpace.HBM)
    call = pl.pallas_call(
        functools.partial(kernel, counts),
        out_shape=pltpu.VMEM(flat, F32),
        in_specs=[hbm] * 8,
        out_specs=pl.BlockSpec(memory_space=pltpu.VMEM),
        scratch_shapes=[
            vmem(*flat), vmem(*flat), vmem(3 * VARS, W), vmem(2, 2, W, W, MD * MD), vmem(2, W, W), vmem(VARS, W),
            vmem(NWAVE * COLS, 2 * COLS, dtype=BF16), vmem(2 * COLS, 2 * COLS, dtype=BF16),
            vmem(ROWS * CIN, COLS), vmem(ROWS * 8, COLS), vmem(ROWS * CIN, COLS),
            vmem(80, COLS), vmem(*flat), vmem(*flat),
            vmem(TILES * TILE, COLS), vmem(TILES * TILE, COLS), vmem(TILES * TILE, COLS), vmem(TILES * TILE, COLS),
            vmem(12 * TILE, COLS), vmem(16 * TILE, COLS),
            pltpu.SemaphoreType.DMA((8,)), pltpu.SemaphoreType.DMA((2, len(AROUND))),
            pltpu.SemaphoreType.DMA((2, len(AROUND))),
            pltpu.SemaphoreType.DMA((4,)), pltpu.SemaphoreType.DMA((4,)), pltpu.SemaphoreType.DMA((4, 5)),
            vmem(TILES * TILE, COLS), pltpu.SemaphoreType.DMA((3, len(AROUND))),
            pltpu.SemaphoreType.REGULAR((len(AROUND),)),
            vmem(2, W, W, COLS), vmem(2, W, W, COLS), vmem(W, NWAVE * COLS), vmem(W, NWAVE * COLS),
            vmem(2 * W, COLS), vmem(W * 8, COLS), vmem(ROWS * W, COLS), vmem(ROWS * W, COLS), vmem(ROWS * W, COLS),
            vmem(ROWS * W, COLS),
        ],
        compiler_params=pltpu.CompilerParams(collective_id=0, has_side_effects=True, vmem_limit_bytes=55300 << 10),
        name="patch_grad",
    )
    out = call(
        field.reshape(flat), cotangent.reshape(flat), lift, spectral.transpose(0, 1, 3, 4, 2), pointwise, project.T,
        jnp.asarray(mode_waves()), jnp.asarray(pool_maps()))
    return out.reshape(field.shape)


def solution(mesh):
    counts = (mesh.shape["gx"], mesh.shape["gy"])
    return jax.shard_map(
        functools.partial(body, counts),
        mesh=mesh,
        in_specs=(P(None, None, "gx", "gy"), P(None, None, "gx", "gy"), P(), P(), P(), P()),
        out_specs=P(None, None, "gx", "gy"),
        check_vma=False,
    )
```

```python
import functools
import math

import jax
import jax.numpy as jnp
import numpy as np
from jax import lax
from jax.experimental import pallas as pl
from jax.experimental.pallas import tpu as pltpu
from jax.sharding import PartitionSpec as P

F32, BF16 = jnp.float32, jnp.bfloat16
LOOP = False
ROWS, COLS, W, CIN, MD = 32, 128, 32, 16, 8
WAVES = [(0, 0), (1, 0), (1, 1), (2, 0), (2, 1), (3, 0), (3, 1), (4, 0), (4, 1)]
NWAVE = len(WAVES)
HIGHEST = lax.Precision.HIGHEST


def mode_waves():
    j = np.arange(COLS)[:, None]
    kx = np.repeat(np.arange(MD) - MD // 2, MD)[None, :]
    ky = np.tile(np.arange(MD), MD)[None, :]
    b = 2 * np.pi * ((j * ky) % COLS) / COLS
    scale = 1.0 / math.sqrt(ROWS * COLS)
    parts = []
    for k, is_sin in WAVES:
        hit = (np.abs(kx) == k).astype(np.float64)
        if is_sin:
            sg = np.sign(kx) * hit
            re, im = -sg * np.sin(b), -sg * np.cos(b)
        else:
            re, im = hit * np.cos(b), -hit * np.sin(b)
        parts.append(np.concatenate([re, im], axis=1) * scale)
    table = np.concatenate(parts, axis=0).astype(np.float32)
    hi = table.astype(jnp.bfloat16)
    lo = (table - hi.astype(np.float32)).astype(jnp.bfloat16)
    return np.concatenate([hi, lo], axis=1)


def wave(k, i):
    return math.cos(2 * math.pi * k * i / ROWS), math.sin(2 * math.pi * k * i / ROWS)


def weighted(terms):
    total = None
    for c, x in terms:
        if abs(c) < 1e-12:
            continue
        t = x if abs(c - 1) < 1e-12 else (-x if abs(c + 1) < 1e-12 else x * np.float32(c))
        total = t if total is None else total + t
    return total


def tree_sum(xs):
    xs = list(xs)
    while len(xs) > 1:
        xs = [xs[i] + xs[i + 1] if i + 1 < len(xs) else xs[i] for i in range(0, len(xs), 2)]
    return xs[0]


def to_waves(x):
    s = [x[i] + x[i + 16] for i in range(16)]
    d = [x[i] - x[i + 16] for i in range(16)]
    dc = [d[0]] + [d[i] - d[16 - i] for i in range(1, 8)]
    ds = [None] + [d[i] + d[16 - i] for i in range(1, 8)] + [d[8]]
    out = {}
    for k in (1, 3):
        out[(k, 0)] = weighted([(wave(k, i)[0], dc[i]) for i in range(8)])
        out[(k, 1)] = weighted([(wave(k, i)[1], ds[i]) for i in range(1, 9)])
    p = [s[i] + s[i + 8] for i in range(8)]
    m = [s[i] - s[i + 8] for i in range(8)]
    mc = [m[0]] + [m[i] - m[8 - i] for i in range(1, 4)]
    ms = [None] + [m[i] + m[8 - i] for i in range(1, 4)] + [m[4]]
    out[(2, 0)] = weighted([(wave(2, i)[0], mc[i]) for i in range(4)])
    out[(2, 1)] = weighted([(wave(2, i)[1], ms[i]) for i in range(1, 5)])
    q = [p[i] - p[i + 4] for i in range(4)]
    r = np.float32(math.sqrt(0.5))
    out[(4, 0)] = q[0] + r * (q[1] - q[3])
    out[(4, 1)] = q[2] + r * (q[1] + q[3])
    out[(0, 0)] = tree_sum([p[i] + p[i + 4] for i in range(4)])
    return [out[w] for w in WAVES]


def to_rows(a):
    a = dict(zip(WAVES, a))
    r = np.float32(math.sqrt(0.5))
    c0, c4, s4 = a[(0, 0)], a[(4, 0)], a[(4, 1)]
    u, v = r * (c4 + s4), r * (s4 - c4)
    e04 = [c0 + c4, c0 + u, c0 + s4, c0 + v, c0 - c4, c0 - u, c0 - s4, c0 - v]
    c2 = [weighted([(wave(2, i)[0], a[(2, 0)])]) for i in range(4)]
    s2 = [None] + [weighted([(wave(2, i)[1], a[(2, 1)])]) for i in range(1, 5)]
    e2 = [c2[0]] + [c2[i] + s2[i] for i in range(1, 4)] + [s2[4]] + [s2[8 - i] - c2[8 - i] for i in range(5, 8)]
    ev = [e04[i] + e2[i] for i in range(8)] + [e04[i] - e2[i] for i in range(8)]
    oc = [weighted([(wave(k, i)[0], a[(k, 0)]) for k in (1, 3)]) for i in range(8)]
    os_ = [None] + [weighted([(wave(k, i)[1], a[(k, 1)]) for k in (1, 3)]) for i in range(1, 9)]
    od = [oc[0]] + [oc[i] + os_[i] for i in range(1, 8)] + [os_[8]] + [os_[16 - i] - oc[16 - i] for i in range(9, 16)]
    return [ev[i] + od[i] for i in range(16)] + [ev[i] - od[i] for i in range(16)]


def split(x):
    hi = x.astype(BF16)
    lo = (x - hi.astype(F32)).astype(BF16)
    return hi, lo


def tall(x):
    hi, lo = split(x)
    return jnp.concatenate([hi, lo, hi], axis=0)


def wide(x):
    hi, lo = split(x)
    return jnp.concatenate([hi, hi, lo], axis=1)


def channel_mix(left, x_ref, width, out_ref, out_width):
    for i in range(0, ROWS, 2):
        right = jnp.concatenate([tall(x_ref[(i + t) * width:(i + t + 1) * width, :]) for t in range(2)], axis=1)
        got = jnp.dot(left, right, preferred_element_type=F32)
        out_ref[i * out_width:(i + 1) * out_width, :] = got[:, :COLS]
        out_ref[(i + 1) * out_width:(i + 2) * out_width, :] = got[:, COLS:]


def each_group(width, fn):
    if LOOP:
        @pl.loop(0, width // 8)
        def _(n):
            fn(pl.multiple_of(n * 8, 8))
    else:
        for g in range(0, width, 8):
            fn(g)


def analyse(x_ref, width, g_ref, waves_ref):
    def group(g):
        got = to_waves([x_ref[pl.ds(i * width + g, 8), :] for i in range(ROWS)])
        for n in range(NWAVE):
            g_ref[pl.ds(g, 8), n * COLS:(n + 1) * COLS] = got[n]
    each_group(width, group)
    hi, lo = split(g_ref[0:width, :])
    both = jnp.dot(jnp.concatenate([hi, lo], axis=0), waves_ref[...], preferred_element_type=F32)
    return (both[:width, :COLS] + both[width:, :COLS]) + (both[:width, COLS:] + both[width:, COLS:])


def synthesise(coef, width, a_ref, waves_ref):
    hi, lo = split(coef)
    left = jnp.concatenate([jnp.concatenate([hi, hi], axis=1), jnp.concatenate([lo, lo], axis=1)], axis=0)
    both = lax.dot_general(left, waves_ref[...], (((1,), (1,)), ((), ())), preferred_element_type=F32)
    a_ref[0:width, :] = both[:width] + both[width:]


def waves_of(a_ref, g):
    return [a_ref[pl.ds(g, 8), n * COLS:(n + 1) * COLS] for n in range(NWAVE)]


def half_swap(x):
    return jnp.concatenate([x[:, 64:], x[:, :64]], axis=1)


def mix_modes(coef, wr_ref, wi_ref, layer, c_ref):
    c_ref[0:W, :] = coef
    c_ref[W:2 * W, :] = half_swap(coef)
    accs = [None] * 4
    for w in range(W):
        t = (wr_ref[layer, w] * jnp.broadcast_to(c_ref[w:w + 1, :], (W, COLS))
             + wi_ref[layer, w] * jnp.broadcast_to(c_ref[W + w:W + w + 1, :], (W, COLS)))
        accs[w % 4] = t if accs[w % 4] is None else accs[w % 4] + t
    return (accs[0] + accs[1]) + (accs[2] + accs[3])


def unmix_modes(grad, wr_ref, wi_ref, layer, r_ref):
    swapped = half_swap(grad)
    for w in range(W):
        t = wr_ref[layer, w] * grad - wi_ref[layer, w] * swapped
        r_ref[w * 8:(w + 1) * 8, :] = (t[0:8] + t[8:16]) + (t[16:24] + t[24:32])
    return tree_sum([r_ref[pl.ds(s, W, stride=8), :] for s in range(8)])


def gelu_parts(x):
    cdf = 0.5 * lax.erf(x * np.float32(math.sqrt(0.5))) + 0.5
    pdf = jnp.exp(-0.5 * (x * x)) * np.float32(1.0 / math.sqrt(2 * math.pi))
    return x * cdf, cdf + x * pdf


def prepare(spectral_ref, wr_ref, wi_ref):
    for layer in range(2):
        for w in range(W):
            re, im = spectral_ref[layer, 0, w], spectral_ref[layer, 1, w]
            wr_ref[layer, w] = jnp.concatenate([re, re], axis=1)
            wi_ref[layer, w] = jnp.concatenate([-im, im], axis=1)


def network_setup(cot_ref, lift_ref, spectral_ref, point_ref, proj_ref, scr):
    prepare(spectral_ref, scr[0], scr[1])
    lift16 = jnp.concatenate([lift_ref[...], jnp.zeros((1, W), F32)], axis=0)
    p1, p2 = point_ref[0], point_ref[1]
    both1 = jnp.dot(lift16, p1, precision=HIGHEST, preferred_element_type=F32)
    both1_t = jnp.transpose(both1)
    lift_t = jnp.transpose(lift16)
    proj8 = jnp.concatenate([proj_ref[...], jnp.zeros((3, W), F32)], axis=0)
    proj_t = jnp.transpose(proj8)
    channel_mix(wide(proj_t), cot_ref, 8, scr[-1], W)
    return {
        "in": wide(both1_t), "out": wide(both1), "point": wide(p2), "point_t": wide(jnp.transpose(p2)),
        "lift": wide(lift16), "lift_t": wide(lift_t),
    }


def network_grad(f_ref, setup, waves_ref, out_ref, scr):
    wr, wi, g, a, c, r, pw, h, d1, pc = scr
    w = setup
    channel_mix(w["in"], f_ref, CIN, pw, W)
    coef = analyse(f_ref, CIN, g, waves_ref)
    coef = jnp.dot(w["lift_t"], tall(coef), preferred_element_type=F32)
    synthesise(mix_modes(coef, wr, wi, 0, c), W, a, waves_ref)
    def group1(gr):
        rows = to_rows(waves_of(a, gr))
        for i in range(ROWS):
            sl = pl.ds(i * W + gr, 8)
            val, der = gelu_parts(rows[i] + pw[sl, :])
            h[sl, :] = val
            d1[sl, :] = der
    each_group(W, group1)
    channel_mix(w["point_t"], h, W, pw, W)
    coef = analyse(h, W, g, waves_ref)
    synthesise(mix_modes(coef, wr, wi, 1, c), W, a, waves_ref)
    def group2(gr):
        rows = to_rows(waves_of(a, gr))
        for i in range(ROWS):
            sl = pl.ds(i * W + gr, 8)
            _, der = gelu_parts(rows[i] + pw[sl, :])
            h[sl, :] = der * pc[sl, :]
    each_group(W, group2)
    channel_mix(w["point"], h, W, pw, W)
    coef = analyse(h, W, g, waves_ref)
    synthesise(unmix_modes(coef, wr, wi, 1, r), W, a, waves_ref)
    def group3(gr):
        rows = to_rows(waves_of(a, gr))
        for i in range(ROWS):
            sl = pl.ds(i * W + gr, 8)
            h[sl, :] = d1[sl, :] * (rows[i] + pw[sl, :])
    each_group(W, group3)
    channel_mix(w["out"], h, W, pw, CIN)
    coef = analyse(h, W, g, waves_ref)
    coef = unmix_modes(coef, wr, wi, 0, r)
    coef = jnp.dot(w["lift"], tall(coef), preferred_element_type=F32)
    synthesise(coef, CIN, a, waves_ref)
    def group4(gr):
        rows = to_rows(waves_of(a, gr))
        for i in range(ROWS):
            sl = pl.ds(i * CIN + gr, 8)
            out_ref[sl, :] = rows[i] + pw[sl, :]
    each_group(CIN, group4)


VARS = 5
TILE = 8
MESH = pl.DeviceIdType.MESH
AROUND = sorted(
    ((dx, dy) for dx in range(-2, 3) for dy in range(-2, 3) if (dx, dy) != (0, 0)),
    key=lambda o: (o[1] == 0, abs(o[1]), abs(o[0]), o),
)


ROUND = [o for o in AROUND if o[0] > 0]


def tiles_of(dx, dy):
    if abs(dx) == 2 or abs(dy) == 2:
        return 1
    return VARS if dx == 0 or dy == 0 else 3


START = {}
TILES = 0
for _o in AROUND:
    START[_o] = TILES
    TILES += tiles_of(*_o)


def pieces(dx, dy):
    out = []
    far_col, near_col = 0, 32 if dy == -1 else 0
    blocks = {-1: (1,), 0: (0, 1), 1: (0,)}[dx]
    for ch in range(VARS):
        if dx == 0:
            for rb in blocks:
                out.append(("near", ch, rb, near_col, 32, ch, 32 * rb))
            out.append(("far", ch, 0, far_col, 32, ch, 64))
        elif dy == 0:
            out.append(("near", ch, blocks[0], 0, 64, ch, 0))
            out.append(("far", ch, 0, 0, 32, ch, 64))
        else:
            base = 64 * (ch % 2)
            out.append(("near", ch, blocks[0], near_col, 32, ch // 2, base))
            out.append(("far", ch, 0, far_col, 32, ch // 2, base + 32))
    return out


def far_edge_col(dy):
    return 16 if dy == -2 else 0


def near_lane(col, dy=0):
    return 32 + col + 64 * dy


def far_lane(col, dy=0):
    return 48 + col + 32 * dy


FAR_ROW = {-2: 0, -1: 4, 0: 12, 1: 20, 2: 28}


def lane_ids():
    return lax.broadcasted_iota(jnp.int32, (TILE, COLS), 1)


def row_ids():
    return lax.broadcasted_iota(jnp.int32, (TILE, COLS), 0)


def turned(x, shift, axis=1, period=None):
    shift %= period or x.shape[axis]
    return x if shift == 0 else pltpu.roll(x, shift, axis)


class Lanes:
    def __init__(self):
        self.lane = lane_ids()
        self.row = row_ids()
        self.masks = {}

    def mask(self, first, width):
        key = (first, width)
        if key not in self.masks:
            self.masks[key] = (self.lane >= first) & (self.lane < first + width)
        return self.masks[key]

    def put(self, base, value, first, width):
        return value if base is None else jnp.where(self.mask(first, width), value, base)

    def only(self, value, first, width):
        return jnp.where(self.mask(first, width), value, 0.0)


def pool_maps():
    j = np.arange(COLS)[:, None]
    lane = np.arange(COLS)[None, :]
    gather = np.concatenate(
        [((lane - 32) % 64 == j // 2) * 0.25, ((lane - 48) % 32 == j // 4) * 0.0625], axis=1
    )
    spread = np.concatenate(
        [(j - 32 == lane // 2) * 0.25, (j - 48 == lane // 4) * 0.0625], axis=1
    )
    return np.concatenate([gather, spread], axis=0).astype(jnp.bfloat16)


def mapped(rows, table):
    hi, lo = split(rows)
    both = jnp.dot(jnp.concatenate([hi, lo], axis=0), table, preferred_element_type=F32)
    return both[: rows.shape[0]] + both[rows.shape[0]:]


def send_tiles(lanes, near, far, buf):
    rolled = {}

    def near_at(ch, rb, col, lane):
        key = ("n", ch, rb, (lane - near_lane(col)) % 64)
        if key not in rolled:
            rolled[key] = turned(near[ch][rb], key[3], period=64)
        return rolled[key]

    def far_at(ch, col, lane):
        key = ("f", ch, (lane - far_lane(col)) % 32)
        if key not in rolled:
            rolled[key] = turned(far[ch], key[2], period=32)
        return rolled[key]

    strips = {}
    for dx, dy in AROUND:
        start = START[dx, dy]
        if abs(dy) == 2:
            if ("y", dy) not in strips:
                tile = None
                for ch in range(VARS):
                    tile = lanes.put(tile, far_at(ch, far_edge_col(dy), 16 * ch), 16 * ch, 16)
                strips["y", dy] = tile
            buf[start * TILE:(start + 1) * TILE, :] = strips["y", dy]
        elif abs(dx) == 2:
            if ("x", dx) not in strips:
                tile = None
                for ch in range(4):
                    tile = lanes.put(tile, far_at(ch, 0, 32 * ch), 32 * ch, 32)
                last = far_at(4, 0, 0)
                if dx == -2:
                    tile = turned(tile, 4, axis=0)
                else:
                    last = turned(last, 4, axis=0)
                strips["x", dx] = jnp.where(lanes.mask(0, 32) & (lanes.row >= 4), last, tile)
            buf[start * TILE:(start + 1) * TILE, :] = strips["x", dx]
        else:
            tiles = [None] * tiles_of(dx, dy)
            for kind, ch, rb, col, width, tile, lane in pieces(dx, dy):
                value = near_at(ch, rb, col, lane) if kind == "near" else far_at(ch, col, lane)
                tiles[tile] = lanes.put(tiles[tile], value, lane, width)
            for n, value in enumerate(tiles):
                buf[(start + n) * TILE:(start + n + 1) * TILE, :] = value


def tile_at(buf, o, n=0):
    first = (START[o] + n) * TILE
    return buf[first:first + TILE, :]


def read_windows(lanes, near, far, buf, f_ref):
    blocks = {}
    rows = {}
    for ch in range(VARS):
        blocks[ch, 1], blocks[ch, 2] = near[ch]
        rows[ch, 0] = far[ch]
    for dx in (0, -1, 1):
        for dy in (0, -1, 1):
            if (dx, dy) == (0, 0):
                continue
            for kind, ch, rb, col, width, tile, lane in pieces(dx, dy):
                value = tile_at(buf, (dx, dy), tile)
                if kind == "near":
                    key = (ch, {-1: 0, 0: 1 + rb, 1: 3}[dx])
                    to, table = near_lane(col, dy), blocks
                else:
                    key, to, table = (ch, dx), far_lane(col, dy), rows
                table[key] = lanes.put(table.get(key), turned(value, to - lane), to, width)
    for dx in (-2, 2):
        for dy in (0, -1, 1):
            value = tile_at(buf, (dx, dy))
            low = turned(value, 4, axis=0)
            for ch in range(VARS):
                to, lane = far_lane(0, dy), 32 * ch if ch < 4 else 0
                got = turned(value if ch < 4 else low, to - lane)
                rows[ch, dx] = lanes.put(rows.get((ch, dx)), got, to, 32)
    for dx in range(-2, 3):
        for dy in (-2, 2):
            value = tile_at(buf, (dx, dy))
            if dx == -2:
                value = turned(value, 4, axis=0)
            for ch in range(VARS):
                to = far_lane(far_edge_col(dy), dy)
                rows[ch, dx] = lanes.put(rows[ch, dx], turned(value, to - 16 * ch), to, 16)
    for (ch, k), value in blocks.items():
        f_ref[pl.ds(8 * k * CIN + VARS + ch, TILE, stride=CIN), :] = value
    for (ch, dx), value in rows.items():
        count = 4 if abs(dx) == 2 else TILE
        f_ref[pl.ds(FAR_ROW[dx] * CIN + 2 * VARS + ch, count, stride=CIN), :] = value[:count]


def window_tiles(go):
    near = {(ch, k): go[pl.ds(8 * k * CIN + VARS + ch, TILE, stride=CIN), :] for ch in range(VARS) for k in range(4)}
    far = {}
    for ch in range(VARS):
        for dx in range(-2, 3):
            first = 24 if dx == 2 else FAR_ROW[dx]
            far[ch, dx] = go[pl.ds(first * CIN + 2 * VARS + ch, TILE, stride=CIN), :]
    return near, far


def send_grads(lanes, near, far, buf, owners):
    for dx, dy in owners:
        start = START[dx, dy]
        if abs(dy) == 2:
            tile = None
            for ch in range(VARS):
                got = turned(far[ch, dx], 16 * ch - far_lane(far_edge_col(dy), dy))
                tile = lanes.put(tile, got, 16 * ch, 16)
            if abs(dx) == 2:
                tile = turned(tile, 4, axis=0)
                keep = lanes.row >= 4 if dx == -2 else lanes.row < 4
                tile = jnp.where(keep, tile, 0.0)
            buf[start * TILE:(start + 1) * TILE, :] = tile
        elif abs(dx) == 2:
            tile = None
            for ch in range(4):
                tile = lanes.put(tile, turned(far[ch, dx], 32 * ch - far_lane(0, dy)), 32 * ch, 32)
            last = turned(far[4, dx], -far_lane(0, dy))
            if dx == -2:
                last = turned(last, 4, axis=0)
            else:
                tile = turned(tile, 4, axis=0)
            buf[start * TILE:(start + 1) * TILE, :] = jnp.where(lanes.mask(0, 32) & (lanes.row >= 4), last, tile)
        else:
            tiles = [None] * tiles_of(dx, dy)
            for kind, ch, rb, col, width, tile, lane in pieces(dx, dy):
                if kind == "near":
                    value = turned(near[ch, {-1: 0, 0: 1 + rb, 1: 3}[dx]], lane - near_lane(col, dy))
                else:
                    value = turned(far[ch, dx], lane - far_lane(col, dy))
                tiles[tile] = lanes.put(tiles[tile], value, lane, width)
            for n, value in enumerate(tiles):
                buf[(start + n) * TILE:(start + n + 1) * TILE, :] = value


def sum_grads(lanes, near, far, buf):
    n_sum = {(ch, rb): lanes.only(near[ch, 1 + rb], 32, 64) for ch in range(VARS) for rb in range(2)}
    f_sum = {ch: lanes.only(far[ch, 0], 48, 32) for ch in range(VARS)}
    for dx in (-1, 0, 1):
        for dy in (-1, 0, 1):
            if (dx, dy) == (0, 0):
                continue
            for kind, ch, rb, col, width, tile, lane in pieces(dx, dy):
                value = tile_at(buf, (dx, dy), tile)
                if kind == "near":
                    to = near_lane(col)
                    n_sum[ch, rb] += lanes.only(turned(value, to - lane), to, width)
                else:
                    to = far_lane(col)
                    f_sum[ch] += lanes.only(turned(value, to - lane), to, width)
    for dx in (-2, 2):
        value = tree_sum([tile_at(buf, (dx, dy)) for dy in (-1, 0, 1)])
        low = turned(value, 4, axis=0)
        keep = lanes.row >= 4 if dx == -2 else lanes.row < 4
        for ch in range(VARS):
            natural = (ch < 4) == (dx == 2)
            lane = 32 * ch if ch < 4 else 0
            got = turned(value if natural else low, far_lane(0) - lane)
            f_sum[ch] += jnp.where(lanes.mask(48, 32) & keep, got, 0.0)
    for dy in (-2, 2):
        value = tree_sum([tile_at(buf, (dx, dy)) for dx in range(-2, 3)])
        for ch in range(VARS):
            to = far_lane(far_edge_col(dy))
            f_sum[ch] += lanes.only(turned(value, to - 16 * ch), to, 16)
    return (
        jnp.concatenate([n_sum[ch, rb] for ch in range(VARS) for rb in range(2)], axis=0),
        jnp.concatenate([f_sum[ch] for ch in range(VARS)], axis=0),
    )


Y_SIDE = 4
EDGES = (1, -1, 2, -2)
RELAY = {1: 0, -1: VARS, 2: 2 * VARS, -2: 2 * VARS + 1}
PASSED = {-1: 0, 1: 3, -2: 6, 2: 7}


def repack(lanes, main, e, buf, first):
    for dx in (-1, 1):
        tiles = [None] * 3
        for kind, ch, rb, _, width, tile, lane in pieces(dx, -e):
            value = turned(main[ch], lane - (32 * rb if kind == "near" else 64))
            tiles[tile] = lanes.put(tiles[tile], value, lane, width)
        for n, value in enumerate(tiles):
            row = (first + PASSED[dx] + n) * TILE
            buf[row:row + TILE, :] = value
    strip = None
    for ch in range(4):
        strip = lanes.put(strip, turned(main[ch], 32 * ch - 64), 32 * ch, 32)
    last = turned(main[4], -64)
    corner = lanes.mask(0, 32) & (lanes.row >= 4)
    for dx in (-2, 2):
        row = (first + PASSED[dx]) * TILE
        low, high = (turned(strip, 4, axis=0), last) if dx == -2 else (strip, turned(last, 4, axis=0))
        buf[row:row + TILE, :] = jnp.where(corner, high, low)


def kernel(counts, field_hbm, cot_hbm, lift_hbm, spectral_hbm, point_hbm, proj_hbm, waves_hbm, maps_hbm, out_ref,
           field, cot, lift, spectral, point, proj, waves, maps, f, ct, go, pooled, spread_near, spread_far,
           fwd_out, fwd_in, bwd_out, bwd_in, relay_in, relay_out, load_sem, send_sem, recv_sem, to_mid_sem, at_mid_sem,
           from_mid_sem, stage_in, stage_sem, ready_sem, *scr):
    gx, gy = lax.axis_index("gx"), lax.axis_index("gy")
    n_gx, n_gy = counts
    loads = [
        pltpu.make_async_copy(src, dst, load_sem.at[n])
        for n, (src, dst) in enumerate([
            (field_hbm, field), (maps_hbm, maps), (cot_hbm, cot), (lift_hbm, lift), (point_hbm, point),
            (proj_hbm, proj), (spectral_hbm, spectral), (waves_hbm, waves)])
    ]
    for copy in loads:
        copy.start()
    half_z = n_gx // 2
    n_z = 2 * half_z
    y = lax.rem(gy, Y_SIDE)
    index = {o: n for n, o in enumerate(AROUND)}

    def device(dx, dy, base=None):
        bx, by = base or (gx, gy)
        return (lax.rem(bx + (dx + n_gx), n_gx), lax.rem(by + (dy + n_gy), n_gy))

    def crosses(e):
        return (y + e < 0) | (y + e >= Y_SIDE)

    def middle(place, sign):
        px, py = place
        core, group = lax.rem(px, 2), lax.div(py, Y_SIDE)
        z = lax.rem(group, 2) * half_z + lax.div(px, 2)
        step = sign * (n_z // 4)
        z = lax.rem(z + jnp.where(core == 0, n_z + step, n_z - step), n_z)
        row = lax.div(group, 2) * (2 * Y_SIDE) + lax.div(z, half_z) * Y_SIDE + lax.rem(py, Y_SIDE)
        return (2 * lax.rem(z, half_z) + core, row)

    mine, source = middle((gx, gy), 1), middle((gx, gy), -1)

    hop = 2 * ((half_z - 1) // 2)
    staged = lax.div(gx, 2) == hop // 2
    stage_source = gx - hop
    edge = gx < 2

    def stage_of(px):
        return px + hop

    def goes_round(o, px):
        round_end = px - o[0] < 0
        return round_end if o[1] == 0 else round_end & jnp.logical_not(crosses(-o[1]))

    def count(flag):
        return jnp.where(flag, 1, 0)

    quarter_z, half_here = n_z // 4, lax.rem(lax.div(gy, Y_SIDE), 2)
    early_here = half_here * half_z + lax.div(gx, 2) < quarter_z
    early, tell_later = {}, {}
    for dx in range(-2, 3):
        ox = lax.rem(gx + (dx + n_gx), n_gx)
        oz = (1 - half_here) * half_z + lax.div(ox, 2)
        oz += jnp.where(lax.rem(ox, 2) == 0, n_z + quarter_z, n_z - quarter_z)
        early[dx] = lax.rem(oz, n_z) < quarter_z

    barrier = pltpu.get_barrier_semaphore()
    by_middle = half_here == 0
    relays = lax.rem(lax.div(source[1], Y_SIDE), 2) == 0
    pl.when(relays)(functools.partial(
        pl.semaphore_signal, barrier, inc=1, device_id=source, device_id_type=MESH))
    for dx, dy in AROUND:
        owner = sender = device(dx, dy)
        if dx != 0:
            round_end = gx + dx >= n_gx
            sender = (jnp.where(round_end, stage_of(owner[0]), owner[0]), owner[1])
        told = functools.partial(pl.semaphore_signal, barrier, inc=1, device_id_type=MESH)
        if dy == 0:
            told(device_id=sender)
            continue
        via, far_one = middle(owner, 1), crosses(dy)
        across = tuple(jnp.where(half_here == 1, a, b) for a, b in zip(via, owner))
        sender = tuple(jnp.where(far_one, a, b) for a, b in zip(across, sender))
        tell_later[dx, dy] = (far_one & (half_here == 1) & early[dx], via)
        pl.when(jnp.logical_not(tell_later[dx, dy][0]))(functools.partial(told, device_id=sender))

    @pl.when(early_here & relays)
    def _():
        for e in EDGES:
            @pl.when(crosses(e))
            def _(e=e):
                for ex in range(-2, 3):
                    pl.semaphore_signal(barrier, inc=1, device_id=device(ex, e, source), device_id_type=MESH)

    @pl.when(staged)
    def _():
        pl.semaphore_signal(barrier, inc=1, device_id=(stage_source, gy), device_id_type=MESH)

    expected = len(AROUND) + count(by_middle) + count(edge)
    for o in AROUND:
        if o[0] > 0:
            expected += count(staged & goes_round(o, stage_source)) - count(goes_round(o, gx))
    for later, _ in tell_later.values():
        expected += count(later)
    for e in EDGES:
        expected += 5 * (count(crosses(e) & relays & jnp.logical_not(early_here)) - count(crosses(e) & by_middle))
    def span(o):
        return pl.ds(START[o] * TILE, tiles_of(*o) * TILE)

    def direct(turn, src, dst, o):
        sign = -1 if turn == 0 else 1
        return pltpu.make_async_remote_copy(
            src_ref=src.at[span(o)], dst_ref=dst.at[span(o)], send_sem=send_sem.at[turn, index[o]],
            recv_sem=recv_sem.at[turn, index[o]], device_id=device(sign * o[0], sign * o[1]), device_id_type=MESH)

    def to_middle(e):
        tiles = tiles_of(0, -e)
        return pltpu.make_async_remote_copy(
            src_ref=fwd_out.at[span((0, -e))], dst_ref=relay_in.at[pl.ds(RELAY[e] * TILE, tiles * TILE)],
            send_sem=to_mid_sem.at[EDGES.index(e)], recv_sem=at_mid_sem.at[EDGES.index(e)], device_id=mine,
            device_id_type=MESH)

    def from_middle(e, ex):
        o = (-ex, -e)
        if abs(e) == 2 or ex == 0:
            first, ref = RELAY[e], relay_in
        else:
            first, ref = PASSED[-ex] + (0 if e == 1 else 8), relay_out
        return pltpu.make_async_remote_copy(
            src_ref=ref.at[pl.ds(first * TILE, tiles_of(*o) * TILE)], dst_ref=fwd_in.at[span(o)],
            send_sem=from_mid_sem.at[EDGES.index(e), ex + 2], recv_sem=recv_sem.at[0, index[o]],
            device_id=device(ex, e, source), device_id_type=MESH)

    def to_stage(o):
        return pltpu.make_async_remote_copy(
            src_ref=fwd_out.at[span(o)], dst_ref=stage_in.at[span(o)], send_sem=stage_sem.at[0, index[o]],
            recv_sem=stage_sem.at[1, index[o]], device_id=(stage_of(gx), gy), device_id_type=MESH)

    def from_stage(o):
        return pltpu.make_async_remote_copy(
            src_ref=stage_in.at[span(o)], dst_ref=fwd_in.at[span(o)], send_sem=stage_sem.at[2, index[o]],
            recv_sem=recv_sem.at[0, index[o]], device_id=device(-o[0], -o[1], (stage_source, gy)), device_id_type=MESH)

    lanes = Lanes()
    loads[0].wait()
    loads[1].wait()
    half = field[pl.ds(0, 80, stride=2), :] + field[pl.ds(1, 80, stride=2), :]
    pooled[...] = half
    quarter = pooled[pl.ds(0, 40, stride=2), :] + pooled[pl.ds(1, 40, stride=2), :]
    got = mapped(jnp.concatenate([half, quarter], axis=0), maps[0:COLS, :])
    near = [[got[ch * 16 + rb * 8:ch * 16 + rb * 8 + 8, :COLS] for rb in range(2)] for ch in range(VARS)]
    far = [got[80 + ch * 8:80 + ch * 8 + 8, COLS:] for ch in range(VARS)]
    send_tiles(lanes, near, far, fwd_out)
    pl.semaphore_wait(barrier, expected)
    for o, (later, via) in tell_later.items():
        pl.when(later)(functools.partial(
            pl.semaphore_signal, ready_sem.at[index[o]], inc=1, device_id=via, device_id_type=MESH))

    def pass_on(e, ex):
        pl.when(early_here)(functools.partial(pl.semaphore_wait, ready_sem.at[index[-ex, -e]], 1))
        from_middle(e, ex).start()

    for e in EDGES:
        @pl.when(crosses(e) & by_middle)
        def _(e=e):
            to_middle(e).start()
    for o in ROUND:
        @pl.when(goes_round(o, gx))
        def _(o=o):
            to_stage(o).start()

    def goes_directly(o):
        target = gx - o[0]
        inside = target >= 0
        if o[1] == 0:
            return inside
        across = crosses(-o[1])
        return (across & jnp.logical_not(by_middle)) | (inside & jnp.logical_not(across))

    for o in AROUND:
        @pl.when(goes_directly(o))
        def _(o=o):
            direct(0, fwd_out, fwd_in, o).start()

    for copy in loads[2:]:
        copy.wait()
    f[...] = jnp.zeros_like(f)
    ct[...] = jnp.zeros_like(ct)
    for v in range(VARS):
        f[pl.ds(v, ROWS, stride=CIN), :] = field[v * ROWS:(v + 1) * ROWS, :]
        ct[pl.ds(v, ROWS, stride=8), :] = cot[v * ROWS:(v + 1) * ROWS, :]
    setup = network_setup(ct, lift, spectral, point, proj, scr)

    @pl.when(staged)
    def _():
        for o in ROUND:
            @pl.when(goes_round(o, stage_source))
            def _(o=o):
                to_stage(o).wait_recv()
                from_stage(o).start()

    for e in EDGES:
        @pl.when(crosses(e) & relays)
        def _(e=e):
            to_middle(e).wait_recv()
            pass_on(e, 0)
            if abs(e) == 1:
                main = [relay_in[(RELAY[e] + ch) * TILE:(RELAY[e] + ch + 1) * TILE, :] for ch in range(VARS)]
                repack(Lanes(), main, e, relay_out, 0 if e == 1 else 8)
            for ex in (-1, 1, -2, 2):
                pass_on(e, ex)

    for o in AROUND:
        direct(0, fwd_out, fwd_in, o).wait_recv()
    read_windows(lanes, near, far, fwd_in, f)
    network_grad(f, setup, waves, go, scr)

    near, far = window_tiles(go)
    for owners in ([o for o in AROUND if o[1] != 0], [o for o in AROUND if o[1] == 0]):
        send_grads(lanes, near, far, bwd_out, owners)
        for o in owners:
            direct(1, bwd_out, bwd_in, o).start()
    for o in AROUND:
        direct(1, bwd_out, bwd_in, o).wait_recv()
    n_sum, f_sum = sum_grads(lanes, near, far, bwd_in)
    got = mapped(jnp.concatenate([n_sum, f_sum], axis=0), maps[COLS:, :])
    for k in range(2):
        spread_near[pl.ds(k, 80, stride=2), :] = got[:80, :COLS]
    for k in range(4):
        spread_far[pl.ds(k, 40, stride=4), :] = got[80:, COLS:]
    for v in range(VARS):
        rows = slice(v * ROWS, (v + 1) * ROWS)
        out_ref[rows, :] = go[pl.ds(v, ROWS, stride=CIN), :] + spread_near[rows, :] + spread_far[rows, :]
    for o in AROUND:
        direct(1, bwd_out, bwd_in, o).wait_send()

        @pl.when(goes_directly(o))
        def _(o=o):
            direct(0, fwd_out, fwd_in, o).wait_send()
    for e in EDGES:
        pl.when(crosses(e) & by_middle)(to_middle(e).wait_send)

        @pl.when(crosses(e) & relays)
        def _(e=e):
            for ex in range(-2, 3):
                from_middle(e, ex).wait_send()
    for o in ROUND:
        @pl.when(goes_round(o, gx))
        def _(o=o):
            to_stage(o).wait_send()

        @pl.when(staged & goes_round(o, stage_source))
        def _(o=o):
            from_stage(o).wait_send()


def body(counts, field, cotangent, lift, spectral, pointwise, project):
    vmem = lambda *shape, dtype=F32: pltpu.VMEM(shape, dtype)
    flat = (VARS * ROWS, COLS)
    hbm = pl.BlockSpec(memory_space=pltpu.MemorySpace.HBM)
    call = pl.pallas_call(
        functools.partial(kernel, counts),
        out_shape=pltpu.VMEM(flat, F32),
        in_specs=[hbm] * 8,
        out_specs=pl.BlockSpec(memory_space=pltpu.VMEM),
        scratch_shapes=[
            vmem(*flat), vmem(*flat), vmem(3 * VARS, W), vmem(2, 2, W, W, MD * MD), vmem(2, W, W), vmem(VARS, W),
            vmem(NWAVE * COLS, 2 * COLS, dtype=BF16), vmem(2 * COLS, 2 * COLS, dtype=BF16),
            vmem(ROWS * CIN, COLS), vmem(ROWS * 8, COLS), vmem(ROWS * CIN, COLS),
            vmem(80, COLS), vmem(*flat), vmem(*flat),
            vmem(TILES * TILE, COLS), vmem(TILES * TILE, COLS), vmem(TILES * TILE, COLS), vmem(TILES * TILE, COLS),
            vmem(12 * TILE, COLS), vmem(16 * TILE, COLS),
            pltpu.SemaphoreType.DMA((8,)), pltpu.SemaphoreType.DMA((2, len(AROUND))),
            pltpu.SemaphoreType.DMA((2, len(AROUND))),
            pltpu.SemaphoreType.DMA((4,)), pltpu.SemaphoreType.DMA((4,)), pltpu.SemaphoreType.DMA((4, 5)),
            vmem(TILES * TILE, COLS), pltpu.SemaphoreType.DMA((3, len(AROUND))),
            pltpu.SemaphoreType.REGULAR((len(AROUND),)),
            vmem(2, W, W, COLS), vmem(2, W, W, COLS), vmem(W, NWAVE * COLS), vmem(W, NWAVE * COLS),
            vmem(2 * W, COLS), vmem(W * 8, COLS), vmem(ROWS * W, COLS), vmem(ROWS * W, COLS), vmem(ROWS * W, COLS),
            vmem(ROWS * W, COLS),
        ],
        compiler_params=pltpu.CompilerParams(collective_id=0, has_side_effects=True, vmem_limit_bytes=55300 << 10),
        name="patch_grad",
    )
    out = call(
        field.reshape(flat), cotangent.reshape(flat), lift, spectral.transpose(0, 1, 3, 4, 2), pointwise, project.T,
        jnp.asarray(mode_waves()), jnp.asarray(pool_maps()))
    return out.reshape(field.shape)


def solution(mesh):
    counts = (mesh.shape["gx"], mesh.shape["gy"])
    return jax.shard_map(
        functools.partial(body, counts),
        mesh=mesh,
        in_specs=(P(None, None, "gx", "gy"), P(None, None, "gx", "gy"), P(), P(), P(), P()),
        out_specs=P(None, None, "gx", "gy"),
        check_vma=False,
    )
```

```python
import functools
import math

import jax
import jax.numpy as jnp
import numpy as np
from jax import lax
from jax.experimental import pallas as pl
from jax.experimental.pallas import tpu as pltpu
from jax.sharding import PartitionSpec as P

F32, BF16 = jnp.float32, jnp.bfloat16
LOOP = False
ROWS, COLS, W, CIN, MD = 32, 128, 32, 16, 8
WAVES = [(0, 0), (1, 0), (1, 1), (2, 0), (2, 1), (3, 0), (3, 1), (4, 0), (4, 1)]
NWAVE = len(WAVES)
HIGHEST = lax.Precision.HIGHEST


def mode_waves():
    j = np.arange(COLS)[:, None]
    kx = np.repeat(np.arange(MD) - MD // 2, MD)[None, :]
    ky = np.tile(np.arange(MD), MD)[None, :]
    b = 2 * np.pi * ((j * ky) % COLS) / COLS
    scale = 1.0 / math.sqrt(ROWS * COLS)
    parts = []
    for k, is_sin in WAVES:
        hit = (np.abs(kx) == k).astype(np.float64)
        if is_sin:
            sg = np.sign(kx) * hit
            re, im = -sg * np.sin(b), -sg * np.cos(b)
        else:
            re, im = hit * np.cos(b), -hit * np.sin(b)
        parts.append(np.concatenate([re, im], axis=1) * scale)
    table = np.concatenate(parts, axis=0).astype(np.float32)
    hi = table.astype(jnp.bfloat16)
    lo = (table - hi.astype(np.float32)).astype(jnp.bfloat16)
    return np.concatenate([hi, lo], axis=1)


def wave(k, i):
    return math.cos(2 * math.pi * k * i / ROWS), math.sin(2 * math.pi * k * i / ROWS)


def weighted(terms):
    total = None
    for c, x in terms:
        if abs(c) < 1e-12:
            continue
        t = x if abs(c - 1) < 1e-12 else (-x if abs(c + 1) < 1e-12 else x * np.float32(c))
        total = t if total is None else total + t
    return total


def tree_sum(xs):
    xs = list(xs)
    while len(xs) > 1:
        xs = [xs[i] + xs[i + 1] if i + 1 < len(xs) else xs[i] for i in range(0, len(xs), 2)]
    return xs[0]


def to_waves(x):
    s = [x[i] + x[i + 16] for i in range(16)]
    d = [x[i] - x[i + 16] for i in range(16)]
    dc = [d[0]] + [d[i] - d[16 - i] for i in range(1, 8)]
    ds = [None] + [d[i] + d[16 - i] for i in range(1, 8)] + [d[8]]
    out = {}
    for k in (1, 3):
        out[(k, 0)] = weighted([(wave(k, i)[0], dc[i]) for i in range(8)])
        out[(k, 1)] = weighted([(wave(k, i)[1], ds[i]) for i in range(1, 9)])
    p = [s[i] + s[i + 8] for i in range(8)]
    m = [s[i] - s[i + 8] for i in range(8)]
    mc = [m[0]] + [m[i] - m[8 - i] for i in range(1, 4)]
    ms = [None] + [m[i] + m[8 - i] for i in range(1, 4)] + [m[4]]
    out[(2, 0)] = weighted([(wave(2, i)[0], mc[i]) for i in range(4)])
    out[(2, 1)] = weighted([(wave(2, i)[1], ms[i]) for i in range(1, 5)])
    q = [p[i] - p[i + 4] for i in range(4)]
    r = np.float32(math.sqrt(0.5))
    out[(4, 0)] = q[0] + r * (q[1] - q[3])
    out[(4, 1)] = q[2] + r * (q[1] + q[3])
    out[(0, 0)] = tree_sum([p[i] + p[i + 4] for i in range(4)])
    return [out[w] for w in WAVES]


def to_rows(a):
    a = dict(zip(WAVES, a))
    r = np.float32(math.sqrt(0.5))
    c0, c4, s4 = a[(0, 0)], a[(4, 0)], a[(4, 1)]
    u, v = r * (c4 + s4), r * (s4 - c4)
    e04 = [c0 + c4, c0 + u, c0 + s4, c0 + v, c0 - c4, c0 - u, c0 - s4, c0 - v]
    c2 = [weighted([(wave(2, i)[0], a[(2, 0)])]) for i in range(4)]
    s2 = [None] + [weighted([(wave(2, i)[1], a[(2, 1)])]) for i in range(1, 5)]
    e2 = [c2[0]] + [c2[i] + s2[i] for i in range(1, 4)] + [s2[4]] + [s2[8 - i] - c2[8 - i] for i in range(5, 8)]
    ev = [e04[i] + e2[i] for i in range(8)] + [e04[i] - e2[i] for i in range(8)]
    oc = [weighted([(wave(k, i)[0], a[(k, 0)]) for k in (1, 3)]) for i in range(8)]
    os_ = [None] + [weighted([(wave(k, i)[1], a[(k, 1)]) for k in (1, 3)]) for i in range(1, 9)]
    od = [oc[0]] + [oc[i] + os_[i] for i in range(1, 8)] + [os_[8]] + [os_[16 - i] - oc[16 - i] for i in range(9, 16)]
    return [ev[i] + od[i] for i in range(16)] + [ev[i] - od[i] for i in range(16)]


def split(x):
    hi = x.astype(BF16)
    lo = (x - hi.astype(F32)).astype(BF16)
    return hi, lo


def tall(x):
    hi, lo = split(x)
    return jnp.concatenate([hi, lo, hi], axis=0)


def wide(x):
    hi, lo = split(x)
    return jnp.concatenate([hi, hi, lo], axis=1)


def channel_mix(left, x_ref, width, out_ref, out_width):
    for i in range(0, ROWS, 2):
        right = jnp.concatenate([tall(x_ref[(i + t) * width:(i + t + 1) * width, :]) for t in range(2)], axis=1)
        got = jnp.dot(left, right, preferred_element_type=F32)
        out_ref[i * out_width:(i + 1) * out_width, :] = got[:, :COLS]
        out_ref[(i + 1) * out_width:(i + 2) * out_width, :] = got[:, COLS:]


def each_group(width, fn):
    if LOOP:
        @pl.loop(0, width // 8)
        def _(n):
            fn(pl.multiple_of(n * 8, 8))
    else:
        for g in range(0, width, 8):
            fn(g)


def analyse(x_ref, width, g_ref, waves_ref):
    def group(g):
        got = to_waves([x_ref[pl.ds(i * width + g, 8), :] for i in range(ROWS)])
        for n in range(NWAVE):
            g_ref[pl.ds(g, 8), n * COLS:(n + 1) * COLS] = got[n]
    each_group(width, group)
    hi, lo = split(g_ref[0:width, :])
    both = jnp.dot(jnp.concatenate([hi, lo], axis=0), waves_ref[...], preferred_element_type=F32)
    return (both[:width, :COLS] + both[width:, :COLS]) + (both[:width, COLS:] + both[width:, COLS:])


def synthesise(coef, width, a_ref, waves_ref):
    hi, lo = split(coef)
    left = jnp.concatenate([jnp.concatenate([hi, hi], axis=1), jnp.concatenate([lo, lo], axis=1)], axis=0)
    both = lax.dot_general(left, waves_ref[...], (((1,), (1,)), ((), ())), preferred_element_type=F32)
    a_ref[0:width, :] = both[:width] + both[width:]


def waves_of(a_ref, g):
    return [a_ref[pl.ds(g, 8), n * COLS:(n + 1) * COLS] for n in range(NWAVE)]


def half_swap(x):
    return jnp.concatenate([x[:, 64:], x[:, :64]], axis=1)


def mix_modes(coef, wr_ref, wi_ref, layer, c_ref):
    c_ref[0:W, :] = coef
    c_ref[W:2 * W, :] = half_swap(coef)
    accs = [None] * 4
    for w in range(W):
        t = (wr_ref[layer, w] * jnp.broadcast_to(c_ref[w:w + 1, :], (W, COLS))
             + wi_ref[layer, w] * jnp.broadcast_to(c_ref[W + w:W + w + 1, :], (W, COLS)))
        accs[w % 4] = t if accs[w % 4] is None else accs[w % 4] + t
    return (accs[0] + accs[1]) + (accs[2] + accs[3])


def unmix_modes(grad, wr_ref, wi_ref, layer, r_ref):
    swapped = half_swap(grad)
    for w in range(W):
        t = wr_ref[layer, w] * grad - wi_ref[layer, w] * swapped
        r_ref[w * 8:(w + 1) * 8, :] = (t[0:8] + t[8:16]) + (t[16:24] + t[24:32])
    return tree_sum([r_ref[pl.ds(s, W, stride=8), :] for s in range(8)])


def gelu_parts(x):
    cdf = 0.5 * lax.erf(x * np.float32(math.sqrt(0.5))) + 0.5
    pdf = jnp.exp(-0.5 * (x * x)) * np.float32(1.0 / math.sqrt(2 * math.pi))
    return x * cdf, cdf + x * pdf


def prepare(spectral_ref, wr_ref, wi_ref):
    for layer in range(2):
        for w in range(W):
            re, im = spectral_ref[layer, 0, w], spectral_ref[layer, 1, w]
            wr_ref[layer, w] = jnp.concatenate([re, re], axis=1)
            wi_ref[layer, w] = jnp.concatenate([-im, im], axis=1)


def network_setup(cot_ref, lift_ref, spectral_ref, point_ref, proj_ref, scr):
    prepare(spectral_ref, scr[0], scr[1])
    lift16 = jnp.concatenate([lift_ref[...], jnp.zeros((1, W), F32)], axis=0)
    p1, p2 = point_ref[0], point_ref[1]
    both1 = jnp.dot(lift16, p1, precision=HIGHEST, preferred_element_type=F32)
    both1_t = jnp.transpose(both1)
    lift_t = jnp.transpose(lift16)
    proj8 = jnp.concatenate([proj_ref[...], jnp.zeros((3, W), F32)], axis=0)
    proj_t = jnp.transpose(proj8)
    channel_mix(wide(proj_t), cot_ref, 8, scr[-1], W)
    return {
        "in": wide(both1_t), "out": wide(both1), "point": wide(p2), "point_t": wide(jnp.transpose(p2)),
        "lift": lift16, "lift_t": lift_t,
    }


def network_grad(f_ref, setup, waves_ref, out_ref, scr):
    wr, wi, g, a, c, r, pw, h, d1, pc = scr
    w = setup
    channel_mix(w["in"], f_ref, CIN, pw, W)
    coef = analyse(f_ref, CIN, g, waves_ref)
    coef = jnp.dot(w["lift_t"], coef, precision=HIGHEST, preferred_element_type=F32)
    synthesise(mix_modes(coef, wr, wi, 0, c), W, a, waves_ref)
    def group1(gr):
        rows = to_rows(waves_of(a, gr))
        for i in range(ROWS):
            sl = pl.ds(i * W + gr, 8)
            val, der = gelu_parts(rows[i] + pw[sl, :])
            h[sl, :] = val
            d1[sl, :] = der
    each_group(W, group1)
    channel_mix(w["point_t"], h, W, pw, W)
    coef = analyse(h, W, g, waves_ref)
    synthesise(mix_modes(coef, wr, wi, 1, c), W, a, waves_ref)
    def group2(gr):
        rows = to_rows(waves_of(a, gr))
        for i in range(ROWS):
            sl = pl.ds(i * W + gr, 8)
            _, der = gelu_parts(rows[i] + pw[sl, :])
            h[sl, :] = der * pc[sl, :]
    each_group(W, group2)
    channel_mix(w["point"], h, W, pw, W)
    coef = analyse(h, W, g, waves_ref)
    synthesise(unmix_modes(coef, wr, wi, 1, r), W, a, waves_ref)
    def group3(gr):
        rows = to_rows(waves_of(a, gr))
        for i in range(ROWS):
            sl = pl.ds(i * W + gr, 8)
            h[sl, :] = d1[sl, :] * (rows[i] + pw[sl, :])
    each_group(W, group3)
    channel_mix(w["out"], h, W, pw, CIN)
    coef = analyse(h, W, g, waves_ref)
    coef = unmix_modes(coef, wr, wi, 0, r)
    coef = jnp.dot(w["lift"], coef, precision=HIGHEST, preferred_element_type=F32)
    synthesise(coef, CIN, a, waves_ref)
    def group4(gr):
        rows = to_rows(waves_of(a, gr))
        for i in range(ROWS):
            sl = pl.ds(i * CIN + gr, 8)
            out_ref[sl, :] = rows[i] + pw[sl, :]
    each_group(CIN, group4)


VARS = 5
TILE = 8
MESH = pl.DeviceIdType.MESH
AROUND = sorted(
    ((dx, dy) for dx in range(-2, 3) for dy in range(-2, 3) if (dx, dy) != (0, 0)),
    key=lambda o: (o[1] == 0, abs(o[1]), abs(o[0]), o),
)


ROUND = [o for o in AROUND if o[0] > 0]


def tiles_of(dx, dy):
    if abs(dx) == 2 or abs(dy) == 2:
        return 1
    return VARS if dx == 0 or dy == 0 else 3


START = {}
TILES = 0
for _o in AROUND:
    START[_o] = TILES
    TILES += tiles_of(*_o)


def pieces(dx, dy):
    out = []
    far_col, near_col = 0, 32 if dy == -1 else 0
    blocks = {-1: (1,), 0: (0, 1), 1: (0,)}[dx]
    for ch in range(VARS):
        if dx == 0:
            for rb in blocks:
                out.append(("near", ch, rb, near_col, 32, ch, 32 * rb))
            out.append(("far", ch, 0, far_col, 32, ch, 64))
        elif dy == 0:
            out.append(("near", ch, blocks[0], 0, 64, ch, 0))
            out.append(("far", ch, 0, 0, 32, ch, 64))
        else:
            base = 64 * (ch % 2)
            out.append(("near", ch, blocks[0], near_col, 32, ch // 2, base))
            out.append(("far", ch, 0, far_col, 32, ch // 2, base + 32))
    return out


def far_edge_col(dy):
    return 16 if dy == -2 else 0


def near_lane(col, dy=0):
    return 32 + col + 64 * dy


def far_lane(col, dy=0):
    return 48 + col + 32 * dy


FAR_ROW = {-2: 0, -1: 4, 0: 12, 1: 20, 2: 28}


def lane_ids():
    return lax.broadcasted_iota(jnp.int32, (TILE, COLS), 1)


def row_ids():
    return lax.broadcasted_iota(jnp.int32, (TILE, COLS), 0)


def turned(x, shift, axis=1, period=None):
    shift %= period or x.shape[axis]
    return x if shift == 0 else pltpu.roll(x, shift, axis)


class Lanes:
    def __init__(self):
        self.lane = lane_ids()
        self.row = row_ids()
        self.masks = {}

    def mask(self, first, width):
        key = (first, width)
        if key not in self.masks:
            self.masks[key] = (self.lane >= first) & (self.lane < first + width)
        return self.masks[key]

    def put(self, base, value, first, width):
        return value if base is None else jnp.where(self.mask(first, width), value, base)

    def only(self, value, first, width):
        return jnp.where(self.mask(first, width), value, 0.0)


def pool_maps():
    j = np.arange(COLS)[:, None]
    lane = np.arange(COLS)[None, :]
    gather = np.concatenate(
        [((lane - 32) % 64 == j // 2) * 0.25, ((lane - 48) % 32 == j // 4) * 0.0625], axis=1
    )
    spread = np.concatenate(
        [(j - 32 == lane // 2) * 0.25, (j - 48 == lane // 4) * 0.0625], axis=1
    )
    return np.concatenate([gather, spread], axis=0).astype(jnp.bfloat16)


def mapped(rows, table):
    hi, lo = split(rows)
    both = jnp.dot(jnp.concatenate([hi, lo], axis=0), table, preferred_element_type=F32)
    return both[: rows.shape[0]] + both[rows.shape[0]:]


def send_tiles(lanes, near, far, buf):
    rolled = {}

    def near_at(ch, rb, col, lane):
        key = ("n", ch, rb, (lane - near_lane(col)) % 64)
        if key not in rolled:
            rolled[key] = turned(near[ch][rb], key[3], period=64)
        return rolled[key]

    def far_at(ch, col, lane):
        key = ("f", ch, (lane - far_lane(col)) % 32)
        if key not in rolled:
            rolled[key] = turned(far[ch], key[2], period=32)
        return rolled[key]

    strips = {}
    for dx, dy in AROUND:
        start = START[dx, dy]
        if abs(dy) == 2:
            if ("y", dy) not in strips:
                tile = None
                for ch in range(VARS):
                    tile = lanes.put(tile, far_at(ch, far_edge_col(dy), 16 * ch), 16 * ch, 16)
                strips["y", dy] = tile
            buf[start * TILE:(start + 1) * TILE, :] = strips["y", dy]
        elif abs(dx) == 2:
            if ("x", dx) not in strips:
                tile = None
                for ch in range(4):
                    tile = lanes.put(tile, far_at(ch, 0, 32 * ch), 32 * ch, 32)
                last = far_at(4, 0, 0)
                if dx == -2:
                    tile = turned(tile, 4, axis=0)
                else:
                    last = turned(last, 4, axis=0)
                strips["x", dx] = jnp.where(lanes.mask(0, 32) & (lanes.row >= 4), last, tile)
            buf[start * TILE:(start + 1) * TILE, :] = strips["x", dx]
        else:
            tiles = [None] * tiles_of(dx, dy)
            for kind, ch, rb, col, width, tile, lane in pieces(dx, dy):
                value = near_at(ch, rb, col, lane) if kind == "near" else far_at(ch, col, lane)
                tiles[tile] = lanes.put(tiles[tile], value, lane, width)
            for n, value in enumerate(tiles):
                buf[(start + n) * TILE:(start + n + 1) * TILE, :] = value


def tile_at(buf, o, n=0):
    first = (START[o] + n) * TILE
    return buf[first:first + TILE, :]


def read_windows(lanes, near, far, buf, f_ref):
    blocks = {}
    rows = {}
    for ch in range(VARS):
        blocks[ch, 1], blocks[ch, 2] = near[ch]
        rows[ch, 0] = far[ch]
    for dx in (0, -1, 1):
        for dy in (0, -1, 1):
            if (dx, dy) == (0, 0):
                continue
            for kind, ch, rb, col, width, tile, lane in pieces(dx, dy):
                value = tile_at(buf, (dx, dy), tile)
                if kind == "near":
                    key = (ch, {-1: 0, 0: 1 + rb, 1: 3}[dx])
                    to, table = near_lane(col, dy), blocks
                else:
                    key, to, table = (ch, dx), far_lane(col, dy), rows
                table[key] = lanes.put(table.get(key), turned(value, to - lane), to, width)
    for dx in (-2, 2):
        for dy in (0, -1, 1):
            value = tile_at(buf, (dx, dy))
            low = turned(value, 4, axis=0)
            for ch in range(VARS):
                to, lane = far_lane(0, dy), 32 * ch if ch < 4 else 0
                got = turned(value if ch < 4 else low, to - lane)
                rows[ch, dx] = lanes.put(rows.get((ch, dx)), got, to, 32)
    for dx in range(-2, 3):
        for dy in (-2, 2):
            value = tile_at(buf, (dx, dy))
            if dx == -2:
                value = turned(value, 4, axis=0)
            for ch in range(VARS):
                to = far_lane(far_edge_col(dy), dy)
                rows[ch, dx] = lanes.put(rows[ch, dx], turned(value, to - 16 * ch), to, 16)
    for (ch, k), value in blocks.items():
        f_ref[pl.ds(8 * k * CIN + VARS + ch, TILE, stride=CIN), :] = value
    for (ch, dx), value in rows.items():
        count = 4 if abs(dx) == 2 else TILE
        f_ref[pl.ds(FAR_ROW[dx] * CIN + 2 * VARS + ch, count, stride=CIN), :] = value[:count]


def window_tiles(go):
    near = {(ch, k): go[pl.ds(8 * k * CIN + VARS + ch, TILE, stride=CIN), :] for ch in range(VARS) for k in range(4)}
    far = {}
    for ch in range(VARS):
        for dx in range(-2, 3):
            first = 24 if dx == 2 else FAR_ROW[dx]
            far[ch, dx] = go[pl.ds(first * CIN + 2 * VARS + ch, TILE, stride=CIN), :]
    return near, far


def send_grads(lanes, near, far, buf):
    for dx, dy in AROUND:
        start = START[dx, dy]
        if abs(dy) == 2:
            tile = None
            for ch in range(VARS):
                got = turned(far[ch, dx], 16 * ch - far_lane(far_edge_col(dy), dy))
                tile = lanes.put(tile, got, 16 * ch, 16)
            if abs(dx) == 2:
                tile = turned(tile, 4, axis=0)
                keep = lanes.row >= 4 if dx == -2 else lanes.row < 4
                tile = jnp.where(keep, tile, 0.0)
            buf[start * TILE:(start + 1) * TILE, :] = tile
        elif abs(dx) == 2:
            tile = None
            for ch in range(4):
                tile = lanes.put(tile, turned(far[ch, dx], 32 * ch - far_lane(0, dy)), 32 * ch, 32)
            last = turned(far[4, dx], -far_lane(0, dy))
            if dx == -2:
                last = turned(last, 4, axis=0)
            else:
                tile = turned(tile, 4, axis=0)
            buf[start * TILE:(start + 1) * TILE, :] = jnp.where(lanes.mask(0, 32) & (lanes.row >= 4), last, tile)
        else:
            tiles = [None] * tiles_of(dx, dy)
            for kind, ch, rb, col, width, tile, lane in pieces(dx, dy):
                if kind == "near":
                    value = turned(near[ch, {-1: 0, 0: 1 + rb, 1: 3}[dx]], lane - near_lane(col, dy))
                else:
                    value = turned(far[ch, dx], lane - far_lane(col, dy))
                tiles[tile] = lanes.put(tiles[tile], value, lane, width)
            for n, value in enumerate(tiles):
                buf[(start + n) * TILE:(start + n + 1) * TILE, :] = value


def sum_grads(lanes, near, far, buf, wait):
    n_sum = {(ch, rb): lanes.only(near[ch, 1 + rb], 32, 64) for ch in range(VARS) for rb in range(2)}
    f_sum = {ch: lanes.only(far[ch, 0], 48, 32) for ch in range(VARS)}
    for o in AROUND:
        if o[1] == 0:
            wait(o)
    for dy in (0, -1, 1):
        for dx in (-1, 0, 1):
            if (dx, dy) == (0, 0):
                continue
            if dy != 0:
                wait((dx, dy))
            for kind, ch, rb, col, width, tile, lane in pieces(dx, dy):
                value = tile_at(buf, (dx, dy), tile)
                if kind == "near":
                    to = near_lane(col)
                    n_sum[ch, rb] += lanes.only(turned(value, to - lane), to, width)
                else:
                    to = far_lane(col)
                    f_sum[ch] += lanes.only(turned(value, to - lane), to, width)
    for o in AROUND:
        if o[1] != 0 and max(abs(o[0]), abs(o[1])) == 2:
            wait(o)
    for dx in (-2, 2):
        value = tree_sum([tile_at(buf, (dx, dy)) for dy in (-1, 0, 1)])
        low = turned(value, 4, axis=0)
        keep = lanes.row >= 4 if dx == -2 else lanes.row < 4
        for ch in range(VARS):
            natural = (ch < 4) == (dx == 2)
            lane = 32 * ch if ch < 4 else 0
            got = turned(value if natural else low, far_lane(0) - lane)
            f_sum[ch] += jnp.where(lanes.mask(48, 32) & keep, got, 0.0)
    for dy in (-2, 2):
        value = tree_sum([tile_at(buf, (dx, dy)) for dx in range(-2, 3)])
        for ch in range(VARS):
            to = far_lane(far_edge_col(dy))
            f_sum[ch] += lanes.only(turned(value, to - 16 * ch), to, 16)
    return (
        jnp.concatenate([n_sum[ch, rb] for ch in range(VARS) for rb in range(2)], axis=0),
        jnp.concatenate([f_sum[ch] for ch in range(VARS)], axis=0),
    )


Y_SIDE = 4
EDGES = (1, -1, 2, -2)
RELAY = {1: 0, -1: VARS, 2: 2 * VARS, -2: 2 * VARS + 1}
PASSED = {-1: 0, 1: 3, -2: 6, 2: 7}


def repack(lanes, main, e, buf, first):
    for dx in (-1, 1):
        tiles = [None] * 3
        for kind, ch, rb, _, width, tile, lane in pieces(dx, -e):
            value = turned(main[ch], lane - (32 * rb if kind == "near" else 64))
            tiles[tile] = lanes.put(tiles[tile], value, lane, width)
        for n, value in enumerate(tiles):
            row = (first + PASSED[dx] + n) * TILE
            buf[row:row + TILE, :] = value
    strip = None
    for ch in range(4):
        strip = lanes.put(strip, turned(main[ch], 32 * ch - 64), 32 * ch, 32)
    last = turned(main[4], -64)
    corner = lanes.mask(0, 32) & (lanes.row >= 4)
    for dx in (-2, 2):
        row = (first + PASSED[dx]) * TILE
        low, high = (turned(strip, 4, axis=0), last) if dx == -2 else (strip, turned(last, 4, axis=0))
        buf[row:row + TILE, :] = jnp.where(corner, high, low)


def kernel(counts, field_hbm, cot_hbm, lift_hbm, spectral_hbm, point_hbm, proj_hbm, waves_hbm, maps_hbm, out_ref,
           field, cot, lift, spectral, point, proj, waves, maps, f, ct, go, pooled, spread_near, spread_far,
           fwd_out, fwd_in, bwd_out, bwd_in, relay_in, relay_out, load_sem, send_sem, recv_sem, to_mid_sem, at_mid_sem,
           from_mid_sem, stage_in, stage_sem, ready_sem, *scr):
    gx, gy = lax.axis_index("gx"), lax.axis_index("gy")
    n_gx, n_gy = counts
    loads = [
        pltpu.make_async_copy(src, dst, load_sem.at[n])
        for n, (src, dst) in enumerate([
            (field_hbm, field), (maps_hbm, maps), (cot_hbm, cot), (lift_hbm, lift), (point_hbm, point),
            (proj_hbm, proj), (spectral_hbm, spectral), (waves_hbm, waves)])
    ]
    for copy in loads:
        copy.start()
    half_z = n_gx // 2
    n_z = 2 * half_z
    y = lax.rem(gy, Y_SIDE)
    index = {o: n for n, o in enumerate(AROUND)}

    def device(dx, dy, base=None):
        bx, by = base or (gx, gy)
        return (lax.rem(bx + (dx + n_gx), n_gx), lax.rem(by + (dy + n_gy), n_gy))

    def crosses(e):
        return (y + e < 0) | (y + e >= Y_SIDE)

    def middle(place, sign):
        px, py = place
        core, group = lax.rem(px, 2), lax.div(py, Y_SIDE)
        z = lax.rem(group, 2) * half_z + lax.div(px, 2)
        step = sign * (n_z // 4)
        z = lax.rem(z + jnp.where(core == 0, n_z + step, n_z - step), n_z)
        row = lax.div(group, 2) * (2 * Y_SIDE) + lax.div(z, half_z) * Y_SIDE + lax.rem(py, Y_SIDE)
        return (2 * lax.rem(z, half_z) + core, row)

    mine, source = middle((gx, gy), 1), middle((gx, gy), -1)

    hop = 2 * ((half_z - 1) // 2)
    staged = lax.div(gx, 2) == hop // 2
    stage_source = gx - hop
    edge = gx < 2

    def stage_of(px):
        return px + hop

    def goes_round(o, px):
        round_end = px - o[0] < 0
        return round_end if o[1] == 0 else round_end & jnp.logical_not(crosses(-o[1]))

    def count(flag):
        return jnp.where(flag, 1, 0)

    quarter_z, half_here = n_z // 4, lax.rem(lax.div(gy, Y_SIDE), 2)
    early_here = half_here * half_z + lax.div(gx, 2) < quarter_z
    early, tell_later = {}, {}
    for dx in range(-2, 3):
        ox = lax.rem(gx + (dx + n_gx), n_gx)
        oz = (1 - half_here) * half_z + lax.div(ox, 2)
        oz += jnp.where(lax.rem(ox, 2) == 0, n_z + quarter_z, n_z - quarter_z)
        early[dx] = lax.rem(oz, n_z) < quarter_z

    barrier = pltpu.get_barrier_semaphore()
    by_middle = half_here == 0
    relays = lax.rem(lax.div(source[1], Y_SIDE), 2) == 0
    pl.when(relays)(functools.partial(
        pl.semaphore_signal, barrier, inc=1, device_id=source, device_id_type=MESH))
    for dx, dy in AROUND:
        owner = sender = device(dx, dy)
        if dx != 0:
            round_end = gx + dx >= n_gx
            sender = (jnp.where(round_end, stage_of(owner[0]), owner[0]), owner[1])
        told = functools.partial(pl.semaphore_signal, barrier, inc=1, device_id_type=MESH)
        if dy == 0:
            told(device_id=sender)
            continue
        via, far_one = middle(owner, 1), crosses(dy)
        across = tuple(jnp.where(half_here == 1, a, b) for a, b in zip(via, owner))
        sender = tuple(jnp.where(far_one, a, b) for a, b in zip(across, sender))
        tell_later[dx, dy] = (far_one & (half_here == 1) & early[dx], via)
        pl.when(jnp.logical_not(tell_later[dx, dy][0]))(functools.partial(told, device_id=sender))

    @pl.when(early_here & relays)
    def _():
        for e in EDGES:
            @pl.when(crosses(e))
            def _(e=e):
                for ex in range(-2, 3):
                    pl.semaphore_signal(barrier, inc=1, device_id=device(ex, e, source), device_id_type=MESH)

    @pl.when(staged)
    def _():
        pl.semaphore_signal(barrier, inc=1, device_id=(stage_source, gy), device_id_type=MESH)

    expected = len(AROUND) + count(by_middle) + count(edge)
    for o in AROUND:
        if o[0] > 0:
            expected += count(staged & goes_round(o, stage_source)) - count(goes_round(o, gx))
    for later, _ in tell_later.values():
        expected += count(later)
    for e in EDGES:
        expected += 5 * (count(crosses(e) & relays & jnp.logical_not(early_here)) - count(crosses(e) & by_middle))
    def span(o):
        return pl.ds(START[o] * TILE, tiles_of(*o) * TILE)

    def direct(turn, src, dst, o):
        sign = -1 if turn == 0 else 1
        return pltpu.make_async_remote_copy(
            src_ref=src.at[span(o)], dst_ref=dst.at[span(o)], send_sem=send_sem.at[turn, index[o]],
            recv_sem=recv_sem.at[turn, index[o]], device_id=device(sign * o[0], sign * o[1]), device_id_type=MESH)

    def to_middle(e):
        tiles = tiles_of(0, -e)
        return pltpu.make_async_remote_copy(
            src_ref=fwd_out.at[span((0, -e))], dst_ref=relay_in.at[pl.ds(RELAY[e] * TILE, tiles * TILE)],
            send_sem=to_mid_sem.at[EDGES.index(e)], recv_sem=at_mid_sem.at[EDGES.index(e)], device_id=mine,
            device_id_type=MESH)

    def from_middle(e, ex):
        o = (-ex, -e)
        if abs(e) == 2 or ex == 0:
            first, ref = RELAY[e], relay_in
        else:
            first, ref = PASSED[-ex] + (0 if e == 1 else 8), relay_out
        return pltpu.make_async_remote_copy(
            src_ref=ref.at[pl.ds(first * TILE, tiles_of(*o) * TILE)], dst_ref=fwd_in.at[span(o)],
            send_sem=from_mid_sem.at[EDGES.index(e), ex + 2], recv_sem=recv_sem.at[0, index[o]],
            device_id=device(ex, e, source), device_id_type=MESH)

    def to_stage(o):
        return pltpu.make_async_remote_copy(
            src_ref=fwd_out.at[span(o)], dst_ref=stage_in.at[span(o)], send_sem=stage_sem.at[0, index[o]],
            recv_sem=stage_sem.at[1, index[o]], device_id=(stage_of(gx), gy), device_id_type=MESH)

    def from_stage(o):
        return pltpu.make_async_remote_copy(
            src_ref=stage_in.at[span(o)], dst_ref=fwd_in.at[span(o)], send_sem=stage_sem.at[2, index[o]],
            recv_sem=recv_sem.at[0, index[o]], device_id=device(-o[0], -o[1], (stage_source, gy)), device_id_type=MESH)

    lanes = Lanes()
    loads[0].wait()
    loads[1].wait()
    half = field[pl.ds(0, 80, stride=2), :] + field[pl.ds(1, 80, stride=2), :]
    pooled[...] = half
    quarter = pooled[pl.ds(0, 40, stride=2), :] + pooled[pl.ds(1, 40, stride=2), :]
    got = mapped(jnp.concatenate([half, quarter], axis=0), maps[0:COLS, :])
    near = [[got[ch * 16 + rb * 8:ch * 16 + rb * 8 + 8, :COLS] for rb in range(2)] for ch in range(VARS)]
    far = [got[80 + ch * 8:80 + ch * 8 + 8, COLS:] for ch in range(VARS)]
    send_tiles(lanes, near, far, fwd_out)
    pl.semaphore_wait(barrier, expected)
    for o, (later, via) in tell_later.items():
        pl.when(later)(functools.partial(
            pl.semaphore_signal, ready_sem.at[index[o]], inc=1, device_id=via, device_id_type=MESH))

    def pass_on(e, ex):
        pl.when(early_here)(functools.partial(pl.semaphore_wait, ready_sem.at[index[-ex, -e]], 1))
        from_middle(e, ex).start()

    for e in EDGES:
        @pl.when(crosses(e) & by_middle)
        def _(e=e):
            to_middle(e).start()
    for o in ROUND:
        @pl.when(goes_round(o, gx))
        def _(o=o):
            to_stage(o).start()

    def goes_directly(o):
        target = gx - o[0]
        inside = target >= 0
        if o[1] == 0:
            return inside
        across = crosses(-o[1])
        return (across & jnp.logical_not(by_middle)) | (inside & jnp.logical_not(across))

    for o in AROUND:
        @pl.when(goes_directly(o))
        def _(o=o):
            direct(0, fwd_out, fwd_in, o).start()

    for copy in loads[2:]:
        copy.wait()
    f[...] = jnp.zeros_like(f)
    ct[...] = jnp.zeros_like(ct)
    for v in range(VARS):
        f[pl.ds(v, ROWS, stride=CIN), :] = field[v * ROWS:(v + 1) * ROWS, :]
        ct[pl.ds(v, ROWS, stride=8), :] = cot[v * ROWS:(v + 1) * ROWS, :]
    setup = network_setup(ct, lift, spectral, point, proj, scr)

    @pl.when(staged)
    def _():
        for o in ROUND:
            @pl.when(goes_round(o, stage_source))
            def _(o=o):
                to_stage(o).wait_recv()
                from_stage(o).start()

    for e in EDGES:
        @pl.when(crosses(e) & relays)
        def _(e=e):
            to_middle(e).wait_recv()
            pass_on(e, 0)
            if abs(e) == 1:
                main = [relay_in[(RELAY[e] + ch) * TILE:(RELAY[e] + ch + 1) * TILE, :] for ch in range(VARS)]
                repack(Lanes(), main, e, relay_out, 0 if e == 1 else 8)
            for ex in (-1, 1, -2, 2):
                pass_on(e, ex)

    for o in AROUND:
        direct(0, fwd_out, fwd_in, o).wait_recv()
    read_windows(lanes, near, far, fwd_in, f)
    network_grad(f, setup, waves, go, scr)

    near, far = window_tiles(go)
    send_grads(lanes, near, far, bwd_out)
    for o in AROUND:
        direct(1, bwd_out, bwd_in, o).start()
    n_sum, f_sum = sum_grads(lanes, near, far, bwd_in, lambda o: direct(1, bwd_out, bwd_in, o).wait_recv())
    got = mapped(jnp.concatenate([n_sum, f_sum], axis=0), maps[COLS:, :])
    for k in range(2):
        spread_near[pl.ds(k, 80, stride=2), :] = got[:80, :COLS]
    for k in range(4):
        spread_far[pl.ds(k, 40, stride=4), :] = got[80:, COLS:]
    for v in range(VARS):
        rows = slice(v * ROWS, (v + 1) * ROWS)
        out_ref[rows, :] = go[pl.ds(v, ROWS, stride=CIN), :] + spread_near[rows, :] + spread_far[rows, :]
    for o in AROUND:
        direct(1, bwd_out, bwd_in, o).wait_send()

        @pl.when(goes_directly(o))
        def _(o=o):
            direct(0, fwd_out, fwd_in, o).wait_send()
    for e in EDGES:
        pl.when(crosses(e) & by_middle)(to_middle(e).wait_send)

        @pl.when(crosses(e) & relays)
        def _(e=e):
            for ex in range(-2, 3):
                from_middle(e, ex).wait_send()
    for o in ROUND:
        @pl.when(goes_round(o, gx))
        def _(o=o):
            to_stage(o).wait_send()

        @pl.when(staged & goes_round(o, stage_source))
        def _(o=o):
            from_stage(o).wait_send()


def body(counts, field, cotangent, lift, spectral, pointwise, project):
    vmem = lambda *shape, dtype=F32: pltpu.VMEM(shape, dtype)
    flat = (VARS * ROWS, COLS)
    hbm = pl.BlockSpec(memory_space=pltpu.MemorySpace.HBM)
    call = pl.pallas_call(
        functools.partial(kernel, counts),
        out_shape=pltpu.VMEM(flat, F32),
        in_specs=[hbm] * 8,
        out_specs=pl.BlockSpec(memory_space=pltpu.VMEM),
        scratch_shapes=[
            vmem(*flat), vmem(*flat), vmem(3 * VARS, W), vmem(2, 2, W, W, MD * MD), vmem(2, W, W), vmem(VARS, W),
            vmem(NWAVE * COLS, 2 * COLS, dtype=BF16), vmem(2 * COLS, 2 * COLS, dtype=BF16),
            vmem(ROWS * CIN, COLS), vmem(ROWS * 8, COLS), vmem(ROWS * CIN, COLS),
            vmem(80, COLS), vmem(*flat), vmem(*flat),
            vmem(TILES * TILE, COLS), vmem(TILES * TILE, COLS), vmem(TILES * TILE, COLS), vmem(TILES * TILE, COLS),
            vmem(12 * TILE, COLS), vmem(16 * TILE, COLS),
            pltpu.SemaphoreType.DMA((8,)), pltpu.SemaphoreType.DMA((2, len(AROUND))),
            pltpu.SemaphoreType.DMA((2, len(AROUND))),
            pltpu.SemaphoreType.DMA((4,)), pltpu.SemaphoreType.DMA((4,)), pltpu.SemaphoreType.DMA((4, 5)),
            vmem(TILES * TILE, COLS), pltpu.SemaphoreType.DMA((3, len(AROUND))),
            pltpu.SemaphoreType.REGULAR((len(AROUND),)),
            vmem(2, W, W, COLS), vmem(2, W, W, COLS), vmem(W, NWAVE * COLS), vmem(W, NWAVE * COLS),
            vmem(2 * W, COLS), vmem(W * 8, COLS), vmem(ROWS * W, COLS), vmem(ROWS * W, COLS), vmem(ROWS * W, COLS),
            vmem(ROWS * W, COLS),
        ],
        compiler_params=pltpu.CompilerParams(collective_id=0, has_side_effects=True, vmem_limit_bytes=55300 << 10),
        name="patch_grad",
    )
    out = call(
        field.reshape(flat), cotangent.reshape(flat), lift, spectral.transpose(0, 1, 3, 4, 2), pointwise, project.T,
        jnp.asarray(mode_waves()), jnp.asarray(pool_maps()))
    return out.reshape(field.shape)


def solution(mesh):
    counts = (mesh.shape["gx"], mesh.shape["gy"])
    return jax.shard_map(
        functools.partial(body, counts),
        mesh=mesh,
        in_specs=(P(None, None, "gx", "gy"), P(None, None, "gx", "gy"), P(), P(), P(), P()),
        out_specs=P(None, None, "gx", "gy"),
        check_vma=False,
    )
```
